32 devices in a mesh: wide: 8 (over z, x), narrow: 4 (over y, core).
Axes of the slice: x: 2, y: 2, z: 4, core: 2. Of those that a mesh axis runs over, the one named last changes fastest.
Arguments:
- old_basis: float32 [16, 2048, 512], P(None, ('wide', 'narrow')), may hold values from -6 to 6
- restart_coeffs: float32 [16], replicated, may hold values from -1 to 1
- geometry: float32 [4, 2048, 512], P(None, ('wide', 'narrow')), may hold values from 0.01 to 18, as said below
- orientation: int32 [6, 2048], P(None, ('wide', 'narrow')), may hold values from 0 to 7
Outputs:
- new_basis: float32 [2, 2048, 512], P(None, ('wide', 'narrow'))
- hessenberg: float32 [2, 18], replicated
The draws below stay inside these ranges and needn't reach their ends.
Inputs may be any that keep to these rules, and one draw needn't show every extreme that they name: `geometry`: every entry is positive.
All inputs are finite; a program needn't handle non-finite values.
Results may differ from the reference program's by a relative error of at most 0.0003.
Values sent between devices are 32-bit elements; how exact they have to be, the bound alone decides.
A program may use at most 64 MiB of HBM per device.

```python
import jax
import jax.numpy as jnp
import numpy as np
from jax import lax

NP = 8
PTS = 512
KB = 16
EX = 4
EY = 4
EZ = 4
ELEMS = 2048
N_WIDE = 8
N_NARROW = 4


def draw_geometry(key, part):
    noise = jax.random.uniform(jax.random.fold_in(key, 17), (4, ELEMS, PTS), jnp.float32)
    lower = jnp.array([0.01, 0.01, 0.01, 0.5], jnp.float32).reshape(4, 1, 1)
    upper = jnp.array([0.04, 0.04, 0.04, 2.0], jnp.float32).reshape(4, 1, 1)
    position = jnp.arange(ELEMS, dtype=jnp.float32) / max(ELEMS - 1, 1)
    base_vals = jnp.exp(jnp.log(lower) + noise * (jnp.log(upper) - jnp.log(lower)))
    ramp_vals = 1.0 + 2.0 * position
    return (base_vals * ramp_vals.reshape(1, ELEMS, 1)).astype(jnp.float32)


def plant(entries, stream_key, smallest, high):
    shape = entries.shape
    place = [jax.random.randint(jax.random.fold_in(stream_key, axis), (), 0, shape[axis]) for axis in range(len(shape))]
    entries = entries.at[tuple(place)].set(smallest)
    longest = shape.index(max(shape))
    place[longest] = (place[longest] + 1) % shape[longest]
    return entries.at[tuple(place)].set(high)


def shard_levels(stream_key, shape, split, least, largest):
    gain, own = 1.0, jax.random.fold_in(stream_key, 6)
    for axis_at, blocks in split:
        steps = jnp.exp(jax.random.uniform(jax.random.fold_in(own, axis_at), (blocks,), jnp.float32, least / len(split), largest / len(split)))
        gain = gain * jnp.repeat(steps, shape[axis_at] // blocks).reshape([-1 if axis == axis_at else 1 for axis in range(len(shape))])
    return gain


def gaussian(stream_key, dims, spread, bound, cuts=(), held_as=jnp.bfloat16):
    factor_of = shard_levels(stream_key, dims, cuts, -0.22, 0.18) if cuts else 1.0
    values = jax.random.normal(stream_key, dims, jnp.float32) * spread * factor_of
    return jnp.minimum(jnp.maximum(values, -bound), bound).astype(held_as)


def setup_inputs(seed: int = 0) -> dict:
    arg_keys = jax.random.split(jax.random.key(seed), 5)
    return {
        "old_basis": gaussian(arg_keys[0], (KB, ELEMS, PTS), 1.0, 6.0, ((1, 32),), jnp.float32),
        "restart_coeffs": gaussian(arg_keys[1], (KB,), 0.25, 1.0, (), jnp.float32),
        "geometry": draw_geometry(jax.random.fold_in(arg_keys[4], 71), 0),
        "orientation": plant(jax.random.randint(arg_keys[3], (6, ELEMS), 0, 8), jax.random.fold_in(arg_keys[3], 1), 0, 7).astype(jnp.int32),
    }


highest = lax.Precision.HIGHEST
epsilon = 1e-06

def legendre_columns(nodes, degree):
    columns = [nodes * 0.0 + 1.0, nodes * 1.0]
    for order in range(2, degree + 1):
        columns.append(((2 * order - 1) * nodes * columns[order - 1] - (order - 1) * columns[order - 2]) / order)
    return columns

def gll_derivative(extent):
    degree = extent - 1
    nodes = np.cos(np.pi * np.arange(extent) / degree)
    for sweep in range(100):
        columns = legendre_columns(nodes, degree)
        nodes = nodes - (nodes * columns[degree] - columns[degree - 1]) / (extent * columns[degree])
    gll_nodes = nodes[::-1] * 1.0
    values = legendre_columns(gll_nodes, degree)[degree]
    matrix = np.zeros((extent, extent))
    for row_idx in range(extent):
        for col_idx in range(extent):
            if row_idx != col_idx:
                matrix[row_idx, col_idx] = values[row_idx] / (values[col_idx] * (gll_nodes[row_idx] - gll_nodes[col_idx]))
    matrix[0, 0] = -degree * (degree + 1) / 4.0
    matrix[extent - 1, extent - 1] = degree * (degree + 1) / 4.0
    return matrix

def face_point(face_kind, row_pos, col_pos, extent):
    far_end = extent - 1
    if face_kind == 0:
        return (0, row_pos, col_pos)
    if face_kind == 1:
        return (far_end, row_pos, col_pos)
    if face_kind == 2:
        return (row_pos, 0, col_pos)
    if face_kind == 3:
        return (row_pos, far_end, col_pos)
    if face_kind == 4:
        return (row_pos, col_pos, 0)
    return (row_pos, col_pos, far_end)

def spectral_tables(extent):
    matrix = gll_derivative(extent)
    identity = np.eye(extent)
    along_x = np.kron(np.kron(matrix, identity), identity)
    along_y = np.kron(np.kron(identity, matrix), identity)
    along_z = np.kron(np.kron(identity, identity), matrix)
    forward = np.concatenate([along_x.T, along_y.T, along_z.T], axis=1)
    backward = np.concatenate([along_x, along_y, along_z], axis=0)
    square = extent * extent
    select = np.zeros((extent ** 3, 6 * square))
    rotations = np.zeros((square, 8 * square))
    for face_kind in range(6):
        for row_pos in range(extent):
            for col_pos in range(extent):
                triple = face_point(face_kind, row_pos, col_pos, extent)
                point_idx = (triple[0] * extent + triple[1]) * extent + triple[2]
                select[point_idx, face_kind * square + row_pos * extent + col_pos] = 1.0
    for code_value in range(8):
        for row_pos in range(extent):
            for col_pos in range(extent):
                row_src = extent - 1 - row_pos if code_value % 2 == 1 else row_pos
                col_src = extent - 1 - col_pos if code_value // 2 % 2 == 1 else col_pos
                if code_value >= 4:
                    source = col_src * extent + row_src
                else:
                    source = row_src * extent + col_src
                rotations[source, code_value * square + row_pos * extent + col_pos] = 1.0
    return (jnp.asarray(forward, dtype=jnp.float32), jnp.asarray(backward, dtype=jnp.float32), jnp.asarray(select, dtype=jnp.float32), jnp.asarray(rotations, dtype=jnp.float32))

def stiffness(field_in, geom_cat, mass_term, forward, backward):
    gradients = jnp.dot(field_in, forward, precision=highest, preferred_element_type=jnp.float32)
    return jnp.dot(gradients * geom_cat, backward, precision=highest, preferred_element_type=jnp.float32) + mass_term * field_in

def local_faces(local_out, select):
    face_vals = jnp.dot(local_out, select, precision=highest, preferred_element_type=jnp.float32)
    return face_vals.reshape(face_vals.shape[:-1] + (6, face_vals.shape[-1] // 6))

def shift_lower(values, direction):
    extent = values.shape[direction]
    leading = jnp.zeros_like(lax.slice_in_dim(values, 0, 1, axis=direction))
    return jnp.concatenate([leading, lax.slice_in_dim(values, 0, extent - 1, axis=direction)], axis=direction)

def shift_upper(values, direction):
    extent = values.shape[direction]
    trailing = jnp.zeros_like(lax.slice_in_dim(values, 0, 1, axis=direction))
    return jnp.concatenate([lax.slice_in_dim(values, 1, extent, axis=direction), trailing], axis=direction)

def assemble(local_out, incoming, orient_block, select, rotations):
    rotated = jnp.dot(incoming, rotations, precision=highest, preferred_element_type=jnp.float32)
    rotated = rotated.reshape(incoming.shape[:-1] + (8, incoming.shape[-1]))
    chosen_mask = orient_block[..., None] == jnp.arange(8, dtype=jnp.int32)
    chosen = lax.optimization_barrier(jnp.sum(jnp.where(chosen_mask[..., None], rotated, 0.0), axis=-2))
    flattened = chosen.reshape(chosen.shape[:-2] + (chosen.shape[-2] * chosen.shape[-1],))
    return local_out + jnp.dot(flattened, select.T, precision=highest, preferred_element_type=jnp.float32)

def to_grid(values):
    last_dim = values.shape[-1]
    shaped = values.reshape(N_WIDE, N_NARROW, EX, EY, EZ, last_dim).transpose(2, 1, 3, 0, 4, 5)
    return shaped.reshape(EX, N_NARROW * EY, N_WIDE * EZ, last_dim)

def from_grid(values):
    last_dim = values.shape[-1]
    shaped = values.reshape(EX, N_NARROW, EY, N_WIDE, EZ, last_dim).transpose(3, 1, 0, 2, 4, 5)
    return shaped.reshape(-1, last_dim)

def reference(old_basis, restart_coeffs, geometry, orientation):
    forward, backward, select, rotations = spectral_tables(NP)
    kept = old_basis.shape[0]
    total = float(old_basis.shape[1] * old_basis.shape[2])
    geom_cat = to_grid(jnp.concatenate([geometry[0], geometry[1], geometry[2]], axis=-1))
    mass_term = to_grid(geometry[3])
    orient_block = to_grid(orientation.T)
    flat_basis = old_basis.reshape(kept, -1)

    def operate(vector):
        local_out = stiffness(to_grid(vector), geom_cat, mass_term, forward, backward)
        face_vals = local_faces(local_out, select)
        incoming = jnp.stack([shift_lower(face_vals[..., 1, :], 0), shift_upper(face_vals[..., 0, :], 0), shift_lower(face_vals[..., 3, :], 1), shift_upper(face_vals[..., 2, :], 1), shift_lower(face_vals[..., 5, :], 2), shift_upper(face_vals[..., 4, :], 2)], axis=-2)
        return from_grid(assemble(local_out, incoming, orient_block, select, rotations))

    def inner(vector):
        return jnp.dot(flat_basis, vector.reshape(-1), precision=highest, preferred_element_type=jnp.float32) / total

    def combine(weights):
        return jnp.einsum('k,kep->ep', weights, old_basis, precision=highest, preferred_element_type=jnp.float32)
    start_vec = combine(restart_coeffs)
    image_one = operate(start_vec)
    first_proj = inner(image_one)
    residue_one = image_one - combine(first_proj)
    first_norm = jnp.sqrt(jnp.sum(residue_one * residue_one) / total + epsilon)
    first_vec = residue_one / first_norm
    image_two = operate(first_vec)
    second_proj = inner(image_two)
    second_self = jnp.sum(first_vec * image_two) / total
    residue_two = image_two - combine(second_proj) - second_self * first_vec
    second_norm = jnp.sqrt(jnp.sum(residue_two * residue_two) / total + epsilon)
    second_vec = residue_two / second_norm
    new_basis = jnp.stack([first_vec, second_vec])
    row_first = jnp.concatenate([first_proj, jnp.stack([first_norm, jnp.zeros_like(first_norm)])])
    row_second = jnp.concatenate([second_proj, jnp.stack([second_self, second_norm])])
    return (new_basis, jnp.stack([row_first, row_second]))
```

```python
import functools

import jax
import jax.numpy as jnp
import numpy as np
from jax import lax
from jax.experimental import pallas as pl
from jax.experimental.pallas import tpu as pltpu
from jax.sharding import PartitionSpec as P

NP = 8
EX = 4
EY = 4
EZ = 4
LANES = 128
FACE = NP * NP
MESH = pl.DeviceIdType.MESH
highest = lax.Precision.HIGHEST
epsilon = 1e-06


def legendre_columns(nodes, degree):
    columns = [nodes * 0.0 + 1.0, nodes * 1.0]
    for order in range(2, degree + 1):
        columns.append(
            ((2 * order - 1) * nodes * columns[order - 1] - (order - 1) * columns[order - 2])
            / order
        )
    return columns


def gll_derivative(extent):
    degree = extent - 1
    nodes = np.cos(np.pi * np.arange(extent) / degree)
    for sweep in range(100):
        columns = legendre_columns(nodes, degree)
        nodes = nodes - (nodes * columns[degree] - columns[degree - 1]) / (extent * columns[degree])
    gll_nodes = nodes[::-1] * 1.0
    values = legendre_columns(gll_nodes, degree)[degree]
    matrix = np.zeros((extent, extent))
    for row_idx in range(extent):
        for col_idx in range(extent):
            if row_idx != col_idx:
                matrix[row_idx, col_idx] = values[row_idx] / (
                    values[col_idx] * (gll_nodes[row_idx] - gll_nodes[col_idx])
                )
    matrix[0, 0] = -degree * (degree + 1) / 4.0
    matrix[extent - 1, extent - 1] = degree * (degree + 1) / 4.0
    return matrix


def halves(table):
    table = np.asarray(table, np.float32)
    upper = table.astype(jnp.bfloat16).astype(np.float32)
    return upper, table - upper


def tables():
    matrix = gll_derivative(NP)
    identity = np.eye(NP)
    pair = np.eye(2)
    along_y = np.kron(pair, np.kron(matrix, identity))
    along_z = np.kron(pair, np.kron(identity, matrix))
    forward = np.concatenate([along_y.T, along_z.T], axis=1)
    backward = np.concatenate([along_y, along_z], axis=0)
    tiles = NP // 2
    coef = np.zeros((2, tiles, tiles, 2, LANES))
    for way, table in enumerate((matrix, matrix.T)):
        for out_tile in range(tiles):
            for in_tile in range(tiles):
                for half in range(2):
                    lanes = slice(half * FACE, (half + 1) * FACE)
                    row = 2 * out_tile + half
                    coef[way, out_tile, in_tile, 0, lanes] = table[row, 2 * in_tile + half]
                    coef[way, out_tile, in_tile, 1, lanes] = table[row, 2 * in_tile + 1 - half]
    ahead, ahead_rest = halves(forward)
    back, back_rest = halves(backward)
    packed = np.concatenate([ahead, ahead_rest, np.concatenate([back, back_rest], axis=1)], axis=0)
    return (
        jnp.asarray(packed, jnp.bfloat16),
        jnp.asarray(coef.reshape(-1, LANES), jnp.float32),
    )


def pair_rows(kept):
    count = kept + 2
    listed = [(at, kept + 1) for at in range(count)]
    listed += [(at, kept) for at in range(kept + 1)]
    block = 4
    for left in range(0, kept, block):
        for right in range(left, kept, block):
            for one in range(left, left + block):
                for two in range(max(right, one), right + block):
                    listed.append((one, two))
    return -(-len(listed) // LANES), listed


def take_lanes(values, index):
    return jnp.take_along_axis(values, index, axis=1, mode="promise_in_bounds")


def rotated(row, col, code):
    row = row ^ (7 * (code & 1))
    col = col ^ (7 * ((code >> 1) & 1))
    return jnp.where((code & 4) != 0, col * NP + row, row * NP + col)


def kernel(
    n_wide,
    n_narrow,
    coeffs_hbm,
    basis_hbm,
    geom_hbm,
    orient_hbm,
    packed_hbm,
    coef_hbm,
    pairs_hbm,
    out,
    hess,
    coeffs,
    basis,
    geom,
    orient,
    packed,
    coef,
    index,
    orient_pad,
    image,
    first,
    face_y,
    face_z,
    halo_y,
    halo_z,
    outbox,
    inbox,
    pairs,
    row_out,
    row_in,
    pair_out,
    pair_in,
    load_sem,
    halo_send,
    halo_recv,
    row_send,
    row_recv,
):
    wide = lax.axis_index("wide")
    narrow = lax.axis_index("narrow")
    devices = n_wide * n_narrow
    me = wide * n_narrow + narrow
    kept, elements, points = basis.shape
    tiles = points // LANES
    total = float(elements * points * devices)

    def load(source, target, slot):
        return pltpu.make_async_copy(source, target, load_sem.at[slot])

    chunk = kept // 4
    loads = [
        load(basis_hbm.at[pl.ds(part * chunk, chunk)], basis.at[pl.ds(part * chunk, chunk)], part)
        for part in range(4)
    ]
    load_coeffs = load(coeffs_hbm, coeffs, 4)
    load_tables = [
        load(packed_hbm, packed, 5),
        load(coef_hbm, coef, 6),
        load(geom_hbm, geom, 7),
    ]
    load_orient = load(orient_hbm, orient, 8)
    load_pairs = load(pairs_hbm, pairs, 9)
    for copy in [load_coeffs] + loads + load_tables + [load_orient, load_pairs]:
        copy.start()

    messages = ((row_out, row_in), (pair_out, pair_in))

    def peer(step):
        if devices & (devices - 1):
            other = lax.rem(me + step, devices)
        else:
            other = me
            for bit in range(devices.bit_length() - 1):
                if step >> bit & 1:
                    other = other + (1 - 2 * lax.rem(me // 2**bit, 2)) * 2**bit
        return (other // n_narrow, lax.rem(other, n_narrow))

    def each_peer(act):
        if devices <= 64:
            for step in range(devices - 1, 0, -1):
                act(peer(step))
        else:

            def body(step, carry):
                other = lax.rem(me + step, devices)
                act((other // n_narrow, lax.rem(other, n_narrow)))
                return carry

            lax.fori_loop(1, devices, body, 0)

    barrier = pltpu.get_barrier_semaphore()

    def greet(where):
        pl.semaphore_signal(barrier, inc=1, device_id=where, device_id_type=MESH)

    inbox[...] = jnp.zeros_like(inbox)
    each_peer(greet)

    lane = lax.broadcasted_iota(jnp.int32, (elements, LANES), 1)
    line = lax.broadcasted_iota(jnp.int32, (elements, LANES), 0)
    low_half = lane < FACE
    half = lane // FACE
    mid = (lane // NP) % NP
    fast = lane % NP
    row_y = (line // EZ) % EY
    row_z = line % EZ
    at_y = (mid == 0) | (mid == NP - 1)
    at_z = (fast == 0) | (fast == NP - 1)

    pick_y = (mid % 2) * FACE + half * (FACE - NP) + fast
    pick_z = (mid % 2) * FACE + fast * NP + half * (NP - 1)
    source_tile = mid // 2

    def make_index():
        load_orient.wait()
        orient_pad[...] = jnp.zeros_like(orient_pad)
        orient_pad[pl.ds(0, 6), pl.ds(0, elements)] = orient[...]
        codes = jnp.transpose(orient_pad[...])[:elements]
        code = [jnp.broadcast_to(codes[:, f : f + 1], (elements, LANES)) for f in range(6)]
        code_x = jnp.where(low_half, code[0], code[1])
        index[2 * tiles] = rotated(mid, fast, code_x) + jnp.where(low_half, FACE, 0)
        code_y = jnp.where(mid == 0, code[2], code[3])
        code_z = jnp.where(fast == 0, code[4], code[5])
        for tile in range(tiles):
            first_pos = 2 * tile + half
            index[tile] = rotated(first_pos, fast, code_y) + jnp.where(mid == 0, FACE, 0)
            index[tiles + tile] = rotated(first_pos, mid, code_z) + jnp.where(fast == 0, FACE, 0)

    def tile_of(values, tile):
        return values[:, tile * LANES : (tile + 1) * LANES]

    def swap(values):
        return pltpu.roll(values, FACE, axis=1)

    def along_x(parts, way):
        swapped = [swap(part) for part in parts]
        outs = []
        for out_tile in range(tiles):
            acc = None
            for in_tile in range(tiles):
                at = ((way * tiles + out_tile) * tiles + in_tile) * 2
                term = (
                    coef[pl.ds(at, 1), :] * parts[in_tile]
                    + coef[pl.ds(at + 1, 1), :] * swapped[in_tile]
                )
                acc = term if acc is None else acc + term
            outs.append(acc)
        return outs

    def split(values):
        upper = values.astype(jnp.bfloat16)
        return upper, (values - upper.astype(jnp.float32)).astype(jnp.bfloat16)

    def product(left, right):
        return jnp.dot(left, right, preferred_element_type=jnp.float32)

    def local(parts):
        stacked = jnp.concatenate(split(jnp.concatenate(parts, axis=0)), axis=1)
        ahead = packed[pl.ds(0, LANES), :]
        ahead_rest = packed[pl.ds(LANES, LANES), :]
        grads = product(stacked, jnp.concatenate([ahead, ahead], axis=0)) + product(
            stacked, jnp.concatenate([ahead_rest, ahead_rest], axis=0)
        )
        geom_y = jnp.concatenate([geom[1, :, pl.ds(t * LANES, LANES)] for t in range(tiles)], axis=0)
        geom_z = jnp.concatenate([geom[2, :, pl.ds(t * LANES, LANES)] for t in range(tiles)], axis=0)
        flux = jnp.concatenate([grads[:, :LANES] * geom_y, grads[:, LANES:] * geom_z], axis=1)
        flux, flux_rest = split(flux)
        behind = packed[pl.ds(2 * LANES, 2 * LANES), :]
        back = product(flux, behind) + product(flux_rest, behind)
        back = back[:, :LANES] + back[:, LANES:]
        grad_x = along_x(parts, 0)
        flux_x = [grad_x[t] * geom[0, :, pl.ds(t * LANES, LANES)] for t in range(tiles)]
        back_x = along_x(flux_x, 1)
        return [
            back[t * elements : (t + 1) * elements]
            + back_x[t]
            + geom[3, :, pl.ds(t * LANES, LANES)] * parts[t]
            for t in range(tiles)
        ]

    def faces(parts, pick):
        found = take_lanes(parts[0], pick)
        for tile in range(1, tiles):
            found = jnp.where(source_tile == tile, take_lanes(parts[tile], pick), found)
        return found

    has = (narrow > 0, narrow < n_narrow - 1, wide > 0, wide < n_wide - 1)
    where_to = ((wide, narrow - 1), (wide, narrow + 1), (wide - 1, narrow), (wide + 1, narrow))

    def face_copy(step, side):
        return pltpu.make_async_remote_copy(
            src_ref=outbox.at[step, side],
            dst_ref=inbox.at[step, side ^ 1],
            send_sem=halo_send.at[0],
            recv_sem=halo_recv.at[step, side // 2],
            device_id=where_to[side],
            device_id_type=MESH,
        )

    def await_faces(step, axis):
        low, high = has[2 * axis], has[2 * axis + 1]
        for count, here in ((2, low & high), (1, low ^ high)):

            @pl.when(here)
            def _():
                span = inbox.at[step, pl.ds(2 * axis, count)]
                pltpu.make_async_copy(span, span, halo_recv.at[step, axis]).wait()

    def await_sent():
        sides = sum(side.astype(jnp.int32) for side in has)
        for count in range(1, 5):

            @pl.when(sides == count)
            def _():
                span = outbox.at[:, pl.ds(0, count)]
                pltpu.make_async_copy(span, span, halo_send.at[0]).wait()

    def operate(parts, step, ready, beside=lambda: None):
        result = local(parts)
        def send_faces(sides):
            for side in sides:

                @pl.when(has[side])
                def _():
                    face_copy(step, side).start()

        found_z = faces(result, pick_z)
        face_z[...] = found_z
        outbox[step, 2] = face_z[pl.ds(0, EX * EY, stride=EZ), :]
        outbox[step, 3] = face_z[pl.ds(EZ - 1, EX * EY, stride=EZ), :]
        ready()
        send_faces((2, 3))
        found_y = faces(result, pick_y)
        face_y[...] = found_y
        for ex in range(EX):
            outbox[step, 0, pl.ds(ex * EZ, EZ), :] = face_y[pl.ds(ex * EY * EZ, EZ), :]
            outbox[step, 1, pl.ds(ex * EZ, EZ), :] = face_y[pl.ds(ex * EY * EZ + (EY - 1) * EZ, EZ), :]
        send_faces((0, 1))

        if step == 0:
            make_index()

        face_x = jnp.where(low_half, result[0], result[tiles - 1])
        width = EY * EZ
        blank = jnp.zeros((width, LANES), jnp.float32)
        in_x = jnp.where(
            low_half,
            jnp.concatenate([face_x[width:], blank], axis=0),
            jnp.concatenate([blank, face_x[: elements - width]], axis=0),
        )
        in_y = jnp.where(
            low_half, pltpu.roll(found_y, elements - EZ, axis=0), pltpu.roll(found_y, EZ, axis=0)
        )
        in_z = jnp.where(
            low_half, pltpu.roll(found_z, elements - 1, axis=0), pltpu.roll(found_z, 1, axis=0)
        )
        got_x = take_lanes(in_x, index[2 * tiles])
        result[0] = result[0] + jnp.where(low_half, got_x, 0.0)
        result[tiles - 1] = result[tiles - 1] + jnp.where(low_half, 0.0, got_x)

        beside()

        await_faces(step, 0)
        for ex in range(EX):
            halo_y[pl.ds(ex * EY * EZ, EZ), :] = inbox[step, 0, pl.ds(ex * EZ, EZ), :]
            halo_y[pl.ds(ex * EY * EZ + (EY - 1) * EZ, EZ), :] = inbox[step, 1, pl.ds(ex * EZ, EZ), :]
        edge_y = row_y == jnp.where(low_half, EY - 1, 0)
        in_y = jnp.where(edge_y, halo_y[...], in_y)
        for t in range(tiles):
            result[t] = result[t] + jnp.where(at_y, take_lanes(in_y, index[t]), 0.0)
            image[:, pl.ds(t * LANES, LANES)] = result[t]

        await_faces(step, 1)
        halo_z[pl.ds(0, EX * EY, stride=EZ), :] = inbox[step, 2]
        halo_z[pl.ds(EZ - 1, EX * EY, stride=EZ), :] = inbox[step, 3]
        edge_z = row_z == jnp.where(low_half, EZ - 1, 0)
        in_z = jnp.where(edge_z, halo_z[...], in_z)
        return [
            image[:, pl.ds(t * LANES, LANES)]
            + jnp.where(at_z, take_lanes(in_z, index[tiles + t]), 0.0)
            for t in range(tiles)
        ]

    def folded(values):
        acc = tile_of(values, 0)
        for tile in range(1, tiles):
            acc = acc + tile_of(values, tile)
        return jnp.sum(acc.reshape(elements // 8, 8, LANES), axis=0)

    def to_row(partials, begin=0):
        count = -(-len(partials) // 8) * 8
        rows = [jnp.sum(part, axis=0, keepdims=True) for part in partials]
        rows += [jnp.zeros((1, LANES), jnp.float32)] * (count - len(rows))
        block = jnp.concatenate(rows, axis=0)
        sums = jnp.sum(block, axis=1, keepdims=True)
        place = lax.broadcasted_iota(jnp.int32, (count, LANES), 0) + begin == lax.broadcasted_iota(
            jnp.int32, (count, LANES), 1
        )
        return jnp.sum(jnp.where(place, sums, 0.0), axis=0, keepdims=True)

    def all_sum(block, phase, beside):
        outgoing, incoming = messages[phase]
        outgoing[...] = block
        incoming[pl.ds(me, 1)] = block.reshape((1,) + block.shape)

        def send(where):
            pltpu.make_async_remote_copy(
                src_ref=outgoing,
                dst_ref=incoming.at[me],
                send_sem=row_send.at[phase],
                recv_sem=row_recv.at[phase],
                device_id=where,
                device_id_type=MESH,
            ).start()

        each_peer(send)
        result = beside()
        span = incoming.at[pl.ds(0, devices - 1)]
        pltpu.make_async_copy(span, span, row_recv.at[phase]).wait()
        return jnp.sum(incoming[...], axis=0), result

    def weight(row, at):
        return row[:, at : at + 1]

    start = None
    load_coeffs.wait()
    for part in range(4):
        loads[part].wait()
        for at in range(part * chunk, (part + 1) * chunk):
            term = coeffs[at] * basis[at]
            start = term if start is None else start + term
    for copy in load_tables:
        copy.wait()

    def greeted():
        pl.semaphore_wait(barrier, devices - 1)

    image_parts = operate([tile_of(start, t) for t in range(tiles)], 0, greeted)
    for t in range(tiles):
        image[:, pl.ds(t * LANES, LANES)] = image_parts[t]
    rows, listed = pair_rows(kept)
    fresh = 2 * kept + 3

    def gram():
        partials = []
        block = 4
        for left in range(0, kept, block):
            for right in range(left, kept, block):
                wanted = [
                    (one, two)
                    for one in range(left, left + block)
                    for two in range(max(right, one), right + block)
                ]

                def body(step, carry):
                    base = pl.multiple_of(step * 8, 8)
                    carry = list(carry)
                    for tile in range(tiles):
                        at = (pl.ds(base, 8), pl.ds(tile * LANES, LANES))
                        ones = [basis[(left + m,) + at] for m in range(block)]
                        twos = ones if left == right else [
                            basis[(right + m,) + at] for m in range(block)
                        ]
                        for spot, (one, two) in enumerate(wanted):
                            carry[spot] = carry[spot] + ones[one - left] * twos[two - right]
                    return tuple(carry)

                zero = jnp.zeros((8, LANES), jnp.float32)
                partials += list(
                    lax.fori_loop(0, elements // 8, body, (zero,) * len(wanted))
                )
        gram_rows = []
        for begin in range(0, rows * LANES, LANES):
            lo = max(begin, fresh)
            here = partials[lo - fresh : begin + LANES - fresh]
            row = to_row(here, lo - begin) if here else jnp.zeros((1, LANES), jnp.float32)
            gram_rows.append(row)
        return gram_rows

    row = to_row([folded(basis[at] * image[...]) for at in range(kept)])
    sums, gram_part = all_sum(row, 0, gram)
    proj_one = sums / total
    acc = image[...]
    for at in range(kept):
        acc = acc - weight(proj_one, at) * basis[at]
    first[...] = acc

    with_first = []

    def project_first():
        with_first.extend(
            [folded(basis[at] * first[...]) for at in range(kept)]
            + [folded(first[...] * first[...])]
        )

    image_parts = operate(
        [first[:, pl.ds(t * LANES, LANES)] for t in range(tiles)], 1, lambda: None, project_first
    )
    for t in range(tiles):
        image[:, pl.ds(t * LANES, LANES)] = image_parts[t]
    row = to_row(
        [folded(basis[at] * image[...]) for at in range(kept)]
        + [folded(first[...] * image[...]), folded(image[...] * image[...])]
        + with_first
    )
    block = jnp.concatenate([gram_part[0] + row] + gram_part[1:], axis=0)
    sums, _ = all_sum(block, 1, load_pairs.wait)
    sums = sums / total
    along = sums[0:1]
    norm_one = jnp.sqrt(weight(along, fresh - 1) + epsilon)
    scale_one = 1.0 / norm_one
    proj_two = along * scale_one
    self_two = weight(along, kept) * scale_one * scale_one

    spot = lax.broadcasted_iota(jnp.int32, (8, LANES), 1)
    factor = jnp.broadcast_to(along, (8, LANES))
    factor = jnp.where(spot < kept, -factor, 0.0)
    factor = jnp.where(spot == kept, -self_two, factor)
    factor = jnp.where(spot == kept + 1, 1.0, factor)
    square = jnp.zeros((1, LANES), jnp.float32)
    for at in range(rows):
        left = jnp.broadcast_to(pairs[pl.ds(at, 1), :], (8, LANES))
        right = jnp.broadcast_to(pairs[pl.ds(rows + at, 1), :], (8, LANES))
        product = take_lanes(factor, left) * take_lanes(factor, right)
        product = jnp.where(left == right, product, 2.0 * product)
        used = spot + at * LANES < len(listed)
        square = square + jnp.where(used, product * sums[at : at + 1], 0.0)[0:1]
    square = jnp.maximum(jnp.sum(square, axis=1, keepdims=True), 0.0) * (scale_one * scale_one)
    norm_two = jnp.sqrt(square + epsilon)

    acc = image[...] - (self_two * first[...])
    for at in range(kept):
        acc = acc - weight(along, at) * basis[at]
    out[0] = first[...] * scale_one
    out[1] = acc * (scale_one / norm_two)

    spot = lax.broadcasted_iota(jnp.int32, (1, LANES), 1)
    row_first = jnp.where(spot < kept, proj_one, jnp.where(spot == kept, norm_one, 0.0))
    row_second = jnp.where(spot < kept, proj_two, jnp.where(spot == kept, self_two, norm_two))
    hess[pl.ds(0, 1), :] = row_first[:, : kept + 2]
    hess[pl.ds(1, 1), :] = row_second[:, : kept + 2]

    await_sent()
    for phase in range(2):
        span = messages[phase][1].at[pl.ds(0, devices - 1)]
        pltpu.make_async_copy(span, span, row_send.at[phase]).wait()


def on_device(n_wide, n_narrow, old_basis, restart_coeffs, geometry, orientation):
    kept, elements, points = old_basis.shape
    tiles = points // LANES
    devices = n_wide * n_narrow
    packed, coef = tables()
    rows, listed = pair_rows(kept)
    pairs = np.zeros((2 * rows, LANES), np.int32)
    for at, (left, right) in enumerate(listed):
        pairs[at // LANES, at % LANES] = left
        pairs[rows + at // LANES, at % LANES] = right
    pairs = jnp.asarray(pairs)
    anywhere = pl.BlockSpec(memory_space=pl.ANY)
    vmem = pl.BlockSpec(memory_space=pltpu.VMEM)
    f32 = jnp.float32
    border = EX * EY
    shapes = ((2, elements, points), (2, kept + 2))
    held = pl.pallas_call(
        functools.partial(kernel, n_wide, n_narrow),
        out_shape=tuple(pltpu.VMEM(shape, f32) for shape in shapes),
        in_specs=[anywhere] * 7,
        out_specs=(vmem, vmem),
        scratch_shapes=[
            pltpu.SMEM(restart_coeffs.shape, f32),
            pltpu.VMEM(old_basis.shape, f32),
            pltpu.VMEM(geometry.shape, f32),
            pltpu.VMEM(orientation.shape, jnp.int32),
            pltpu.VMEM(packed.shape, jnp.bfloat16),
            pltpu.VMEM(coef.shape, f32),
            pltpu.VMEM((2 * tiles + 1, elements, LANES), jnp.int32),
            pltpu.VMEM((8, LANES), jnp.int32),
            pltpu.VMEM((elements, points), f32),
            pltpu.VMEM((elements, points), f32),
            pltpu.VMEM((elements, LANES), f32),
            pltpu.VMEM((elements, LANES), f32),
            pltpu.VMEM((elements, LANES), f32),
            pltpu.VMEM((elements, LANES), f32),
            pltpu.VMEM((2, 4, border, LANES), f32),
            pltpu.VMEM((2, 4, border, LANES), f32),
            pltpu.VMEM(pairs.shape, jnp.int32),
            pltpu.VMEM((1, LANES), f32),
            pltpu.VMEM((devices, 1, LANES), f32),
            pltpu.VMEM((rows, LANES), f32),
            pltpu.VMEM((devices, rows, LANES), f32),
            pltpu.SemaphoreType.DMA((10,)),
            pltpu.SemaphoreType.DMA((1,)),
            pltpu.SemaphoreType.DMA((2, 2)),
            pltpu.SemaphoreType.DMA((2,)),
            pltpu.SemaphoreType.DMA((2,)),
        ],
        compiler_params=pltpu.CompilerParams(collective_id=0, has_side_effects=True),
        name="arnoldi",
    )(restart_coeffs, old_basis, geometry, orientation, packed, coef, pairs)
    return held


def solution(mesh):
    in_specs = (
        P(None, ("wide", "narrow"), None),
        P(),
        P(None, ("wide", "narrow"), None),
        P(None, ("wide", "narrow")),
    )
    out_specs = (P(None, ("wide", "narrow"), None), P())
    return jax.shard_map(
        functools.partial(on_device, mesh.shape["wide"], mesh.shape["narrow"]),
        mesh=mesh,
        in_specs=in_specs,
        out_specs=out_specs,
        check_vma=False,
    )
```

```python
import functools

import jax
import jax.numpy as jnp
import numpy as np
from jax import lax
from jax.experimental import pallas as pl
from jax.experimental.pallas import tpu as pltpu
from jax.sharding import PartitionSpec as P

NP = 8
EX = 4
EY = 4
EZ = 4
LANES = 128
FACE = NP * NP
MESH = pl.DeviceIdType.MESH
highest = lax.Precision.HIGHEST
epsilon = 1e-06


def legendre_columns(nodes, degree):
    columns = [nodes * 0.0 + 1.0, nodes * 1.0]
    for order in range(2, degree + 1):
        columns.append(
            ((2 * order - 1) * nodes * columns[order - 1] - (order - 1) * columns[order - 2])
            / order
        )
    return columns


def gll_derivative(extent):
    degree = extent - 1
    nodes = np.cos(np.pi * np.arange(extent) / degree)
    for sweep in range(100):
        columns = legendre_columns(nodes, degree)
        nodes = nodes - (nodes * columns[degree] - columns[degree - 1]) / (extent * columns[degree])
    gll_nodes = nodes[::-1] * 1.0
    values = legendre_columns(gll_nodes, degree)[degree]
    matrix = np.zeros((extent, extent))
    for row_idx in range(extent):
        for col_idx in range(extent):
            if row_idx != col_idx:
                matrix[row_idx, col_idx] = values[row_idx] / (
                    values[col_idx] * (gll_nodes[row_idx] - gll_nodes[col_idx])
                )
    matrix[0, 0] = -degree * (degree + 1) / 4.0
    matrix[extent - 1, extent - 1] = degree * (degree + 1) / 4.0
    return matrix


def halves(table):
    table = np.asarray(table, np.float32)
    upper = table.astype(jnp.bfloat16).astype(np.float32)
    return upper, table - upper


def tables():
    matrix = gll_derivative(NP)
    identity = np.eye(NP)
    pair = np.eye(2)
    along_y = np.kron(pair, np.kron(matrix, identity))
    along_z = np.kron(pair, np.kron(identity, matrix))
    forward = np.concatenate([along_y.T, along_z.T], axis=1)
    backward = np.concatenate([along_y, along_z], axis=0)
    tiles = NP // 2
    coef = np.zeros((2, tiles, tiles, 2, LANES))
    for way, table in enumerate((matrix, matrix.T)):
        for out_tile in range(tiles):
            for in_tile in range(tiles):
                for half in range(2):
                    lanes = slice(half * FACE, (half + 1) * FACE)
                    row = 2 * out_tile + half
                    coef[way, out_tile, in_tile, 0, lanes] = table[row, 2 * in_tile + half]
                    coef[way, out_tile, in_tile, 1, lanes] = table[row, 2 * in_tile + 1 - half]
    ahead, ahead_rest = halves(forward)
    back, back_rest = halves(backward)
    packed = np.concatenate([ahead, ahead_rest, np.concatenate([back, back_rest], axis=1)], axis=0)
    return (
        jnp.asarray(packed, jnp.bfloat16),
        jnp.asarray(coef.reshape(-1, LANES), jnp.float32),
    )


def pair_rows(kept):
    count = kept + 2
    listed = [(at, kept + 1) for at in range(count)]
    listed += [(at, kept) for at in range(kept + 1)]
    block = 4
    for left in range(0, kept, block):
        for right in range(left, kept, block):
            for one in range(left, left + block):
                for two in range(max(right, one), right + block):
                    listed.append((one, two))
    return -(-len(listed) // LANES), listed


def take_lanes(values, index):
    return jnp.take_along_axis(values, index, axis=1, mode="promise_in_bounds")


def rotated(row, col, code):
    row = row ^ (7 * (code & 1))
    col = col ^ (7 * ((code >> 1) & 1))
    return jnp.where((code & 4) != 0, col * NP + row, row * NP + col)


def kernel(
    n_wide,
    n_narrow,
    coeffs_hbm,
    basis_hbm,
    geom_hbm,
    orient_hbm,
    packed_hbm,
    coef_hbm,
    pairs_hbm,
    out,
    hess,
    coeffs,
    basis,
    geom,
    orient,
    packed,
    coef,
    index,
    orient_pad,
    image,
    first,
    face_y,
    face_z,
    halo_y,
    halo_z,
    outbox,
    inbox,
    pairs,
    row_out,
    row_in,
    pair_out,
    pair_in,
    far_code,
    far_index,
    far_tile,
    far_basis,
    lined,
    load_sem,
    halo_send,
    halo_recv,
    row_send,
    row_recv,
    all_ready,
):
    wide = lax.axis_index("wide")
    narrow = lax.axis_index("narrow")
    devices = n_wide * n_narrow
    me = wide * n_narrow + narrow
    kept, elements, points = basis.shape
    tiles = points // LANES
    total = float(elements * points * devices)

    def load(source, target, slot):
        return pltpu.make_async_copy(source, target, load_sem.at[slot])

    chunk = kept // 4
    loads = [
        load(basis_hbm.at[pl.ds(part * chunk, chunk)], basis.at[pl.ds(part * chunk, chunk)], part)
        for part in range(4)
    ]
    load_coeffs = load(coeffs_hbm, coeffs, 4)
    load_tables = [
        load(packed_hbm, packed, 5),
        load(coef_hbm, coef, 6),
        load(geom_hbm, geom, 7),
    ]
    load_orient = load(orient_hbm, orient, 8)
    load_pairs = load(pairs_hbm, pairs, 9)
    for copy in [load_coeffs] + loads + load_tables + [load_orient, load_pairs]:
        copy.start()

    messages = ((row_out, row_in), (pair_out, pair_in))

    def peer(step):
        if devices & (devices - 1):
            other = lax.rem(me + step, devices)
        else:
            other = me
            for bit in range(devices.bit_length() - 1):
                if step >> bit & 1:
                    other = other + (1 - 2 * lax.rem(me // 2**bit, 2)) * 2**bit
        return (other // n_narrow, lax.rem(other, n_narrow))

    def each_peer(act):
        if devices <= 64:
            for step in range(devices - 1, 0, -1):
                act(peer(step))
        else:

            def body(step, carry):
                other = lax.rem(me + step, devices)
                act((other // n_narrow, lax.rem(other, n_narrow)))
                return carry

            lax.fori_loop(1, devices, body, 0)

    barrier = pltpu.get_barrier_semaphore()

    inner = 1
    while n_wide % (2 * inner) == 0 and 4 * inner * inner <= n_wide:
        inner = 2 * inner
    plane = inner * n_narrow
    planes = n_wide // inner
    layer = wide // inner
    column = lax.rem(wide, inner)
    in_plane = column * n_narrow + narrow

    def in_steps(count, act):
        if count <= 64:
            for step in range(count - 1, 0, -1):
                act(step)
        else:

            def body(step, carry):
                act(step)
                return carry

            lax.fori_loop(1, count, body, 0)

    def signal(semaphore, where):
        pl.semaphore_signal(semaphore, inc=1, device_id=where, device_id_type=MESH)

    def to_planes(semaphore):
        def act(step):
            other = lax.rem(layer + step, planes)
            signal(semaphore, (other * inner + column, narrow))

        in_steps(planes, act)

    def to_plane(semaphore):
        def act(step):
            other = lax.rem(in_plane + step, plane)
            signal(semaphore, (layer * inner + other // n_narrow, lax.rem(other, n_narrow)))

        in_steps(plane, act)

    greetings = plane + planes - 2
    crossing = ()
    if 1 < inner < n_wide:
        crossing = (
            ((column == 0) & (wide > 0), -1),
            ((column == inner - 1) & (wide < n_wide - 1), 1),
        )
    for there, shift in crossing:
        greetings = greetings + there.astype(jnp.int32)

    def greet():
        to_planes(barrier)
        for there, shift in crossing:

            @pl.when(there)
            def _():
                signal(barrier, (wide + shift, narrow))

        to_plane(barrier)

    inbox[...] = jnp.zeros_like(inbox)
    greet()

    lane = lax.broadcasted_iota(jnp.int32, (elements, LANES), 1)
    line = lax.broadcasted_iota(jnp.int32, (elements, LANES), 0)
    low_half = lane < FACE
    border = EX * EY
    low_border = low_half[:border]
    half = lane // FACE
    mid = (lane // NP) % NP
    fast = lane % NP
    row_y = (line // EZ) % EY
    row_z = line % EZ
    at_y = (mid == 0) | (mid == NP - 1)
    at_z = (fast == 0) | (fast == NP - 1)

    pick_y = (mid % 2) * FACE + half * (FACE - NP) + fast
    pick_z = (mid % 2) * FACE + fast * NP + half * (NP - 1)
    source_tile = mid // 2

    def make_index():
        load_orient.wait()
        orient_pad[...] = jnp.zeros_like(orient_pad)
        orient_pad[pl.ds(0, 6), pl.ds(0, elements)] = orient[...]
        codes = jnp.transpose(orient_pad[...])[:elements]
        code = [jnp.broadcast_to(codes[:, f : f + 1], (elements, LANES)) for f in range(6)]
        code_x = jnp.where(low_half, code[0], code[1])
        index[2 * tiles] = rotated(mid, fast, code_x) + jnp.where(low_half, FACE, 0)
        code_y = jnp.where(mid == 0, code[2], code[3])
        code_z = jnp.where(fast == 0, code[4], code[5])
        for tile in range(tiles):
            first_pos = 2 * tile + half
            index[tile] = rotated(first_pos, fast, code_y) + jnp.where(mid == 0, FACE, 0)
            index[tiles + tile] = rotated(first_pos, mid, code_z) + jnp.where(fast == 0, FACE, 0)
        far_code[...] = jnp.where(low_half, code[5], code[4])
        found = jnp.where(
            low_border,
            far_code[pl.ds(EZ - 1, border, stride=EZ), :],
            far_code[pl.ds(0, border, stride=EZ), :],
        )
        turned = (found & 4) != 0
        along_a = jnp.where(turned, fast[:border], mid[:border]) ^ (7 * (found & 1))
        along_b = jnp.where(turned, mid[:border], fast[:border]) ^ (7 * ((found >> 1) & 1))
        far_index[...] = (along_a % 2) * FACE + along_b * NP + jnp.where(low_border, NP - 1, 0)
        far_tile[...] = along_a // 2

    def meeting(ref, *at):
        found = None
        for t in range(tiles):
            lanes = pl.ds(t * LANES, LANES)
            spare = (sum(at) % 2) * tiles + t
            lined[spare] = ref[at + (slice(None), lanes)]
            last = lined[spare, pl.ds(EZ - 1, border, stride=EZ), :]
            begin = lined[spare, pl.ds(0, border, stride=EZ), :]
            got = take_lanes(jnp.where(fast[:border] == NP - 1, last, begin), far_index[...])
            found = got if found is None else jnp.where(far_tile[...] == t, got, found)
        return found

    def tile_of(values, tile):
        return values[:, tile * LANES : (tile + 1) * LANES]

    def swap(values):
        return pltpu.roll(values, FACE, axis=1)

    def along_x(parts, way):
        swapped = [swap(part) for part in parts]
        outs = []
        for out_tile in range(tiles):
            acc = None
            for in_tile in range(tiles):
                at = ((way * tiles + out_tile) * tiles + in_tile) * 2
                term = (
                    coef[pl.ds(at, 1), :] * parts[in_tile]
                    + coef[pl.ds(at + 1, 1), :] * swapped[in_tile]
                )
                acc = term if acc is None else acc + term
            outs.append(acc)
        return outs

    def split(values):
        upper = values.astype(jnp.bfloat16)
        return upper, (values - upper.astype(jnp.float32)).astype(jnp.bfloat16)

    def product(left, right):
        return jnp.dot(left, right, preferred_element_type=jnp.float32)

    def local(parts):
        stacked = jnp.concatenate(split(jnp.concatenate(parts, axis=0)), axis=1)
        ahead = packed[pl.ds(0, LANES), :]
        ahead_rest = packed[pl.ds(LANES, LANES), :]
        grads = product(stacked, jnp.concatenate([ahead, ahead], axis=0)) + product(
            stacked, jnp.concatenate([ahead_rest, ahead_rest], axis=0)
        )
        geom_y = jnp.concatenate([geom[1, :, pl.ds(t * LANES, LANES)] for t in range(tiles)], axis=0)
        geom_z = jnp.concatenate([geom[2, :, pl.ds(t * LANES, LANES)] for t in range(tiles)], axis=0)
        flux = jnp.concatenate([grads[:, :LANES] * geom_y, grads[:, LANES:] * geom_z], axis=1)
        flux, flux_rest = split(flux)
        behind = packed[pl.ds(2 * LANES, 2 * LANES), :]
        back = product(flux, behind) + product(flux_rest, behind)
        back = back[:, :LANES] + back[:, LANES:]
        grad_x = along_x(parts, 0)
        flux_x = [grad_x[t] * geom[0, :, pl.ds(t * LANES, LANES)] for t in range(tiles)]
        back_x = along_x(flux_x, 1)
        return [
            back[t * elements : (t + 1) * elements]
            + back_x[t]
            + geom[3, :, pl.ds(t * LANES, LANES)] * parts[t]
            for t in range(tiles)
        ]

    def faces(parts, pick):
        found = take_lanes(parts[0], pick)
        for tile in range(1, tiles):
            found = jnp.where(source_tile == tile, take_lanes(parts[tile], pick), found)
        return found

    has = (narrow > 0, narrow < n_narrow - 1, wide > 0, wide < n_wide - 1)
    where_to = ((wide, narrow - 1), (wide, narrow + 1), (wide - 1, narrow), (wide + 1, narrow))

    def face_copy(step, side):
        return pltpu.make_async_remote_copy(
            src_ref=outbox.at[step, side],
            dst_ref=inbox.at[step, side ^ 1],
            send_sem=halo_send.at[0],
            recv_sem=halo_recv.at[step, side // 2],
            device_id=where_to[side],
            device_id_type=MESH,
        )

    def await_faces(step, axis):
        low, high = has[2 * axis], has[2 * axis + 1]
        for count, here in ((2, low & high), (1, low ^ high)):

            @pl.when(here)
            def _():
                span = inbox.at[step, pl.ds(2 * axis, count)]
                pltpu.make_async_copy(span, span, halo_recv.at[step, axis]).wait()

    def await_sent():
        sides = sum(side.astype(jnp.int32) for side in has)
        for count in range(1, 5):

            @pl.when(sides == count)
            def _():
                span = outbox.at[:, pl.ds(0, count)]
                pltpu.make_async_copy(span, span, halo_send.at[0]).wait()

    def operate(parts, step, ready, beside=lambda: None):
        result = local(parts)
        def send_faces(sides):
            for side in sides:

                @pl.when(has[side])
                def _():
                    face_copy(step, side).start()

        found_z = faces(result, pick_z)
        face_z[...] = found_z
        outbox[step, 2] = face_z[pl.ds(0, EX * EY, stride=EZ), :]
        outbox[step, 3] = face_z[pl.ds(EZ - 1, EX * EY, stride=EZ), :]
        ready()
        send_faces((2, 3))
        found_y = faces(result, pick_y)
        face_y[...] = found_y
        for ex in range(EX):
            outbox[step, 0, pl.ds(ex * EZ, EZ), :] = face_y[pl.ds(ex * EY * EZ, EZ), :]
            outbox[step, 1, pl.ds(ex * EZ, EZ), :] = face_y[pl.ds(ex * EY * EZ + (EY - 1) * EZ, EZ), :]
        send_faces((0, 1))

        if step == 0:
            make_index()

        face_x = jnp.where(low_half, result[0], result[tiles - 1])
        width = EY * EZ
        blank = jnp.zeros((width, LANES), jnp.float32)
        in_x = jnp.where(
            low_half,
            jnp.concatenate([face_x[width:], blank], axis=0),
            jnp.concatenate([blank, face_x[: elements - width]], axis=0),
        )
        in_y = jnp.where(
            low_half, pltpu.roll(found_y, elements - EZ, axis=0), pltpu.roll(found_y, EZ, axis=0)
        )
        in_z = jnp.where(
            low_half, pltpu.roll(found_z, elements - 1, axis=0), pltpu.roll(found_z, 1, axis=0)
        )
        got_x = take_lanes(in_x, index[2 * tiles])
        result[0] = result[0] + jnp.where(low_half, got_x, 0.0)
        result[tiles - 1] = result[tiles - 1] + jnp.where(low_half, 0.0, got_x)

        edge_z = row_z == jnp.where(low_half, EZ - 1, 0)
        in_z = jnp.where(edge_z, 0.0, in_z)
        for t in range(tiles):
            result[t] = result[t] + jnp.where(at_z, take_lanes(in_z, index[tiles + t]), 0.0)

        beside()

        await_faces(step, 0)
        for ex in range(EX):
            halo_y[pl.ds(ex * EY * EZ, EZ), :] = inbox[step, 0, pl.ds(ex * EZ, EZ), :]
            halo_y[pl.ds(ex * EY * EZ + (EY - 1) * EZ, EZ), :] = inbox[step, 1, pl.ds(ex * EZ, EZ), :]
        edge_y = row_y == jnp.where(low_half, EY - 1, 0)
        in_y = jnp.where(edge_y, halo_y[...], in_y)
        for t in range(tiles):
            result[t] = result[t] + jnp.where(at_y, take_lanes(in_y, index[t]), 0.0)
            image[:, pl.ds(t * LANES, LANES)] = result[t]

    def far_faces(step):
        await_faces(step, 1)
        return jnp.where(low_border, inbox[step, 3], inbox[step, 2])

    def add_far(step):
        halo_z[pl.ds(0, border, stride=EZ), :] = inbox[step, 2]
        halo_z[pl.ds(EZ - 1, border, stride=EZ), :] = inbox[step, 3]
        edge_z = row_z == jnp.where(low_half, EZ - 1, 0)
        in_z = jnp.where(edge_z, halo_z[...], 0.0)
        for t in range(tiles):
            got = jnp.where(at_z, take_lanes(in_z, index[tiles + t]), 0.0)
            image[:, pl.ds(t * LANES, LANES)] = image[:, pl.ds(t * LANES, LANES)] + got

    def stacked_rows(values):
        return jnp.sum(values.reshape(border // 8, 8, LANES), axis=0)

    def folded(values):
        acc = tile_of(values, 0)
        for tile in range(1, tiles):
            acc = acc + tile_of(values, tile)
        return jnp.sum(acc.reshape(elements // 8, 8, LANES), axis=0)

    def to_row(partials, begin=0):
        count = -(-len(partials) // 8) * 8
        rows = [jnp.sum(part, axis=0, keepdims=True) for part in partials]
        rows += [jnp.zeros((1, LANES), jnp.float32)] * (count - len(rows))
        block = jnp.concatenate(rows, axis=0)
        sums = jnp.sum(block, axis=1, keepdims=True)
        place = lax.broadcasted_iota(jnp.int32, (count, LANES), 0) + begin == lax.broadcasted_iota(
            jnp.int32, (count, LANES), 1
        )
        return jnp.sum(jnp.where(place, sums, 0.0), axis=0, keepdims=True)

    def all_sum(block, phase, beside):
        outgoing, incoming = messages[phase]
        outgoing[...] = block
        incoming[pl.ds(me, 1)] = block.reshape((1,) + block.shape)

        def send(where):
            pltpu.make_async_remote_copy(
                src_ref=outgoing,
                dst_ref=incoming.at[me],
                send_sem=row_send.at[phase],
                recv_sem=row_recv.at[phase],
                device_id=where,
                device_id_type=MESH,
            ).start()

        if phase == 0:
            pl.semaphore_wait(all_ready, planes - 1)
        each_peer(send)
        result = beside()
        span = incoming.at[pl.ds(0, devices - 1)]
        pltpu.make_async_copy(span, span, row_recv.at[phase]).wait()
        return jnp.sum(incoming[...], axis=0), result

    def weight(row, at):
        return row[:, at : at + 1]

    start = None
    load_coeffs.wait()
    for part in range(4):
        loads[part].wait()
        for at in range(part * chunk, (part + 1) * chunk):
            term = coeffs[at] * basis[at]
            start = term if start is None else start + term
    for copy in load_tables:
        copy.wait()

    def greeted():
        pl.semaphore_wait(barrier, greetings)
        to_planes(all_ready)

    def meet_basis():
        for at in range(kept):
            far_basis[at] = meeting(basis, at)

    operate([tile_of(start, t) for t in range(tiles)], 0, greeted, meet_basis)
    rows, listed = pair_rows(kept)
    fresh = 2 * kept + 3

    def gram():
        partials = []
        block = 4
        for left in range(0, kept, block):
            for right in range(left, kept, block):
                wanted = [
                    (one, two)
                    for one in range(left, left + block)
                    for two in range(max(right, one), right + block)
                ]

                def body(step, carry):
                    base = pl.multiple_of(step * 8, 8)
                    carry = list(carry)
                    for tile in range(tiles):
                        at = (pl.ds(base, 8), pl.ds(tile * LANES, LANES))
                        ones = [basis[(left + m,) + at] for m in range(block)]
                        twos = ones if left == right else [
                            basis[(right + m,) + at] for m in range(block)
                        ]
                        for spot, (one, two) in enumerate(wanted):
                            carry[spot] = carry[spot] + ones[one - left] * twos[two - right]
                    return tuple(carry)

                zero = jnp.zeros((8, LANES), jnp.float32)
                partials += list(
                    lax.fori_loop(0, elements // 8, body, (zero,) * len(wanted))
                )
        gram_rows = []
        for begin in range(0, rows * LANES, LANES):
            lo = max(begin, fresh)
            here = partials[lo - fresh : begin + LANES - fresh]
            row = to_row(here, lo - begin) if here else jnp.zeros((1, LANES), jnp.float32)
            gram_rows.append(row)
        return gram_rows

    near = [folded(basis[at] * image[...]) for at in range(kept)]
    far = far_faces(0)
    row = to_row([near[at] + stacked_rows(far_basis[at] * far) for at in range(kept)])

    def between():
        add_far(0)
        return gram()

    sums, gram_part = all_sum(row, 0, between)
    proj_one = sums / total
    acc = image[...]
    for at in range(kept):
        acc = acc - weight(proj_one, at) * basis[at]
    first[...] = acc

    with_first = []

    def project_first():
        with_first.append(meeting(first))
        with_first.append(
            to_row(
                [folded(basis[at] * first[...]) for at in range(kept)]
                + [folded(first[...] * first[...])],
                kept + 2,
            )
        )

    operate(
        [first[:, pl.ds(t * LANES, LANES)] for t in range(tiles)], 1, lambda: None, project_first
    )
    near = [folded(basis[at] * image[...]) for at in range(kept)]
    near += [folded(first[...] * image[...]), folded(image[...] * image[...])]
    far_first, row_first = with_first
    far_image = 2.0 * meeting(image)
    far = far_faces(1)
    beyond = [stacked_rows(far_basis[at] * far) for at in range(kept)]
    beyond += [stacked_rows(far_first * far), stacked_rows((far_image + far) * far)]
    row = to_row([one + two for one, two in zip(near, beyond)])
    block = jnp.concatenate([gram_part[0] + row_first + row] + gram_part[1:], axis=0)

    def before_end():
        add_far(1)
        load_pairs.wait()

    sums, _ = all_sum(block, 1, before_end)
    sums = sums / total
    along = sums[0:1]
    norm_one = jnp.sqrt(weight(along, fresh - 1) + epsilon)
    scale_one = 1.0 / norm_one
    proj_two = along * scale_one
    self_two = weight(along, kept) * scale_one * scale_one

    spot = lax.broadcasted_iota(jnp.int32, (8, LANES), 1)
    factor = jnp.broadcast_to(along, (8, LANES))
    factor = jnp.where(spot < kept, -factor, 0.0)
    factor = jnp.where(spot == kept, -self_two, factor)
    factor = jnp.where(spot == kept + 1, 1.0, factor)
    square = jnp.zeros((1, LANES), jnp.float32)
    for at in range(rows):
        left = jnp.broadcast_to(pairs[pl.ds(at, 1), :], (8, LANES))
        right = jnp.broadcast_to(pairs[pl.ds(rows + at, 1), :], (8, LANES))
        product = take_lanes(factor, left) * take_lanes(factor, right)
        product = jnp.where(left == right, product, 2.0 * product)
        used = spot + at * LANES < len(listed)
        square = square + jnp.where(used, product * sums[at : at + 1], 0.0)[0:1]
    square = jnp.maximum(jnp.sum(square, axis=1, keepdims=True), 0.0) * (scale_one * scale_one)
    norm_two = jnp.sqrt(square + epsilon)

    acc = image[...] - (self_two * first[...])
    for at in range(kept):
        acc = acc - weight(along, at) * basis[at]
    out[0] = first[...] * scale_one
    out[1] = acc * (scale_one / norm_two)

    spot = lax.broadcasted_iota(jnp.int32, (1, LANES), 1)
    row_first = jnp.where(spot < kept, proj_one, jnp.where(spot == kept, norm_one, 0.0))
    row_second = jnp.where(spot < kept, proj_two, jnp.where(spot == kept, self_two, norm_two))
    hess[pl.ds(0, 1), :] = row_first[:, : kept + 2]
    hess[pl.ds(1, 1), :] = row_second[:, : kept + 2]

    await_sent()
    for phase in range(2):
        span = messages[phase][1].at[pl.ds(0, devices - 1)]
        pltpu.make_async_copy(span, span, row_send.at[phase]).wait()


def settle(vectors, matrix, out, hess, sem):
    copies = [
        pltpu.make_async_copy(vectors, out, sem.at[0]),
        pltpu.make_async_copy(matrix, hess, sem.at[1]),
    ]
    for copy in copies:
        copy.start()
    for copy in copies:
        copy.wait()


def on_device(n_wide, n_narrow, old_basis, restart_coeffs, geometry, orientation):
    kept, elements, points = old_basis.shape
    tiles = points // LANES
    devices = n_wide * n_narrow
    packed, coef = tables()
    rows, listed = pair_rows(kept)
    pairs = np.zeros((2 * rows, LANES), np.int32)
    for at, (left, right) in enumerate(listed):
        pairs[at // LANES, at % LANES] = left
        pairs[rows + at // LANES, at % LANES] = right
    pairs = jnp.asarray(pairs)
    anywhere = pl.BlockSpec(memory_space=pl.ANY)
    vmem = pl.BlockSpec(memory_space=pltpu.VMEM)
    f32 = jnp.float32
    border = EX * EY
    shapes = ((2, elements, points), (2, kept + 2))
    held = pl.pallas_call(
        functools.partial(kernel, n_wide, n_narrow),
        out_shape=tuple(pltpu.VMEM(shape, f32) for shape in shapes),
        in_specs=[anywhere] * 7,
        out_specs=(vmem, vmem),
        scratch_shapes=[
            pltpu.SMEM(restart_coeffs.shape, f32),
            pltpu.VMEM(old_basis.shape, f32),
            pltpu.VMEM(geometry.shape, f32),
            pltpu.VMEM(orientation.shape, jnp.int32),
            pltpu.VMEM(packed.shape, jnp.bfloat16),
            pltpu.VMEM(coef.shape, f32),
            pltpu.VMEM((2 * tiles + 1, elements, LANES), jnp.int32),
            pltpu.VMEM((8, LANES), jnp.int32),
            pltpu.VMEM((elements, points), f32),
            pltpu.VMEM((elements, points), f32),
            pltpu.VMEM((elements, LANES), f32),
            pltpu.VMEM((elements, LANES), f32),
            pltpu.VMEM((elements, LANES), f32),
            pltpu.VMEM((elements, LANES), f32),
            pltpu.VMEM((2, 4, border, LANES), f32),
            pltpu.VMEM((2, 4, border, LANES), f32),
            pltpu.VMEM(pairs.shape, jnp.int32),
            pltpu.VMEM((1, LANES), f32),
            pltpu.VMEM((devices, 1, LANES), f32),
            pltpu.VMEM((rows, LANES), f32),
            pltpu.VMEM((devices, rows, LANES), f32),
            pltpu.VMEM((elements, LANES), jnp.int32),
            pltpu.VMEM((border, LANES), jnp.int32),
            pltpu.VMEM((border, LANES), jnp.int32),
            pltpu.VMEM((kept, border, LANES), f32),
            pltpu.VMEM((2 * tiles, elements, LANES), f32),
            pltpu.SemaphoreType.DMA((10,)),
            pltpu.SemaphoreType.DMA((1,)),
            pltpu.SemaphoreType.DMA((2, 2)),
            pltpu.SemaphoreType.DMA((2,)),
            pltpu.SemaphoreType.DMA((2,)),
            pltpu.SemaphoreType.REGULAR,
        ],
        compiler_params=pltpu.CompilerParams(collective_id=0, has_side_effects=True),
        name="arnoldi",
    )(restart_coeffs, old_basis, geometry, orientation, packed, coef, pairs)
    return pl.pallas_call(
        settle,
        out_shape=tuple(jax.ShapeDtypeStruct(shape, f32) for shape in shapes),
        in_specs=[vmem, vmem],
        out_specs=(anywhere, anywhere),
        scratch_shapes=[pltpu.SemaphoreType.DMA((2,))],
        name="settle",
    )(*[pltpu.with_memory_space_constraint(each, pltpu.VMEM) for each in held])


def solution(mesh):
    in_specs = (
        P(None, ("wide", "narrow"), None),
        P(),
        P(None, ("wide", "narrow"), None),
        P(None, ("wide", "narrow")),
    )
    out_specs = (P(None, ("wide", "narrow"), None), P())
    return jax.shard_map(
        functools.partial(on_device, mesh.shape["wide"], mesh.shape["narrow"]),
        mesh=mesh,
        in_specs=in_specs,
        out_specs=out_specs,
        check_vma=False,
    )
```

```python
import functools

import jax
import jax.numpy as jnp
import numpy as np
from jax import lax
from jax.experimental import pallas as pl
from jax.experimental.pallas import tpu as pltpu
from jax.sharding import PartitionSpec as P

NP = 8
EX = 4
EY = 4
EZ = 4
LANES = 128
FACE = NP * NP
MESH = pl.DeviceIdType.MESH
highest = lax.Precision.HIGHEST
epsilon = 1e-06


def legendre_columns(nodes, degree):
    columns = [nodes * 0.0 + 1.0, nodes * 1.0]
    for order in range(2, degree + 1):
        columns.append(
            ((2 * order - 1) * nodes * columns[order - 1] - (order - 1) * columns[order - 2])
            / order
        )
    return columns


def gll_derivative(extent):
    degree = extent - 1
    nodes = np.cos(np.pi * np.arange(extent) / degree)
    for sweep in range(100):
        columns = legendre_columns(nodes, degree)
        nodes = nodes - (nodes * columns[degree] - columns[degree - 1]) / (extent * columns[degree])
    gll_nodes = nodes[::-1] * 1.0
    values = legendre_columns(gll_nodes, degree)[degree]
    matrix = np.zeros((extent, extent))
    for row_idx in range(extent):
        for col_idx in range(extent):
            if row_idx != col_idx:
                matrix[row_idx, col_idx] = values[row_idx] / (
                    values[col_idx] * (gll_nodes[row_idx] - gll_nodes[col_idx])
                )
    matrix[0, 0] = -degree * (degree + 1) / 4.0
    matrix[extent - 1, extent - 1] = degree * (degree + 1) / 4.0
    return matrix


def halves(table):
    table = np.asarray(table, np.float32)
    upper = table.astype(jnp.bfloat16).astype(np.float32)
    return upper, table - upper


def tables():
    matrix = gll_derivative(NP)
    identity = np.eye(NP)
    pair = np.eye(2)
    along_y = np.kron(pair, np.kron(matrix, identity))
    along_z = np.kron(pair, np.kron(identity, matrix))
    forward = np.concatenate([along_y.T, along_z.T], axis=1)
    backward = np.concatenate([along_y, along_z], axis=0)
    tiles = NP // 2
    coef = np.zeros((2, tiles, tiles, 2, LANES))
    for way, table in enumerate((matrix, matrix.T)):
        for out_tile in range(tiles):
            for in_tile in range(tiles):
                for half in range(2):
                    lanes = slice(half * FACE, (half + 1) * FACE)
                    row = 2 * out_tile + half
                    coef[way, out_tile, in_tile, 0, lanes] = table[row, 2 * in_tile + half]
                    coef[way, out_tile, in_tile, 1, lanes] = table[row, 2 * in_tile + 1 - half]
    ahead, ahead_rest = halves(forward)
    back, back_rest = halves(backward)
    packed = np.concatenate([ahead, ahead_rest, np.concatenate([back, back_rest], axis=1)], axis=0)
    return (
        jnp.asarray(packed, jnp.bfloat16),
        jnp.asarray(coef.reshape(-1, LANES), jnp.float32),
    )


def take_lanes(values, index):
    return jnp.take_along_axis(values, index, axis=1, mode="promise_in_bounds")


def rotated(row, col, code):
    row = row ^ (7 * (code & 1))
    col = col ^ (7 * ((code >> 1) & 1))
    return jnp.where((code & 4) != 0, col * NP + row, row * NP + col)


def kernel(
    n_wide,
    n_narrow,
    coeffs_hbm,
    basis_hbm,
    geom_hbm,
    orient_hbm,
    packed_hbm,
    coef_hbm,
    out,
    hess,
    coeffs,
    basis,
    geom,
    orient,
    packed,
    coef,
    index,
    orient_pad,
    image,
    first,
    face_y,
    face_z,
    halo_y,
    halo_z,
    outbox,
    inbox,
    row_out,
    row_in,
    pair_out,
    pair_in,
    far_code,
    far_index,
    far_tile,
    far_basis,
    lined,
    load_sem,
    halo_send,
    halo_recv,
    row_send,
    row_recv,
    all_ready,
):
    wide = lax.axis_index("wide")
    narrow = lax.axis_index("narrow")
    devices = n_wide * n_narrow
    me = wide * n_narrow + narrow
    kept, elements, points = basis.shape
    tiles = points // LANES
    total = float(elements * points * devices)

    def load(source, target, slot):
        return pltpu.make_async_copy(source, target, load_sem.at[slot])

    chunk = kept // 4
    loads = [
        load(basis_hbm.at[pl.ds(part * chunk, chunk)], basis.at[pl.ds(part * chunk, chunk)], part)
        for part in range(4)
    ]
    load_coeffs = load(coeffs_hbm, coeffs, 4)
    load_tables = [
        load(packed_hbm, packed, 5),
        load(coef_hbm, coef, 6),
    ]
    load_geom = load(geom_hbm, geom, 7)
    load_orient = load(orient_hbm, orient, 8)
    for copy in [load_coeffs] + loads + load_tables + [load_geom, load_orient]:
        copy.start()

    messages = ((row_out, row_in), (pair_out, pair_in))

    def peer(step):
        if devices & (devices - 1):
            other = lax.rem(me + step, devices)
        else:
            other = me
            for bit in range(devices.bit_length() - 1):
                if step >> bit & 1:
                    other = other + (1 - 2 * lax.rem(me // 2**bit, 2)) * 2**bit
        return (other // n_narrow, lax.rem(other, n_narrow))

    def each_peer(act, ascending):
        if devices > 64:

            def body(step, carry):
                other = lax.rem(me + step, devices)
                act((other // n_narrow, lax.rem(other, n_narrow)))
                return carry

            lax.fori_loop(1, devices, body, 0)
        elif ascending:
            for at in range(devices - 1):
                other = at + (me <= at).astype(jnp.int32)
                act((other // n_narrow, lax.rem(other, n_narrow)))
        else:
            for step in range(devices - 1, 0, -1):
                act(peer(step))

    barrier = pltpu.get_barrier_semaphore()

    inner = 1
    while n_wide % (2 * inner) == 0 and 4 * inner * inner <= n_wide:
        inner = 2 * inner
    plane = inner * n_narrow
    planes = n_wide // inner
    layer = wide // inner
    column = lax.rem(wide, inner)
    in_plane = column * n_narrow + narrow

    def in_steps(count, act):
        if count <= 64:
            for step in range(count - 1, 0, -1):
                act(step)
        else:

            def body(step, carry):
                act(step)
                return carry

            lax.fori_loop(1, count, body, 0)

    def signal(semaphore, where):
        pl.semaphore_signal(semaphore, inc=1, device_id=where, device_id_type=MESH)

    def to_planes(semaphore):
        def act(step):
            other = lax.rem(layer + step, planes)
            signal(semaphore, (other * inner + column, narrow))

        in_steps(planes, act)

    def to_plane(semaphore):
        def act(step):
            other = lax.rem(in_plane + step, plane)
            signal(semaphore, (layer * inner + other // n_narrow, lax.rem(other, n_narrow)))

        in_steps(plane, act)

    greetings = plane + planes - 2
    crossing = ()
    if 1 < inner < n_wide:
        crossing = (
            ((column == 0) & (wide > 0), -1),
            ((column == inner - 1) & (wide < n_wide - 1), 1),
        )
    for there, shift in crossing:
        greetings = greetings + there.astype(jnp.int32)

    def greet():
        to_planes(barrier)
        for there, shift in crossing:

            @pl.when(there)
            def _():
                signal(barrier, (wide + shift, narrow))

        to_plane(barrier)

    inbox[...] = jnp.zeros_like(inbox)
    greet()

    lane = lax.broadcasted_iota(jnp.int32, (elements, LANES), 1)
    line = lax.broadcasted_iota(jnp.int32, (elements, LANES), 0)
    low_half = lane < FACE
    border = EX * EY
    low_border = low_half[:border]
    half = lane // FACE
    mid = (lane // NP) % NP
    fast = lane % NP
    row_y = (line // EZ) % EY
    row_z = line % EZ
    at_y = (mid == 0) | (mid == NP - 1)
    at_z = (fast == 0) | (fast == NP - 1)

    pick_y = (mid % 2) * FACE + half * (FACE - NP) + fast
    pick_z = (mid % 2) * FACE + fast * NP + half * (NP - 1)
    source_tile = mid // 2

    def make_index():
        load_orient.wait()
        orient_pad[...] = jnp.zeros_like(orient_pad)
        orient_pad[pl.ds(0, 6), pl.ds(0, elements)] = orient[...]
        codes = jnp.transpose(orient_pad[...])[:elements]
        code = [jnp.broadcast_to(codes[:, f : f + 1], (elements, LANES)) for f in range(6)]
        code_x = jnp.where(low_half, code[0], code[1])
        index[2 * tiles] = rotated(mid, fast, code_x) + jnp.where(low_half, FACE, 0)
        code_y = jnp.where(mid == 0, code[2], code[3])
        code_z = jnp.where(fast == 0, code[4], code[5])
        for tile in range(tiles):
            first_pos = 2 * tile + half
            index[tile] = rotated(first_pos, fast, code_y) + jnp.where(mid == 0, FACE, 0)
            index[tiles + tile] = rotated(first_pos, mid, code_z) + jnp.where(fast == 0, FACE, 0)
        far_code[...] = jnp.where(low_half, code[5], code[4])
        found = jnp.where(
            low_border,
            far_code[pl.ds(EZ - 1, border, stride=EZ), :],
            far_code[pl.ds(0, border, stride=EZ), :],
        )
        turned = (found & 4) != 0
        along_a = jnp.where(turned, fast[:border], mid[:border]) ^ (7 * (found & 1))
        along_b = jnp.where(turned, mid[:border], fast[:border]) ^ (7 * ((found >> 1) & 1))
        far_index[...] = (along_a % 2) * FACE + along_b * NP + jnp.where(low_border, NP - 1, 0)
        far_tile[...] = along_a // 2

    def meeting(ref, *at):
        found = None
        for t in range(tiles):
            lanes = pl.ds(t * LANES, LANES)
            spare = (sum(at) % 2) * tiles + t
            lined[spare] = ref[at + (slice(None), lanes)]
            last = lined[spare, pl.ds(EZ - 1, border, stride=EZ), :]
            begin = lined[spare, pl.ds(0, border, stride=EZ), :]
            got = take_lanes(jnp.where(fast[:border] == NP - 1, last, begin), far_index[...])
            found = got if found is None else jnp.where(far_tile[...] == t, got, found)
        return found

    def tile_of(values, tile):
        return values[:, tile * LANES : (tile + 1) * LANES]

    def swap(values):
        return pltpu.roll(values, FACE, axis=1)

    def along_x(parts, way):
        swapped = [swap(part) for part in parts]
        outs = []
        for out_tile in range(tiles):
            acc = None
            for in_tile in range(tiles):
                at = ((way * tiles + out_tile) * tiles + in_tile) * 2
                term = (
                    coef[pl.ds(at, 1), :] * parts[in_tile]
                    + coef[pl.ds(at + 1, 1), :] * swapped[in_tile]
                )
                acc = term if acc is None else acc + term
            outs.append(acc)
        return outs

    def split(values):
        upper = values.astype(jnp.bfloat16)
        return upper, (values - upper.astype(jnp.float32)).astype(jnp.bfloat16)

    def product(left, right):
        return jnp.dot(left, right, preferred_element_type=jnp.float32)

    def local(parts, geometry_here=lambda: None):
        stacked = jnp.concatenate(split(jnp.concatenate(parts, axis=0)), axis=1)
        ahead = packed[pl.ds(0, LANES), :]
        ahead_rest = packed[pl.ds(LANES, LANES), :]
        grads = product(stacked, jnp.concatenate([ahead, ahead], axis=0)) + product(
            stacked, jnp.concatenate([ahead_rest, ahead_rest], axis=0)
        )
        grad_x = along_x(parts, 0)
        geometry_here()
        geom_y = jnp.concatenate([geom[1, :, pl.ds(t * LANES, LANES)] for t in range(tiles)], axis=0)
        geom_z = jnp.concatenate([geom[2, :, pl.ds(t * LANES, LANES)] for t in range(tiles)], axis=0)
        flux = jnp.concatenate([grads[:, :LANES] * geom_y, grads[:, LANES:] * geom_z], axis=1)
        flux, flux_rest = split(flux)
        behind = packed[pl.ds(2 * LANES, 2 * LANES), :]
        back = product(flux, behind) + product(flux_rest, behind)
        back = back[:, :LANES] + back[:, LANES:]
        flux_x = [grad_x[t] * geom[0, :, pl.ds(t * LANES, LANES)] for t in range(tiles)]
        back_x = along_x(flux_x, 1)
        return [
            back[t * elements : (t + 1) * elements]
            + back_x[t]
            + geom[3, :, pl.ds(t * LANES, LANES)] * parts[t]
            for t in range(tiles)
        ]

    def faces(parts, pick):
        found = take_lanes(parts[0], pick)
        for tile in range(1, tiles):
            found = jnp.where(source_tile == tile, take_lanes(parts[tile], pick), found)
        return found

    has = (narrow > 0, narrow < n_narrow - 1, wide > 0, wide < n_wide - 1)
    where_to = ((wide, narrow - 1), (wide, narrow + 1), (wide - 1, narrow), (wide + 1, narrow))

    def face_copy(step, side):
        return pltpu.make_async_remote_copy(
            src_ref=outbox.at[step, side],
            dst_ref=inbox.at[step, side ^ 1],
            send_sem=halo_send.at[0],
            recv_sem=halo_recv.at[step, side // 2],
            device_id=where_to[side],
            device_id_type=MESH,
        )

    def await_faces(step, axis):
        low, high = has[2 * axis], has[2 * axis + 1]
        for count, here in ((2, low & high), (1, low ^ high)):

            @pl.when(here)
            def _():
                span = inbox.at[step, pl.ds(2 * axis, count)]
                pltpu.make_async_copy(span, span, halo_recv.at[step, axis]).wait()

    def await_sent():
        sides = sum(side.astype(jnp.int32) for side in has)
        for count in range(1, 5):

            @pl.when(sides == count)
            def _():
                span = outbox.at[:, pl.ds(0, count)]
                pltpu.make_async_copy(span, span, halo_send.at[0]).wait()

    def operate(parts, step, ready, beside=lambda: None):
        result = local(parts, load_geom.wait if step == 0 else lambda: None)
        def send_faces(sides):
            for side in sides:

                @pl.when(has[side])
                def _():
                    face_copy(step, side).start()

        found_z = faces(result, pick_z)
        face_z[...] = found_z
        outbox[step, 2] = face_z[pl.ds(0, EX * EY, stride=EZ), :]
        outbox[step, 3] = face_z[pl.ds(EZ - 1, EX * EY, stride=EZ), :]
        ready()
        send_faces((2, 3))
        found_y = faces(result, pick_y)
        face_y[...] = found_y
        for ex in range(EX):
            outbox[step, 0, pl.ds(ex * EZ, EZ), :] = face_y[pl.ds(ex * EY * EZ, EZ), :]
            outbox[step, 1, pl.ds(ex * EZ, EZ), :] = face_y[pl.ds(ex * EY * EZ + (EY - 1) * EZ, EZ), :]
        send_faces((0, 1))

        if step == 0:
            make_index()

        face_x = jnp.where(low_half, result[0], result[tiles - 1])
        width = EY * EZ
        blank = jnp.zeros((width, LANES), jnp.float32)
        in_x = jnp.where(
            low_half,
            jnp.concatenate([face_x[width:], blank], axis=0),
            jnp.concatenate([blank, face_x[: elements - width]], axis=0),
        )
        in_y = jnp.where(
            low_half, pltpu.roll(found_y, elements - EZ, axis=0), pltpu.roll(found_y, EZ, axis=0)
        )
        in_z = jnp.where(
            low_half, pltpu.roll(found_z, elements - 1, axis=0), pltpu.roll(found_z, 1, axis=0)
        )
        got_x = take_lanes(in_x, index[2 * tiles])
        result[0] = result[0] + jnp.where(low_half, got_x, 0.0)
        result[tiles - 1] = result[tiles - 1] + jnp.where(low_half, 0.0, got_x)

        edge_z = row_z == jnp.where(low_half, EZ - 1, 0)
        in_z = jnp.where(edge_z, 0.0, in_z)
        for t in range(tiles):
            result[t] = result[t] + jnp.where(at_z, take_lanes(in_z, index[tiles + t]), 0.0)

        beside()

        await_faces(step, 0)
        for ex in range(EX):
            halo_y[pl.ds(ex * EY * EZ, EZ), :] = inbox[step, 0, pl.ds(ex * EZ, EZ), :]
            halo_y[pl.ds(ex * EY * EZ + (EY - 1) * EZ, EZ), :] = inbox[step, 1, pl.ds(ex * EZ, EZ), :]
        edge_y = row_y == jnp.where(low_half, EY - 1, 0)
        in_y = jnp.where(edge_y, halo_y[...], in_y)
        for t in range(tiles):
            result[t] = result[t] + jnp.where(at_y, take_lanes(in_y, index[t]), 0.0)
            image[:, pl.ds(t * LANES, LANES)] = result[t]

    def far_faces(step):
        await_faces(step, 1)
        return jnp.where(low_border, inbox[step, 3], inbox[step, 2])

    def add_far(step):
        halo_z[pl.ds(0, border, stride=EZ), :] = inbox[step, 2]
        halo_z[pl.ds(EZ - 1, border, stride=EZ), :] = inbox[step, 3]
        edge_z = row_z == jnp.where(low_half, EZ - 1, 0)
        in_z = jnp.where(edge_z, halo_z[...], 0.0)
        for t in range(tiles):
            got = jnp.where(at_z, take_lanes(in_z, index[tiles + t]), 0.0)
            image[:, pl.ds(t * LANES, LANES)] = image[:, pl.ds(t * LANES, LANES)] + got

    def stacked_rows(values):
        return jnp.sum(values.reshape(border // 8, 8, LANES), axis=0)

    def folded(values):
        acc = tile_of(values, 0)
        for tile in range(1, tiles):
            acc = acc + tile_of(values, tile)
        return jnp.sum(acc.reshape(elements // 8, 8, LANES), axis=0)

    def sums_of(partials):
        count = -(-len(partials) // 8) * 8
        rows = [jnp.sum(part, axis=0, keepdims=True) for part in partials]
        rows += [jnp.zeros((1, LANES), jnp.float32)] * (count - len(rows))
        return jnp.sum(jnp.concatenate(rows, axis=0), axis=1, keepdims=True)

    def put(sums, place_of):
        shape = (sums.shape[0], LANES)
        place = place_of(lax.broadcasted_iota(jnp.int32, shape, 0))
        here = place == lax.broadcasted_iota(jnp.int32, shape, 1)
        return jnp.sum(jnp.where(here, sums, 0.0), axis=0, keepdims=True)

    def to_row(partials, begin=0):
        return put(sums_of(partials), lambda at: at + begin)

    def all_sum(block, phase, beside):
        outgoing, incoming = messages[phase]
        outgoing[...] = block
        incoming[pl.ds(me, 1)] = block.reshape((1,) + block.shape)

        def send(where):
            pltpu.make_async_remote_copy(
                src_ref=outgoing,
                dst_ref=incoming.at[me],
                send_sem=row_send.at[phase],
                recv_sem=row_recv.at[phase],
                device_id=where,
                device_id_type=MESH,
            ).start()

        if phase == 0:
            pl.semaphore_wait(all_ready, planes - 1)
        each_peer(send, phase == 1)
        result = beside()
        span = incoming.at[pl.ds(0, devices - 1)]
        pltpu.make_async_copy(span, span, row_recv.at[phase]).wait()
        if devices > 64:
            return jnp.sum(incoming[...], axis=0), result
        found = [incoming[at] for at in range(devices)]
        while len(found) > 1:
            half_way = len(found) // 2
            odd = found[2 * half_way :]
            found = [found[at] + found[half_way + at] for at in range(half_way)] + odd
        return found[0], result

    def weight(row, at):
        spot = jnp.full((8, LANES), at, jnp.int32)
        return take_lanes(jnp.broadcast_to(row, (8, LANES)), spot)

    pieces = [
        (pl.ds(base, 8), pl.ds(tile * LANES, LANES))
        for base in range(0, elements, 8)
        for tile in range(tiles)
    ]

    def against_basis(ref):
        found = [None] * kept
        for at in pieces:
            piece = ref[at]
            for one in range(kept):
                term = basis[(one,) + at] * piece
                found[one] = term if found[one] is None else found[one] + term
        return found

    def against(left, right):
        found = None
        for at in pieces:
            term = left[at] * right[at]
            found = term if found is None else found + term
        return found

    def less_basis(piece, parts, at):
        for one in range(kept):
            piece = piece - parts[one] * basis[(one,) + at]
        return piece

    start = None
    load_coeffs.wait()
    for part in range(4):
        loads[part].wait()
        for at in range(part * chunk, (part + 1) * chunk):
            term = coeffs[at] * basis[at]
            start = term if start is None else start + term
    for copy in load_tables:
        copy.wait()

    def greeted():
        pl.semaphore_wait(barrier, greetings)
        to_planes(all_ready)

    def meet_basis():
        for at in range(kept):
            far_basis[at] = meeting(basis, at)

    operate([tile_of(start, t) for t in range(tiles)], 0, greeted, meet_basis)
    block = 4
    a_line = LANES // kept
    lines = kept // a_line

    def gram():
        found = [jnp.zeros((1, LANES), jnp.float32)] * lines
        for left in range(0, kept, block):
            for right in range(left, kept, block):

                def body(step, carry):
                    base = pl.multiple_of(step * 8, 8)
                    carry = list(carry)
                    for tile in range(tiles):
                        at = (pl.ds(base, 8), pl.ds(tile * LANES, LANES))
                        ones = [basis[(left + m,) + at] for m in range(block)]
                        twos = ones if left == right else [
                            basis[(right + m,) + at] for m in range(block)
                        ]
                        for spot in range(block * block):
                            carry[spot] = carry[spot] + ones[spot // block] * twos[spot % block]
                    return tuple(carry)

                zero = jnp.zeros((8, LANES), jnp.float32)
                partials = lax.fori_loop(0, elements // 8, body, (zero,) * (block * block))
                begin = (left % a_line) * kept + right
                row = put(
                    sums_of(partials), lambda at: begin + (at // block) * kept + at % block
                )
                line_at = left // a_line
                found[line_at] = found[line_at] + (row if left == right else 2.0 * row)
        return found

    near = against_basis(image)
    far = far_faces(0)
    row = to_row([near[at] + stacked_rows(far_basis[at] * far) for at in range(kept)])

    def between():
        add_far(0)
        return gram()

    sums, gram_lines = all_sum(row, 0, between)
    proj_one = sums / total
    parts = [weight(proj_one, at) for at in range(kept)]
    for at in pieces:
        first[at] = less_basis(image[at], parts, at)

    with_first = []

    def project_first():
        with_first.append(meeting(first))
        with_first.append(
            to_row(
                against_basis(first) + [against(first, first)],
                kept + 2,
            )
        )

    operate(
        [first[:, pl.ds(t * LANES, LANES)] for t in range(tiles)], 1, lambda: None, project_first
    )
    near = against_basis(image) + [against(first, image), against(image, image)]
    far_first, row_first = with_first
    far_image = 2.0 * meeting(image)
    far = far_faces(1)
    beyond = [stacked_rows(far_basis[at] * far) for at in range(kept)]
    beyond += [stacked_rows(far_first * far), stacked_rows((far_image + far) * far)]
    row = to_row([one + two for one, two in zip(near, beyond)])
    block = jnp.concatenate([row_first + row] + gram_lines, axis=0)

    sums, _ = all_sum(block, 1, lambda: add_far(1))
    sums = sums / total
    along = sums[0:1]
    spot = lax.broadcasted_iota(jnp.int32, (1, LANES), 1)
    inside = spot < kept
    parts = [weight(along, at) for at in range(kept)]
    cross, whole, one = [weight(along, at) for at in (kept, kept + 1, 2 * kept + 2)]
    with_one = pltpu.roll(jnp.broadcast_to(along, (8, LANES)), LANES - kept - 2, axis=1)[0:1]
    pick = lax.broadcasted_iota(jnp.int32, (a_line, LANES), 0) * kept + (
        lax.broadcasted_iota(jnp.int32, (a_line, LANES), 1) % kept
    )
    spread = [
        take_lanes(jnp.broadcast_to(sums[1 + at : 2 + at], (a_line, LANES)), pick)
        for at in range(lines)
    ]
    found = [
        parts[at][0:1] * spread[at // a_line][at % a_line : at % a_line + 1] for at in range(kept)
    ]
    while len(found) > 1:
        found = [found[at] + found[at + 1] for at in range(0, len(found), 2)]
    along_in = jnp.where(inside, along, 0.0)
    terms = jnp.concatenate([along_in * (found[0] - 2.0 * along), along_in * with_one], axis=0)
    terms = jnp.sum(terms, axis=1, keepdims=True)

    norm_one = jnp.sqrt(one + epsilon)
    scale_one = 1.0 / norm_one
    self_two = cross * (scale_one * scale_one)
    for at in pieces:
        piece = first[at]
        out[(0,) + at] = piece * scale_one
        image[at] = less_basis(image[at] - self_two * piece, parts, at)

    square = whole + terms[0:1] + self_two * (2.0 * (terms[1:2] - cross) + self_two * one)
    square = jnp.maximum(square, 0.0) * (scale_one * scale_one)
    norm_two = jnp.sqrt(square + epsilon)
    scale_two = scale_one / norm_two
    for at in pieces:
        out[(1,) + at] = image[at] * scale_two

    norm_one, scale_one, self_two, norm_two = (
        each[0:1] for each in (norm_one, scale_one, self_two, norm_two)
    )
    row_first = jnp.where(inside, proj_one, jnp.where(spot == kept, norm_one, 0.0))
    row_second = jnp.where(
        inside, along * scale_one, jnp.where(spot == kept, self_two, norm_two)
    )
    hess[pl.ds(0, 1), :] = row_first[:, : kept + 2]
    hess[pl.ds(1, 1), :] = row_second[:, : kept + 2]

    await_sent()
    for phase in range(2):
        span = messages[phase][1].at[pl.ds(0, devices - 1)]
        pltpu.make_async_copy(span, span, row_send.at[phase]).wait()


def settle(vectors, matrix, out, hess, sem):
    copies = [
        pltpu.make_async_copy(vectors, out, sem.at[0]),
        pltpu.make_async_copy(matrix, hess, sem.at[1]),
    ]
    for copy in copies:
        copy.start()
    for copy in copies:
        copy.wait()


def on_device(n_wide, n_narrow, old_basis, restart_coeffs, geometry, orientation):
    kept, elements, points = old_basis.shape
    tiles = points // LANES
    devices = n_wide * n_narrow
    packed, coef = tables()
    rows = 1 + kept * kept // LANES
    anywhere = pl.BlockSpec(memory_space=pl.ANY)
    vmem = pl.BlockSpec(memory_space=pltpu.VMEM)
    f32 = jnp.float32
    border = EX * EY
    shapes = ((2, elements, points), (2, kept + 2))
    held = pl.pallas_call(
        functools.partial(kernel, n_wide, n_narrow),
        out_shape=tuple(pltpu.VMEM(shape, f32) for shape in shapes),
        in_specs=[anywhere] * 6,
        out_specs=(vmem, vmem),
        scratch_shapes=[
            pltpu.SMEM(restart_coeffs.shape, f32),
            pltpu.VMEM(old_basis.shape, f32),
            pltpu.VMEM(geometry.shape, f32),
            pltpu.VMEM(orientation.shape, jnp.int32),
            pltpu.VMEM(packed.shape, jnp.bfloat16),
            pltpu.VMEM(coef.shape, f32),
            pltpu.VMEM((2 * tiles + 1, elements, LANES), jnp.int32),
            pltpu.VMEM((8, LANES), jnp.int32),
            pltpu.VMEM((elements, points), f32),
            pltpu.VMEM((elements, points), f32),
            pltpu.VMEM((elements, LANES), f32),
            pltpu.VMEM((elements, LANES), f32),
            pltpu.VMEM((elements, LANES), f32),
            pltpu.VMEM((elements, LANES), f32),
            pltpu.VMEM((2, 4, border, LANES), f32),
            pltpu.VMEM((2, 4, border, LANES), f32),
            pltpu.VMEM((1, LANES), f32),
            pltpu.VMEM((devices, 1, LANES), f32),
            pltpu.VMEM((rows, LANES), f32),
            pltpu.VMEM((devices, rows, LANES), f32),
            pltpu.VMEM((elements, LANES), jnp.int32),
            pltpu.VMEM((border, LANES), jnp.int32),
            pltpu.VMEM((border, LANES), jnp.int32),
            pltpu.VMEM((kept, border, LANES), f32),
            pltpu.VMEM((2 * tiles, elements, LANES), f32),
            pltpu.SemaphoreType.DMA((9,)),
            pltpu.SemaphoreType.DMA((1,)),
            pltpu.SemaphoreType.DMA((2, 2)),
            pltpu.SemaphoreType.DMA((2,)),
            pltpu.SemaphoreType.DMA((2,)),
            pltpu.SemaphoreType.REGULAR,
        ],
        compiler_params=pltpu.CompilerParams(collective_id=0, has_side_effects=True),
        name="arnoldi",
    )(restart_coeffs, old_basis, geometry, orientation, packed, coef)
    return pl.pallas_call(
        settle,
        out_shape=tuple(jax.ShapeDtypeStruct(shape, f32) for shape in shapes),
        in_specs=[vmem, vmem],
        out_specs=(anywhere, anywhere),
        scratch_shapes=[pltpu.SemaphoreType.DMA((2,))],
        name="settle",
    )(*[pltpu.with_memory_space_constraint(each, pltpu.VMEM) for each in held])


def solution(mesh):
    in_specs = (
        P(None, ("wide", "narrow"), None),
        P(),
        P(None, ("wide", "narrow"), None),
        P(None, ("wide", "narrow")),
    )
    out_specs = (P(None, ("wide", "narrow"), None), P())
    return jax.shard_map(
        functools.partial(on_device, mesh.shape["wide"], mesh.shape["narrow"]),
        mesh=mesh,
        in_specs=in_specs,
        out_specs=out_specs,
        check_vma=False,
    )
```

```python
import functools

import jax
import jax.numpy as jnp
import numpy as np
from jax import lax
from jax.experimental import pallas as pl
from jax.experimental.pallas import tpu as pltpu
from jax.sharding import PartitionSpec as P

NP = 8
EX = 4
EY = 4
EZ = 4
LANES = 128
FACE = NP * NP
MESH = pl.DeviceIdType.MESH
highest = lax.Precision.HIGHEST
epsilon = 1e-06


def legendre_columns(nodes, degree):
    columns = [nodes * 0.0 + 1.0, nodes * 1.0]
    for order in range(2, degree + 1):
        columns.append(
            ((2 * order - 1) * nodes * columns[order - 1] - (order - 1) * columns[order - 2])
            / order
        )
    return columns


def gll_derivative(extent):
    degree = extent - 1
    nodes = np.cos(np.pi * np.arange(extent) / degree)
    for sweep in range(100):
        columns = legendre_columns(nodes, degree)
        nodes = nodes - (nodes * columns[degree] - columns[degree - 1]) / (extent * columns[degree])
    gll_nodes = nodes[::-1] * 1.0
    values = legendre_columns(gll_nodes, degree)[degree]
    matrix = np.zeros((extent, extent))
    for row_idx in range(extent):
        for col_idx in range(extent):
            if row_idx != col_idx:
                matrix[row_idx, col_idx] = values[row_idx] / (
                    values[col_idx] * (gll_nodes[row_idx] - gll_nodes[col_idx])
                )
    matrix[0, 0] = -degree * (degree + 1) / 4.0
    matrix[extent - 1, extent - 1] = degree * (degree + 1) / 4.0
    return matrix


def halves(table):
    table = np.asarray(table, np.float32)
    upper = table.astype(jnp.bfloat16).astype(np.float32)
    return upper, table - upper


def tables():
    matrix = gll_derivative(NP)
    identity = np.eye(NP)
    pair = np.eye(2)
    along_y = np.kron(pair, np.kron(matrix, identity))
    along_z = np.kron(pair, np.kron(identity, matrix))
    forward = np.concatenate([along_y.T, along_z.T], axis=1)
    backward = np.concatenate([along_y, along_z], axis=0)
    tiles = NP // 2
    coef = np.zeros((2, tiles, tiles, 2, LANES))
    for way, table in enumerate((matrix, matrix.T)):
        for out_tile in range(tiles):
            for in_tile in range(tiles):
                for half in range(2):
                    lanes = slice(half * FACE, (half + 1) * FACE)
                    row = 2 * out_tile + half
                    coef[way, out_tile, in_tile, 0, lanes] = table[row, 2 * in_tile + half]
                    coef[way, out_tile, in_tile, 1, lanes] = table[row, 2 * in_tile + 1 - half]
    ahead, ahead_rest = halves(forward)
    back, back_rest = halves(backward)
    packed = np.concatenate([ahead, ahead_rest, np.concatenate([back, back_rest], axis=1)], axis=0)
    return (
        jnp.asarray(packed, jnp.bfloat16),
        jnp.asarray(coef.reshape(-1, LANES), jnp.float32),
    )


def places():
    order = [0, EZ - 1] + list(range(1, EZ - 1))
    width = EX * EY
    return [
        (slot * width + at, at * EZ + layer) for slot, layer in enumerate(order) for at in range(width)
    ]


def take_lanes(values, index):
    return jnp.take_along_axis(values, index, axis=1, mode="promise_in_bounds")


def rotated(row, col, code):
    row = row ^ (7 * (code & 1))
    col = col ^ (7 * ((code >> 1) & 1))
    return jnp.where((code & 4) != 0, col * NP + row, row * NP + col)


def kernel(
    n_wide,
    n_narrow,
    coeffs_hbm,
    basis_hbm,
    geom_hbm,
    orient_hbm,
    packed_hbm,
    coef_hbm,
    out,
    hess,
    coeffs,
    basis,
    geom,
    orient,
    packed,
    coef,
    index,
    orient_pad,
    image,
    first,
    face_y,
    halo_y,
    outbox,
    inbox,
    row_out,
    row_in,
    pair_out,
    pair_in,
    far_index,
    far_tile,
    far_basis,
    load_sem,
    halo_recv,
    row_recv,
    all_ready,
    from_below,
):
    wide = lax.axis_index("wide")
    narrow = lax.axis_index("narrow")
    devices = n_wide * n_narrow
    me = wide * n_narrow + narrow
    kept, elements, points = basis.shape
    tiles = points // LANES
    total = float(elements * points * devices)

    def load(source, target, slot):
        return pltpu.make_async_copy(source, target, load_sem.at[slot])

    width = EX * EY
    edge = 2 * width

    def load_rows(source, target, begin, count, slot):
        copies = [
            load(source.at[:, pl.ds(there, 1)], target.at[:, pl.ds(here, 1)], slot)
            for here, there in places()[begin : begin + count]
        ]
        for copy in copies:
            copy.start()

    def await_rows(target, begin, count, slot):
        span = target.at[:, pl.ds(begin, count)]
        load(span, span, slot).wait()

    load_coeffs = load(coeffs_hbm, coeffs, 6)
    load_tables = [load(packed_hbm, packed, 7), load(coef_hbm, coef, 8)]
    load_orient = load(orient_hbm, orient, 9)
    load_coeffs.start()
    for copy in load_tables:
        copy.start()
    for slot in range(2):
        load_rows(basis_hbm, basis, slot * width, width, slot)
    messages = ((row_out, row_in), (pair_out, pair_in))

    def peer(step):
        if devices & (devices - 1):
            other = lax.rem(me + step, devices)
        else:
            other = me
            for bit in range(devices.bit_length() - 1):
                if step >> bit & 1:
                    other = other + (1 - 2 * lax.rem(me // 2**bit, 2)) * 2**bit
        return (other // n_narrow, lax.rem(other, n_narrow))

    def each_peer(act, ascending):
        if devices > 64:

            def body(step, carry):
                other = lax.rem(me + step, devices)
                act((other // n_narrow, lax.rem(other, n_narrow)))
                return carry

            lax.fori_loop(1, devices, body, 0)
        elif ascending:
            for at in range(devices - 1):
                other = at + (me <= at).astype(jnp.int32)
                act((other // n_narrow, lax.rem(other, n_narrow)))
        else:
            for step in range(devices - 1, 0, -1):
                act(peer(step))

    barrier = pltpu.get_barrier_semaphore()

    inner = 1
    while n_wide % (2 * inner) == 0 and 4 * inner * inner <= n_wide:
        inner = 2 * inner
    plane = inner * n_narrow
    planes = n_wide // inner
    layer = wide // inner
    column = lax.rem(wide, inner)
    in_plane = column * n_narrow + narrow

    def in_steps(count, act):
        if count <= 64:
            for step in range(count - 1, 0, -1):
                act(step)
        else:

            def body(step, carry):
                act(step)
                return carry

            lax.fori_loop(1, count, body, 0)

    def signal(semaphore, where):
        pl.semaphore_signal(semaphore, inc=1, device_id=where, device_id_type=MESH)

    def to_layer(semaphore, other, there):
        @pl.when(there)
        def _():
            signal(semaphore, (other * inner + column, narrow))

    def to_higher(semaphore):
        for step in range(planes - 1, 0, -1):
            to_layer(semaphore, layer + step, layer + step < planes)

    def to_lower(semaphore):
        for step in range(planes - 1, 0, -1):
            to_layer(semaphore, layer - step, layer >= step)

    def to_plane(semaphore):
        def act(step):
            other = lax.rem(in_plane + step, plane)
            signal(semaphore, (layer * inner + other // n_narrow, lax.rem(other, n_narrow)))

        in_steps(plane, act)

    below = layer > 0
    above = layer < planes - 1
    greetings = plane - 1 + layer + above.astype(jnp.int32)
    crossing = ()
    if 1 < inner < n_wide:
        crossing = (
            ((column == 0) & (wide > 0), -1),
            ((column == inner - 1) & (wide < n_wide - 1), 1),
        )
    for there, shift in crossing:
        greetings = greetings + there.astype(jnp.int32)

    def greet():
        to_layer(barrier, layer - 1, below)
        to_higher(barrier)
        for there, shift in crossing:

            @pl.when(there)
            def _():
                signal(barrier, (wide + shift, narrow))

        to_plane(barrier)

    inbox[...] = jnp.zeros_like(inbox)
    greet()
    load_rows(geom_hbm, geom, 0, edge, 4)
    for slot in range(2, EZ):
        load_rows(basis_hbm, basis, slot * width, width, slot)
    load_rows(geom_hbm, geom, edge, elements - edge, 5)
    load_orient.start()

    lane = lax.broadcasted_iota(jnp.int32, (elements, LANES), 1)
    line = lax.broadcasted_iota(jnp.int32, (elements, LANES), 0)
    low_half = lane < FACE
    border = width
    low_border = low_half[:border]
    half = lane // FACE
    mid = (lane // NP) % NP
    fast = lane % NP
    row_x = (line // EY) % EX
    row_y = line % EY
    at_y = (mid == 0) | (mid == NP - 1)
    at_z = (fast == 0) | (fast == NP - 1)

    pick_y = (mid % 2) * FACE + half * (FACE - NP) + fast
    pick_z = (mid % 2) * FACE + fast * NP + half * (NP - 1)
    source_tile = mid // 2

    def make_index():
        load_orient.wait()
        orient_pad[...] = jnp.zeros_like(orient_pad)
        orient_pad[pl.ds(0, 6), pl.ds(0, elements)] = orient[...]
        across = lax.broadcasted_iota(jnp.int32, (8, LANES), 1)
        slot = (across // width) % EZ
        depth = jnp.where(slot < 2, slot * (EZ - 1), slot - 1)
        shuffled = take_lanes(orient_pad[...], (across % width) * EZ + depth)
        codes = jnp.transpose(shuffled)[:elements]
        code = [jnp.broadcast_to(codes[:, f : f + 1], (elements, LANES)) for f in range(6)]
        code_x = jnp.where(low_half, code[0], code[1])
        index[2 * tiles] = rotated(mid, fast, code_x) + jnp.where(low_half, FACE, 0)
        code_y = jnp.where(mid == 0, code[2], code[3])
        code_z = jnp.where(fast == 0, code[4], code[5])
        for tile in range(tiles):
            first_pos = 2 * tile + half
            index[tile] = rotated(first_pos, fast, code_y) + jnp.where(mid == 0, FACE, 0)
            index[tiles + tile] = rotated(first_pos, mid, code_z) + jnp.where(fast == 0, FACE, 0)
        found = jnp.where(low_border, code[5][width:edge], code[4][:width])
        turned = (found & 4) != 0
        along_a = jnp.where(turned, fast[:border], mid[:border]) ^ (7 * (found & 1))
        along_b = jnp.where(turned, mid[:border], fast[:border]) ^ (7 * ((found >> 1) & 1))
        far_index[...] = (along_a % 2) * FACE + along_b * NP + jnp.where(low_border, NP - 1, 0)
        far_tile[...] = along_a // 2

    def meeting(ref, *at):
        found = None
        for t in range(tiles):
            lanes = pl.ds(t * LANES, LANES)
            last = ref[at + (pl.ds(width, width), lanes)]
            begin = ref[at + (pl.ds(0, width), lanes)]
            got = take_lanes(jnp.where(fast[:border] == NP - 1, last, begin), far_index[...])
            found = got if found is None else jnp.where(far_tile[...] == t, got, found)
        return found

    def tile_of(values, tile):
        return values[:, tile * LANES : (tile + 1) * LANES]

    def swap(values):
        return pltpu.roll(values, FACE, axis=1)

    def along_x(parts, way):
        swapped = [swap(part) for part in parts]
        outs = []
        for out_tile in range(tiles):
            acc = None
            for in_tile in range(tiles):
                at = ((way * tiles + out_tile) * tiles + in_tile) * 2
                term = (
                    coef[pl.ds(at, 1), :] * parts[in_tile]
                    + coef[pl.ds(at + 1, 1), :] * swapped[in_tile]
                )
                acc = term if acc is None else acc + term
            outs.append(acc)
        return outs

    def split(values):
        upper = values.astype(jnp.bfloat16)
        return upper, (values - upper.astype(jnp.float32)).astype(jnp.bfloat16)

    def product(left, right):
        return jnp.dot(left, right, preferred_element_type=jnp.float32)

    def local(parts, rows, geometry_here=lambda: None):
        count = parts[0].shape[0]
        stacked = jnp.concatenate(split(jnp.concatenate(parts, axis=0)), axis=1)
        ahead = packed[pl.ds(0, LANES), :]
        ahead_rest = packed[pl.ds(LANES, LANES), :]
        grads = product(stacked, jnp.concatenate([ahead, ahead], axis=0)) + product(
            stacked, jnp.concatenate([ahead_rest, ahead_rest], axis=0)
        )
        grad_x = along_x(parts, 0)
        geometry_here()
        geom_y = jnp.concatenate([geom[1, rows, pl.ds(t * LANES, LANES)] for t in range(tiles)], axis=0)
        geom_z = jnp.concatenate([geom[2, rows, pl.ds(t * LANES, LANES)] for t in range(tiles)], axis=0)
        flux = jnp.concatenate([grads[:, :LANES] * geom_y, grads[:, LANES:] * geom_z], axis=1)
        flux, flux_rest = split(flux)
        behind = packed[pl.ds(2 * LANES, 2 * LANES), :]
        back = product(flux, behind) + product(flux_rest, behind)
        back = back[:, :LANES] + back[:, LANES:]
        flux_x = [grad_x[t] * geom[0, rows, pl.ds(t * LANES, LANES)] for t in range(tiles)]
        back_x = along_x(flux_x, 1)
        return [
            back[t * count : (t + 1) * count]
            + back_x[t]
            + geom[3, rows, pl.ds(t * LANES, LANES)] * parts[t]
            for t in range(tiles)
        ]

    def faces(parts, pick):
        count = parts[0].shape[0]
        pick, source = pick[:count], source_tile[:count]
        found = take_lanes(parts[0], pick)
        for tile in range(1, tiles):
            found = jnp.where(source == tile, take_lanes(parts[tile], pick), found)
        return found

    has = (narrow > 0, narrow < n_narrow - 1, wide > 0, wide < n_wide - 1)
    where_to = ((wide, narrow - 1), (wide, narrow + 1), (wide - 1, narrow), (wide + 1, narrow))

    def face_copy(step, side):
        return pltpu.make_async_remote_copy(
            src_ref=outbox.at[step, min(side, 2)],
            dst_ref=inbox.at[step, side ^ 1],
            send_sem=load_sem.at[6],
            recv_sem=halo_recv.at[side // 2],
            device_id=where_to[side],
            device_id_type=MESH,
        )

    def await_faces(step, axis):
        low, high = has[2 * axis], has[2 * axis + 1]
        for count, here in ((2, low & high), (1, low ^ high)):

            @pl.when(here)
            def _():
                span = inbox.at[step, pl.ds(2 * axis, count)]
                pltpu.make_async_copy(span, span, halo_recv.at[axis]).wait()

    def await_sent():
        sides = sum(side.astype(jnp.int32) for side in has)
        for count in range(1, 5):

            @pl.when(sides == count)
            def _():
                span = inbox.at[:, pl.ds(0, count)]
                pltpu.make_async_copy(span, span, load_sem.at[6]).wait()

    ahead_of_most = 2 * layer < planes

    def operate(prepare, step, ready, beside):
        def send_faces(sides):
            for side in sides:

                @pl.when(has[side])
                def _():
                    face_copy(step, side).start()

        parts = prepare(0)
        rows = pl.ds(0, edge)
        outer = local(parts, rows, lambda: step or await_rows(geom, 0, edge, 4))
        ends = [
            jnp.where(fast[:width] == NP - 1, part[width:], part[:width]) for part in outer
        ]
        outbox[step, 2] = faces(ends, pick_z)

        def inner_work():
            parts = prepare(1)
            rows = pl.ds(edge, elements - edge)
            found = local(
                parts, rows, lambda: step or await_rows(geom, edge, elements - edge, 5)
            )
            if step == 0:
                for t in range(tiles):
                    image[rows, pl.ds(t * LANES, LANES)] = found[t]
                return None
            return found

        if step == 0:
            pl.when(ahead_of_most)(inner_work)
            ready()
            send_faces((2, 3))
            pl.when(jnp.logical_not(ahead_of_most))(inner_work)
            inner_part = [
                image[pl.ds(edge, elements - edge), pl.ds(t * LANES, LANES)] for t in range(tiles)
            ]
        else:
            send_faces((2, 3))
            inner_part = inner_work()
        result = [jnp.concatenate(pair, axis=0) for pair in zip(outer, inner_part)]
        found_y = faces(result, pick_y)
        face_y[...] = found_y
        outbox[step, 0] = face_y[pl.ds(0, width, stride=EY), :]
        outbox[step, 1] = face_y[pl.ds(EY - 1, width, stride=EY), :]
        send_faces((0, 1))
        found_z = faces(result, pick_z)

        if step == 0:
            make_index()

        face_x = jnp.where(low_half, result[0], result[tiles - 1])
        in_x = jnp.where(
            low_half,
            jnp.where(row_x < EX - 1, pltpu.roll(face_x, elements - EY, axis=0), 0.0),
            jnp.where(row_x > 0, pltpu.roll(face_x, EY, axis=0), 0.0),
        )
        in_y = jnp.where(
            low_half, pltpu.roll(found_y, elements - 1, axis=0), pltpu.roll(found_y, 1, axis=0)
        )
        slot_of = [0] + list(range(2, EZ)) + [1]
        blank = jnp.zeros((width, LANES), jnp.float32)

        def layer(at):
            if at < 0 or at >= EZ:
                return blank
            return found_z[slot_of[at] * width : (slot_of[at] + 1) * width]

        in_z = jnp.concatenate(
            [
                jnp.where(low_border, layer(at + 1), layer(at - 1))
                for at in [0, EZ - 1] + list(range(1, EZ - 1))
            ],
            axis=0,
        )
        got_x = take_lanes(in_x, index[2 * tiles])
        result[0] = result[0] + jnp.where(low_half, got_x, 0.0)
        result[tiles - 1] = result[tiles - 1] + jnp.where(low_half, 0.0, got_x)

        for t in range(tiles):
            result[t] = result[t] + jnp.where(at_z, take_lanes(in_z, index[tiles + t]), 0.0)

        beside()

        await_faces(step, 0)
        halo_y[pl.ds(0, width, stride=EY), :] = inbox[step, 0]
        halo_y[pl.ds(EY - 1, width, stride=EY), :] = inbox[step, 1]
        edge_y = row_y == jnp.where(low_half, EY - 1, 0)
        in_y = jnp.where(edge_y, halo_y[...], in_y)
        for t in range(tiles):
            result[t] = result[t] + jnp.where(at_y, take_lanes(in_y, index[t]), 0.0)
            image[:, pl.ds(t * LANES, LANES)] = result[t]

    def far_faces(step):
        await_faces(step, 1)
        return jnp.where(low_border, inbox[step, 3], inbox[step, 2])

    def add_far(step):
        in_z = jnp.concatenate(
            [
                jnp.where(low_border, 0.0, inbox[step, 2]),
                jnp.where(low_border, inbox[step, 3], 0.0),
            ],
            axis=0,
        )
        for t in range(tiles):
            at = (pl.ds(0, edge), pl.ds(t * LANES, LANES))
            got = take_lanes(in_z, index[tiles + t, pl.ds(0, edge), :])
            image[at] = image[at] + jnp.where(at_z[:edge], got, 0.0)

    def stacked_rows(values):
        return jnp.sum(values.reshape(border // 8, 8, LANES), axis=0)

    def folded(values):
        acc = tile_of(values, 0)
        for tile in range(1, tiles):
            acc = acc + tile_of(values, tile)
        return jnp.sum(acc.reshape(elements // 8, 8, LANES), axis=0)

    def sums_of(partials):
        count = -(-len(partials) // 8) * 8
        rows = [jnp.sum(part, axis=0, keepdims=True) for part in partials]
        rows += [jnp.zeros((1, LANES), jnp.float32)] * (count - len(rows))
        return jnp.sum(jnp.concatenate(rows, axis=0), axis=1, keepdims=True)

    def put(sums, place_of):
        shape = (sums.shape[0], LANES)
        place = place_of(lax.broadcasted_iota(jnp.int32, shape, 0))
        here = place == lax.broadcasted_iota(jnp.int32, shape, 1)
        return jnp.sum(jnp.where(here, sums, 0.0), axis=0, keepdims=True)

    def to_row(partials, begin=0):
        return put(sums_of(partials), lambda at: at + begin)

    def all_sum(block, phase, beside):
        outgoing, incoming = messages[phase]
        outgoing[...] = block
        incoming[pl.ds(me, 1)] = block.reshape((1,) + block.shape)

        def send(where):
            pltpu.make_async_remote_copy(
                src_ref=outgoing,
                dst_ref=incoming.at[me],
                send_sem=load_sem.at[7 + phase],
                recv_sem=(row_recv if phase == 0 else load_sem).at[0],
                device_id=where,
                device_id_type=MESH,
            ).start()

        if phase == 0:

            @pl.when(above)
            def _():
                pl.semaphore_wait(all_ready, planes - 1 - layer)

            @pl.when(below & jnp.logical_not(above))
            def _():
                pl.semaphore_wait(from_below, 1)

        each_peer(send, phase == 1)
        result = beside()
        span = incoming.at[pl.ds(0, devices - 1)]
        pltpu.make_async_copy(span, span, (row_recv if phase == 0 else load_sem).at[0]).wait()
        if devices > 64:
            return jnp.sum(incoming[...], axis=0), result
        found = [incoming[at] for at in range(devices)]
        while len(found) > 1:
            half_way = len(found) // 2
            odd = found[2 * half_way :]
            found = [found[at] + found[half_way + at] for at in range(half_way)] + odd
        return found[0], result

    def weight(row, at):
        spot = jnp.full((8, LANES), at, jnp.int32)
        return take_lanes(jnp.broadcast_to(row, (8, LANES)), spot)

    pieces = [
        (pl.ds(base, 8), pl.ds(tile * LANES, LANES))
        for base in range(0, elements, 8)
        for tile in range(tiles)
    ]

    def against_basis(ref):
        found = [None] * kept
        for at in pieces:
            piece = ref[at]
            for one in range(kept):
                term = basis[(one,) + at] * piece
                found[one] = term if found[one] is None else found[one] + term
        return found

    def against(left, right):
        found = None
        for at in pieces:
            term = left[at] * right[at]
            found = term if found is None else found + term
        return found

    def store_out(which, at, piece):
        begin, tile = at[0].start, at[1].start // LANES
        out[which, tile, pl.ds(places()[begin][1], 8, stride=EZ), :] = piece

    def less_basis(piece, parts, at):
        for one in range(kept):
            piece = piece - parts[one] * basis[(one,) + at]
        return piece

    load_coeffs.wait()

    def start_of(half):
        slots = (0, 1) if half == 0 else range(2, EZ)
        parts = [[] for t in range(tiles)]
        for slot in slots:
            await_rows(basis, slot * width, width, slot)
            for base in range(slot * width, (slot + 1) * width, 8):
                for t in range(tiles):
                    at = (pl.ds(base, 8), pl.ds(t * LANES, LANES))
                    found = None
                    for one in range(kept):
                        term = coeffs[one] * basis[(one,) + at]
                        found = term if found is None else found + term
                    parts[t].append(found)
        if half == 0:
            for copy in load_tables:
                copy.wait()
        return [jnp.concatenate(part, axis=0) for part in parts]

    def greeted():
        pl.semaphore_wait(barrier, greetings)
        to_lower(all_ready)
        to_layer(from_below, layer + 1, jnp.logical_not(below) & above)

    def relay():
        @pl.when(below & above)
        def _():
            pl.semaphore_wait(from_below, 1)

        to_layer(from_below, layer + 1, below & above)

    def meet_basis():
        relay()
        for at in range(kept):
            far_basis[at] = meeting(basis, at)

    operate(start_of, 0, greeted, meet_basis)
    block = 4
    a_line = LANES // kept
    lines = kept // a_line

    def gram():
        found = [jnp.zeros((1, LANES), jnp.float32)] * lines
        for left in range(0, kept, block):
            for right in range(left, kept, block):

                def body(step, carry):
                    base = pl.multiple_of(step * 8, 8)
                    carry = list(carry)
                    for tile in range(tiles):
                        at = (pl.ds(base, 8), pl.ds(tile * LANES, LANES))
                        ones = [basis[(left + m,) + at] for m in range(block)]
                        twos = ones if left == right else [
                            basis[(right + m,) + at] for m in range(block)
                        ]
                        for spot in range(block * block):
                            carry[spot] = carry[spot] + ones[spot // block] * twos[spot % block]
                    return tuple(carry)

                zero = jnp.zeros((8, LANES), jnp.float32)
                partials = lax.fori_loop(0, elements // 8, body, (zero,) * (block * block))
                begin = (left % a_line) * kept + right
                row = put(
                    sums_of(partials), lambda at: begin + (at // block) * kept + at % block
                )
                line_at = left // a_line
                found[line_at] = found[line_at] + (row if left == right else 2.0 * row)
        return found

    near = against_basis(image)
    far = far_faces(0)
    row = to_row([near[at] + stacked_rows(far_basis[at] * far) for at in range(kept)])

    def between():
        add_far(0)
        return gram()

    sums, gram_lines = all_sum(row, 0, between)
    proj_one = sums / total
    parts = [weight(proj_one, at) for at in range(kept)]
    def first_of(half):
        begin, end = (0, edge) if half == 0 else (edge, elements)
        found = []
        for t in range(tiles):
            lanes = pl.ds(t * LANES, LANES)
            for base in range(begin, end, 8):
                at = (pl.ds(base, 8), lanes)
                first[at] = less_basis(image[at], parts, at)
            found.append(first[pl.ds(begin, end - begin), lanes])
        return found

    with_first = []

    def project_first():
        with_first.append(meeting(first))
        with_first.append(
            to_row(
                against_basis(first) + [against(first, first)],
                kept + 2,
            )
        )

    operate(first_of, 1, lambda: None, project_first)
    near = against_basis(image) + [against(first, image), against(image, image)]
    far_first, row_first = with_first
    far_image = 2.0 * meeting(image)
    far = far_faces(1)
    beyond = [stacked_rows(far_basis[at] * far) for at in range(kept)]
    beyond += [stacked_rows(far_first * far), stacked_rows((far_image + far) * far)]
    row = to_row([one + two for one, two in zip(near, beyond)])
    block = jnp.concatenate([row_first + row] + gram_lines, axis=0)

    sums, _ = all_sum(block, 1, lambda: add_far(1))
    sums = sums / total
    along = sums[0:1]
    spot = lax.broadcasted_iota(jnp.int32, (1, LANES), 1)
    inside = spot < kept
    parts = [weight(along, at) for at in range(kept)]
    cross, whole, one = [weight(along, at) for at in (kept, kept + 1, 2 * kept + 2)]
    with_one = pltpu.roll(jnp.broadcast_to(along, (8, LANES)), LANES - kept - 2, axis=1)[0:1]
    pick = lax.broadcasted_iota(jnp.int32, (a_line, LANES), 0) * kept + (
        lax.broadcasted_iota(jnp.int32, (a_line, LANES), 1) % kept
    )
    spread = [
        take_lanes(jnp.broadcast_to(sums[1 + at : 2 + at], (a_line, LANES)), pick)
        for at in range(lines)
    ]
    found = [
        parts[at][0:1] * spread[at // a_line][at % a_line : at % a_line + 1] for at in range(kept)
    ]
    while len(found) > 1:
        found = [found[at] + found[at + 1] for at in range(0, len(found), 2)]
    along_in = jnp.where(inside, along, 0.0)
    terms = jnp.concatenate([along_in * (found[0] - 2.0 * along), along_in * with_one], axis=0)
    terms = jnp.sum(terms, axis=1, keepdims=True)

    norm_one = jnp.sqrt(one + epsilon)
    scale_one = 1.0 / norm_one
    self_two = cross * (scale_one * scale_one)
    for at in pieces:
        piece = first[at]
        store_out(0, at, piece * scale_one)
        image[at] = less_basis(image[at] - self_two * piece, parts, at)

    square = whole + terms[0:1] + self_two * (2.0 * (terms[1:2] - cross) + self_two * one)
    square = jnp.maximum(square, 0.0) * (scale_one * scale_one)
    norm_two = jnp.sqrt(square + epsilon)
    scale_two = scale_one / norm_two
    for at in pieces:
        store_out(1, at, image[at] * scale_two)

    norm_one, scale_one, self_two, norm_two = (
        each[0:1] for each in (norm_one, scale_one, self_two, norm_two)
    )
    row_first = jnp.where(inside, proj_one, jnp.where(spot == kept, norm_one, 0.0))
    row_second = jnp.where(
        inside, along * scale_one, jnp.where(spot == kept, self_two, norm_two)
    )
    hess[pl.ds(0, 1), :] = row_first[:, : kept + 2]
    hess[pl.ds(1, 1), :] = row_second[:, : kept + 2]

    await_sent()
    for phase in range(2):
        span = messages[phase][1].at[pl.ds(0, devices - 1)]
        pltpu.make_async_copy(span, span, load_sem.at[7 + phase]).wait()


def settle(vectors, matrix, out, hess, sem):
    copies = [pltpu.make_async_copy(matrix, hess, sem.at[1])]
    tiles = vectors.shape[1]
    for tile in range(tiles):
        lanes = pl.ds(tile * LANES, LANES)
        copies.append(
            pltpu.make_async_copy(vectors.at[:, tile], out.at[:, :, lanes], sem.at[0])
        )
    for copy in copies:
        copy.start()
    pltpu.make_async_copy(out, out, sem.at[0]).wait()
    copies[0].wait()


def on_device(n_wide, n_narrow, old_basis, restart_coeffs, geometry, orientation):
    kept, elements, points = old_basis.shape
    tiles = points // LANES
    devices = n_wide * n_narrow
    packed, coef = tables()
    rows = 1 + kept * kept // LANES
    anywhere = pl.BlockSpec(memory_space=pl.ANY)
    vmem = pl.BlockSpec(memory_space=pltpu.VMEM)
    f32 = jnp.float32
    border = EX * EY
    shapes = ((2, tiles, elements, LANES), (2, kept + 2))
    held = pl.pallas_call(
        functools.partial(kernel, n_wide, n_narrow),
        out_shape=tuple(pltpu.VMEM(shape, f32) for shape in shapes),
        in_specs=[anywhere] * 6,
        out_specs=(vmem, vmem),
        scratch_shapes=[
            pltpu.SMEM(restart_coeffs.shape, f32),
            pltpu.VMEM(old_basis.shape, f32),
            pltpu.VMEM(geometry.shape, f32),
            pltpu.VMEM(orientation.shape, jnp.int32),
            pltpu.VMEM(packed.shape, jnp.bfloat16),
            pltpu.VMEM(coef.shape, f32),
            pltpu.VMEM((2 * tiles + 1, elements, LANES), jnp.int32),
            pltpu.VMEM((8, LANES), jnp.int32),
            pltpu.VMEM((elements, points), f32),
            pltpu.VMEM((elements, points), f32),
            pltpu.VMEM((elements, LANES), f32),
            pltpu.VMEM((elements, LANES), f32),
            pltpu.VMEM((2, 3, border, LANES), f32),
            pltpu.VMEM((2, 4, border, LANES), f32),
            pltpu.VMEM((1, LANES), f32),
            pltpu.VMEM((devices, 1, LANES), f32),
            pltpu.VMEM((rows, LANES), f32),
            pltpu.VMEM((devices, rows, LANES), f32),
            pltpu.VMEM((border, LANES), jnp.int32),
            pltpu.VMEM((border, LANES), jnp.int32),
            pltpu.VMEM((kept, border, LANES), f32),
            pltpu.SemaphoreType.DMA((10,)),
            pltpu.SemaphoreType.DMA((2,)),
            pltpu.SemaphoreType.DMA((1,)),
            pltpu.SemaphoreType.REGULAR,
            pltpu.SemaphoreType.REGULAR,
        ],
        compiler_params=pltpu.CompilerParams(collective_id=0, has_side_effects=True),
        name="arnoldi",
    )(restart_coeffs, old_basis, geometry, orientation, packed, coef)
    return pl.pallas_call(
        settle,
        out_shape=tuple(
            jax.ShapeDtypeStruct(shape, f32) for shape in ((2, elements, points), shapes[1])
        ),
        in_specs=[vmem, vmem],
        out_specs=(anywhere, anywhere),
        scratch_shapes=[pltpu.SemaphoreType.DMA((2,))],
        name="settle",
    )(*[pltpu.with_memory_space_constraint(each, pltpu.VMEM) for each in held])


def solution(mesh):
    in_specs = (
        P(None, ("wide", "narrow"), None),
        P(),
        P(None, ("wide", "narrow"), None),
        P(None, ("wide", "narrow")),
    )
    out_specs = (P(None, ("wide", "narrow"), None), P())
    return jax.shard_map(
        functools.partial(on_device, mesh.shape["wide"], mesh.shape["narrow"]),
        mesh=mesh,
        in_specs=in_specs,
        out_specs=out_specs,
        check_vma=False,
    )
```

```python
import functools

import jax
import jax.numpy as jnp
import numpy as np
from jax import lax
from jax.experimental import pallas as pl
from jax.experimental.pallas import tpu as pltpu
from jax.sharding import PartitionSpec as P

NP = 8
EX = 4
EY = 4
EZ = 4
LANES = 128
FACE = NP * NP
MESH = pl.DeviceIdType.MESH
highest = lax.Precision.HIGHEST
epsilon = 1e-06


def legendre_columns(nodes, degree):
    columns = [nodes * 0.0 + 1.0, nodes * 1.0]
    for order in range(2, degree + 1):
        columns.append(
            ((2 * order - 1) * nodes * columns[order - 1] - (order - 1) * columns[order - 2])
            / order
        )
    return columns


def gll_derivative(extent):
    degree = extent - 1
    nodes = np.cos(np.pi * np.arange(extent) / degree)
    for sweep in range(100):
        columns = legendre_columns(nodes, degree)
        nodes = nodes - (nodes * columns[degree] - columns[degree - 1]) / (extent * columns[degree])
    gll_nodes = nodes[::-1] * 1.0
    values = legendre_columns(gll_nodes, degree)[degree]
    matrix = np.zeros((extent, extent))
    for row_idx in range(extent):
        for col_idx in range(extent):
            if row_idx != col_idx:
                matrix[row_idx, col_idx] = values[row_idx] / (
                    values[col_idx] * (gll_nodes[row_idx] - gll_nodes[col_idx])
                )
    matrix[0, 0] = -degree * (degree + 1) / 4.0
    matrix[extent - 1, extent - 1] = degree * (degree + 1) / 4.0
    return matrix


def halves(table):
    table = np.asarray(table, np.float32)
    upper = table.astype(jnp.bfloat16).astype(np.float32)
    return upper, table - upper


def tables():
    matrix = gll_derivative(NP)
    identity = np.eye(NP)
    pair = np.eye(2)
    along_y = np.kron(pair, np.kron(matrix, identity))
    along_z = np.kron(pair, np.kron(identity, matrix))
    forward = np.concatenate([along_y.T, along_z.T], axis=1)
    backward = np.concatenate([along_y, along_z], axis=0)
    tiles = NP // 2
    coef = np.zeros((2, tiles, tiles, 2, LANES))
    for way, table in enumerate((matrix, matrix.T)):
        for out_tile in range(tiles):
            for in_tile in range(tiles):
                for half in range(2):
                    lanes = slice(half * FACE, (half + 1) * FACE)
                    row = 2 * out_tile + half
                    coef[way, out_tile, in_tile, 0, lanes] = table[row, 2 * in_tile + half]
                    coef[way, out_tile, in_tile, 1, lanes] = table[row, 2 * in_tile + 1 - half]
    ahead, ahead_rest = halves(forward)
    back, back_rest = halves(backward)
    packed = np.concatenate([ahead, ahead_rest, np.concatenate([back, back_rest], axis=1)], axis=0)
    return (
        jnp.asarray(packed, jnp.bfloat16),
        jnp.asarray(coef.reshape(-1, LANES), jnp.float32),
    )


def places():
    order = [0, EZ - 1] + list(range(1, EZ - 1))
    width = EX * EY
    return [
        (slot * width + at, at * EZ + layer) for slot, layer in enumerate(order) for at in range(width)
    ]


def take_lanes(values, index):
    return jnp.take_along_axis(values, index, axis=1, mode="promise_in_bounds")


def rotated(row, col, code):
    row = row ^ (7 * (code & 1))
    col = col ^ (7 * ((code >> 1) & 1))
    return jnp.where((code & 4) != 0, col * NP + row, row * NP + col)


def kernel(
    n_wide,
    n_narrow,
    coeffs_hbm,
    basis_hbm,
    geom_hbm,
    orient_hbm,
    packed_hbm,
    coef_hbm,
    out,
    hess,
    coeffs,
    basis,
    geom,
    orient,
    packed,
    coef,
    index,
    orient_pad,
    image,
    first,
    face_y,
    halo_y,
    outbox,
    inbox,
    row_out,
    row_in,
    pair_out,
    pair_in,
    far_index,
    far_tile,
    far_basis,
    load_sem,
    halo_recv,
    row_recv,
    all_ready,
    from_below,
):
    wide = lax.axis_index("wide")
    narrow = lax.axis_index("narrow")
    devices = n_wide * n_narrow
    me = wide * n_narrow + narrow
    kept, elements, points = basis.shape
    tiles = points // LANES
    total = float(elements * points * devices)

    def load(source, target, slot):
        return pltpu.make_async_copy(source, target, load_sem.at[slot])

    width = EX * EY
    edge = 2 * width

    def load_rows(source, target, begin, count, slot):
        copies = [
            load(source.at[:, pl.ds(there, 1)], target.at[:, pl.ds(here, 1)], slot)
            for here, there in places()[begin : begin + count]
        ]
        for copy in copies:
            copy.start()

    def await_rows(target, begin, count, slot):
        span = target.at[:, pl.ds(begin, count)]
        load(span, span, slot).wait()

    load_coeffs = load(coeffs_hbm, coeffs, 6)
    load_tables = [load(packed_hbm, packed, 7), load(coef_hbm, coef, 8)]
    load_orient = load(orient_hbm, orient, 9)
    load_coeffs.start()
    for copy in load_tables:
        copy.start()
    for slot in range(2):
        load_rows(basis_hbm, basis, slot * width, width, slot)
    messages = ((row_out, row_in), (pair_out, pair_in))

    def peer(step):
        if devices & (devices - 1):
            other = lax.rem(me + step, devices)
        else:
            other = me
            for bit in range(devices.bit_length() - 1):
                if step >> bit & 1:
                    other = other + (1 - 2 * lax.rem(me // 2**bit, 2)) * 2**bit
        return (other // n_narrow, lax.rem(other, n_narrow))

    def each_peer(act, ascending):
        if devices > 64:

            def body(step, carry):
                other = lax.rem(me + step, devices)
                act((other // n_narrow, lax.rem(other, n_narrow)))
                return carry

            lax.fori_loop(1, devices, body, 0)
        elif ascending:
            for at in range(devices - 1):
                other = at + (me <= at).astype(jnp.int32)
                act((other // n_narrow, lax.rem(other, n_narrow)))
        else:
            for step in range(devices - 1, 0, -1):
                act(peer(step))

    barrier = pltpu.get_barrier_semaphore()

    inner = 1
    while n_wide % (2 * inner) == 0 and 4 * inner * inner <= n_wide:
        inner = 2 * inner
    plane = inner * n_narrow
    planes = n_wide // inner
    layer = wide // inner
    column = lax.rem(wide, inner)
    in_plane = column * n_narrow + narrow

    def in_steps(count, act):
        if count <= 64:
            for step in range(count - 1, 0, -1):
                act(step)
        else:

            def body(step, carry):
                act(step)
                return carry

            lax.fori_loop(1, count, body, 0)

    def signal(semaphore, where):
        pl.semaphore_signal(semaphore, inc=1, device_id=where, device_id_type=MESH)

    def to_layer(semaphore, other, there):
        @pl.when(there)
        def _():
            signal(semaphore, (other * inner + column, narrow))

    def to_higher(semaphore):
        for step in range(planes - 1, 0, -1):
            to_layer(semaphore, layer + step, layer + step < planes)

    def to_lower(semaphore):
        for step in range(planes - 1, 0, -1):
            to_layer(semaphore, layer - step, layer >= step)

    def to_plane(semaphore):
        def act(step):
            other = lax.rem(in_plane + step, plane)
            signal(semaphore, (layer * inner + other // n_narrow, lax.rem(other, n_narrow)))

        in_steps(plane, act)

    below = layer > 0
    above = layer < planes - 1
    greetings = plane - 1 + layer + above.astype(jnp.int32)
    crossing = ()
    if 1 < inner < n_wide:
        crossing = (
            ((column == 0) & (wide > 0), -1),
            ((column == inner - 1) & (wide < n_wide - 1), 1),
        )
    for there, shift in crossing:
        greetings = greetings + there.astype(jnp.int32)

    def greet():
        to_plane(barrier)
        to_layer(barrier, layer - 1, below)
        for there, shift in crossing:

            @pl.when(there)
            def _():
                signal(barrier, (wide + shift, narrow))

        to_higher(barrier)

    inbox[...] = jnp.zeros_like(inbox)
    greet()
    load_rows(geom_hbm, geom, 0, edge, 4)
    for slot in range(2, EZ):
        load_rows(basis_hbm, basis, slot * width, width, slot)
    load_rows(geom_hbm, geom, edge, elements - edge, 5)
    load_orient.start()

    lane = lax.broadcasted_iota(jnp.int32, (elements, LANES), 1)
    line = lax.broadcasted_iota(jnp.int32, (elements, LANES), 0)
    low_half = lane < FACE
    border = width
    low_border = low_half[:border]
    half = lane // FACE
    mid = (lane // NP) % NP
    fast = lane % NP
    row_x = (line // EY) % EX
    row_y = line % EY
    at_y = (mid == 0) | (mid == NP - 1)
    at_z = (fast == 0) | (fast == NP - 1)

    pick_y = (mid % 2) * FACE + half * (FACE - NP) + fast
    pick_z = (mid % 2) * FACE + fast * NP + half * (NP - 1)
    source_tile = mid // 2

    def make_index():
        load_orient.wait()
        orient_pad[...] = jnp.zeros_like(orient_pad)
        orient_pad[pl.ds(0, 6), pl.ds(0, elements)] = orient[...]
        across = lax.broadcasted_iota(jnp.int32, (8, LANES), 1)
        slot = (across // width) % EZ
        depth = jnp.where(slot < 2, slot * (EZ - 1), slot - 1)
        shuffled = take_lanes(orient_pad[...], (across % width) * EZ + depth)
        codes = jnp.transpose(shuffled)[:elements]
        code = [jnp.broadcast_to(codes[:, f : f + 1], (elements, LANES)) for f in range(6)]
        code_x = jnp.where(low_half, code[0], code[1])
        index[2 * tiles] = rotated(mid, fast, code_x) + jnp.where(low_half, FACE, 0)
        code_y = jnp.where(mid == 0, code[2], code[3])
        code_z = jnp.where(fast == 0, code[4], code[5])
        for tile in range(tiles):
            first_pos = 2 * tile + half
            index[tile] = rotated(first_pos, fast, code_y) + jnp.where(mid == 0, FACE, 0)
            index[tiles + tile] = rotated(first_pos, mid, code_z) + jnp.where(fast == 0, FACE, 0)
        found = jnp.where(low_border, code[5][width:edge], code[4][:width])
        turned = (found & 4) != 0
        along_a = jnp.where(turned, fast[:border], mid[:border]) ^ (7 * (found & 1))
        along_b = jnp.where(turned, mid[:border], fast[:border]) ^ (7 * ((found >> 1) & 1))
        far_index[...] = (along_a % 2) * FACE + along_b * NP + jnp.where(low_border, NP - 1, 0)
        far_tile[...] = along_a // 2

    def meeting(ref, *at):
        found = None
        for t in range(tiles):
            lanes = pl.ds(t * LANES, LANES)
            last = ref[at + (pl.ds(width, width), lanes)]
            begin = ref[at + (pl.ds(0, width), lanes)]
            got = take_lanes(jnp.where(fast[:border] == NP - 1, last, begin), far_index[...])
            found = got if found is None else jnp.where(far_tile[...] == t, got, found)
        return found

    def tile_of(values, tile):
        return values[:, tile * LANES : (tile + 1) * LANES]

    def swap(values):
        return pltpu.roll(values, FACE, axis=1)

    def along_x(parts, way):
        swapped = [swap(part) for part in parts]
        outs = []
        for out_tile in range(tiles):
            acc = None
            for in_tile in range(tiles):
                at = ((way * tiles + out_tile) * tiles + in_tile) * 2
                term = (
                    coef[pl.ds(at, 1), :] * parts[in_tile]
                    + coef[pl.ds(at + 1, 1), :] * swapped[in_tile]
                )
                acc = term if acc is None else acc + term
            outs.append(acc)
        return outs

    def split(values):
        upper = values.astype(jnp.bfloat16)
        return upper, (values - upper.astype(jnp.float32)).astype(jnp.bfloat16)

    def product(left, right):
        return jnp.dot(left, right, preferred_element_type=jnp.float32)

    def local(parts, rows, geometry_here=lambda: None):
        count = parts[0].shape[0]
        stacked = jnp.concatenate(split(jnp.concatenate(parts, axis=0)), axis=1)
        ahead = packed[pl.ds(0, LANES), :]
        ahead_rest = packed[pl.ds(LANES, LANES), :]
        grads = product(stacked, jnp.concatenate([ahead, ahead], axis=0)) + product(
            stacked, jnp.concatenate([ahead_rest, ahead_rest], axis=0)
        )
        grad_x = along_x(parts, 0)
        geometry_here()
        geom_y = jnp.concatenate([geom[1, rows, pl.ds(t * LANES, LANES)] for t in range(tiles)], axis=0)
        geom_z = jnp.concatenate([geom[2, rows, pl.ds(t * LANES, LANES)] for t in range(tiles)], axis=0)
        flux = jnp.concatenate([grads[:, :LANES] * geom_y, grads[:, LANES:] * geom_z], axis=1)
        flux, flux_rest = split(flux)
        behind = packed[pl.ds(2 * LANES, 2 * LANES), :]
        back = product(flux, behind) + product(flux_rest, behind)
        back = back[:, :LANES] + back[:, LANES:]
        flux_x = [grad_x[t] * geom[0, rows, pl.ds(t * LANES, LANES)] for t in range(tiles)]
        back_x = along_x(flux_x, 1)
        return [
            back[t * count : (t + 1) * count]
            + back_x[t]
            + geom[3, rows, pl.ds(t * LANES, LANES)] * parts[t]
            for t in range(tiles)
        ]

    def faces(parts, pick):
        count = parts[0].shape[0]
        pick, source = pick[:count], source_tile[:count]
        found = take_lanes(parts[0], pick)
        for tile in range(1, tiles):
            found = jnp.where(source == tile, take_lanes(parts[tile], pick), found)
        return found

    has = (narrow > 0, narrow < n_narrow - 1, wide > 0, wide < n_wide - 1)
    where_to = ((wide, narrow - 1), (wide, narrow + 1), (wide - 1, narrow), (wide + 1, narrow))

    def face_copy(step, side):
        return pltpu.make_async_remote_copy(
            src_ref=outbox.at[step, min(side, 2)],
            dst_ref=inbox.at[step, side ^ 1],
            send_sem=load_sem.at[6],
            recv_sem=halo_recv.at[side // 2],
            device_id=where_to[side],
            device_id_type=MESH,
        )

    def await_faces(step, axis):
        low, high = has[2 * axis], has[2 * axis + 1]
        for count, here in ((2, low & high), (1, low ^ high)):

            @pl.when(here)
            def _():
                span = inbox.at[step, pl.ds(2 * axis, count)]
                pltpu.make_async_copy(span, span, halo_recv.at[axis]).wait()

    def await_sent():
        sides = sum(side.astype(jnp.int32) for side in has)
        for count in range(1, 5):

            @pl.when(sides == count)
            def _():
                span = inbox.at[:, pl.ds(0, count)]
                pltpu.make_async_copy(span, span, load_sem.at[6]).wait()

    ahead_of_most = 2 * layer < planes

    def operate(prepare, step, ready, beside):
        def send_faces(sides):
            for side in sides:

                @pl.when(has[side])
                def _():
                    face_copy(step, side).start()

        parts = prepare(0)
        rows = pl.ds(0, edge)
        outer = local(parts, rows, lambda: step or await_rows(geom, 0, edge, 4))
        ends = [
            jnp.where(fast[:width] == NP - 1, part[width:], part[:width]) for part in outer
        ]
        outbox[step, 2] = faces(ends, pick_z)

        def inner_work():
            parts = prepare(1)
            rows = pl.ds(edge, elements - edge)
            found = local(
                parts, rows, lambda: step or await_rows(geom, edge, elements - edge, 5)
            )
            if step == 0:
                for t in range(tiles):
                    image[rows, pl.ds(t * LANES, LANES)] = found[t]
                return None
            return found

        if step == 0:
            pl.when(ahead_of_most)(inner_work)
            ready()
            send_faces((2, 3))
            pl.when(jnp.logical_not(ahead_of_most))(inner_work)
            inner_part = [
                image[pl.ds(edge, elements - edge), pl.ds(t * LANES, LANES)] for t in range(tiles)
            ]
        else:
            send_faces((2, 3))
            inner_part = inner_work()
        result = [jnp.concatenate(pair, axis=0) for pair in zip(outer, inner_part)]
        found_y = faces(result, pick_y)
        face_y[...] = found_y
        outbox[step, 0] = face_y[pl.ds(0, width, stride=EY), :]
        outbox[step, 1] = face_y[pl.ds(EY - 1, width, stride=EY), :]
        send_faces((0, 1))
        found_z = faces(result, pick_z)

        if step == 0:
            make_index()

        face_x = jnp.where(low_half, result[0], result[tiles - 1])
        in_x = jnp.where(
            low_half,
            jnp.where(row_x < EX - 1, pltpu.roll(face_x, elements - EY, axis=0), 0.0),
            jnp.where(row_x > 0, pltpu.roll(face_x, EY, axis=0), 0.0),
        )
        in_y = jnp.where(
            low_half, pltpu.roll(found_y, elements - 1, axis=0), pltpu.roll(found_y, 1, axis=0)
        )
        slot_of = [0] + list(range(2, EZ)) + [1]
        blank = jnp.zeros((width, LANES), jnp.float32)

        def layer(at):
            if at < 0 or at >= EZ:
                return blank
            return found_z[slot_of[at] * width : (slot_of[at] + 1) * width]

        in_z = jnp.concatenate(
            [
                jnp.where(low_border, layer(at + 1), layer(at - 1))
                for at in [0, EZ - 1] + list(range(1, EZ - 1))
            ],
            axis=0,
        )
        got_x = take_lanes(in_x, index[2 * tiles])
        result[0] = result[0] + jnp.where(low_half, got_x, 0.0)
        result[tiles - 1] = result[tiles - 1] + jnp.where(low_half, 0.0, got_x)

        for t in range(tiles):
            result[t] = result[t] + jnp.where(at_z, take_lanes(in_z, index[tiles + t]), 0.0)

        beside()

        await_faces(step, 0)
        halo_y[pl.ds(0, width, stride=EY), :] = inbox[step, 0]
        halo_y[pl.ds(EY - 1, width, stride=EY), :] = inbox[step, 1]
        edge_y = row_y == jnp.where(low_half, EY - 1, 0)
        in_y = jnp.where(edge_y, halo_y[...], in_y)
        for t in range(tiles):
            result[t] = result[t] + jnp.where(at_y, take_lanes(in_y, index[t]), 0.0)
            image[:, pl.ds(t * LANES, LANES)] = result[t]

    def far_faces(step):
        await_faces(step, 1)
        return jnp.where(low_border, inbox[step, 3], inbox[step, 2])

    def add_far(step):
        in_z = jnp.concatenate(
            [
                jnp.where(low_border, 0.0, inbox[step, 2]),
                jnp.where(low_border, inbox[step, 3], 0.0),
            ],
            axis=0,
        )
        for t in range(tiles):
            at = (pl.ds(0, edge), pl.ds(t * LANES, LANES))
            got = take_lanes(in_z, index[tiles + t, pl.ds(0, edge), :])
            image[at] = image[at] + jnp.where(at_z[:edge], got, 0.0)

    def stacked_rows(values):
        return jnp.sum(values.reshape(border // 8, 8, LANES), axis=0)

    def folded(values):
        acc = tile_of(values, 0)
        for tile in range(1, tiles):
            acc = acc + tile_of(values, tile)
        return jnp.sum(acc.reshape(elements // 8, 8, LANES), axis=0)

    def sums_of(partials):
        count = -(-len(partials) // 8) * 8
        rows = [jnp.sum(part, axis=0, keepdims=True) for part in partials]
        rows += [jnp.zeros((1, LANES), jnp.float32)] * (count - len(rows))
        return jnp.sum(jnp.concatenate(rows, axis=0), axis=1, keepdims=True)

    def put(sums, place_of):
        shape = (sums.shape[0], LANES)
        place = place_of(lax.broadcasted_iota(jnp.int32, shape, 0))
        here = place == lax.broadcasted_iota(jnp.int32, shape, 1)
        return jnp.sum(jnp.where(here, sums, 0.0), axis=0, keepdims=True)

    def to_row(partials, begin=0):
        return put(sums_of(partials), lambda at: at + begin)

    def all_sum(block, phase, beside):
        outgoing, incoming = messages[phase]
        outgoing[...] = block
        incoming[pl.ds(me, 1)] = block.reshape((1,) + block.shape)

        def send(where):
            pltpu.make_async_remote_copy(
                src_ref=outgoing,
                dst_ref=incoming.at[me],
                send_sem=load_sem.at[7 + phase],
                recv_sem=(row_recv if phase == 0 else load_sem).at[0],
                device_id=where,
                device_id_type=MESH,
            ).start()

        if phase == 0:

            @pl.when(above)
            def _():
                pl.semaphore_wait(all_ready, planes - 1 - layer)

            @pl.when(below & jnp.logical_not(above))
            def _():
                pl.semaphore_wait(from_below, 1)

        each_peer(send, phase == 1)
        result = beside()
        span = incoming.at[pl.ds(0, devices - 1)]
        pltpu.make_async_copy(span, span, (row_recv if phase == 0 else load_sem).at[0]).wait()
        if devices > 64:
            return jnp.sum(incoming[...], axis=0), result
        found = [incoming[at] for at in range(devices)]
        while len(found) > 1:
            half_way = len(found) // 2
            odd = found[2 * half_way :]
            found = [found[at] + found[half_way + at] for at in range(half_way)] + odd
        return found[0], result

    def weight(row, at):
        spot = jnp.full((8, LANES), at, jnp.int32)
        return take_lanes(jnp.broadcast_to(row, (8, LANES)), spot)

    pieces = [
        (pl.ds(base, 8), pl.ds(tile * LANES, LANES))
        for base in range(0, elements, 8)
        for tile in range(tiles)
    ]

    def against_basis(ref):
        found = [None] * kept
        for at in pieces:
            piece = ref[at]
            for one in range(kept):
                term = basis[(one,) + at] * piece
                found[one] = term if found[one] is None else found[one] + term
        return found

    def against(left, right):
        found = None
        for at in pieces:
            term = left[at] * right[at]
            found = term if found is None else found + term
        return found

    def store_out(which, at, piece):
        begin, tile = at[0].start, at[1].start // LANES
        out[which, tile, pl.ds(places()[begin][1], 8, stride=EZ), :] = piece

    def less_basis(piece, parts, at):
        for one in range(kept):
            piece = piece - parts[one] * basis[(one,) + at]
        return piece

    load_coeffs.wait()

    def start_of(half):
        slots = (0, 1) if half == 0 else range(2, EZ)
        parts = [[] for t in range(tiles)]
        for slot in slots:
            await_rows(basis, slot * width, width, slot)
            for base in range(slot * width, (slot + 1) * width, 8):
                for t in range(tiles):
                    at = (pl.ds(base, 8), pl.ds(t * LANES, LANES))
                    found = None
                    for one in range(kept):
                        term = coeffs[one] * basis[(one,) + at]
                        found = term if found is None else found + term
                    parts[t].append(found)
        if half == 0:
            for copy in load_tables:
                copy.wait()
        return [jnp.concatenate(part, axis=0) for part in parts]

    def greeted():
        pl.semaphore_wait(barrier, greetings)
        to_lower(all_ready)
        to_layer(from_below, layer + 1, jnp.logical_not(below) & above)

    def relay():
        @pl.when(below & above)
        def _():
            pl.semaphore_wait(from_below, 1)

        to_layer(from_below, layer + 1, below & above)

    def meet_basis():
        relay()
        for at in range(kept):
            far_basis[at] = meeting(basis, at)

    operate(start_of, 0, greeted, meet_basis)
    block = 4
    a_line = LANES // kept
    lines = kept // a_line

    def gram():
        found = [jnp.zeros((1, LANES), jnp.float32)] * lines
        for left in range(0, kept, block):
            for right in range(left, kept, block):

                def body(step, carry):
                    base = pl.multiple_of(step * 8, 8)
                    carry = list(carry)
                    for tile in range(tiles):
                        at = (pl.ds(base, 8), pl.ds(tile * LANES, LANES))
                        ones = [basis[(left + m,) + at] for m in range(block)]
                        twos = ones if left == right else [
                            basis[(right + m,) + at] for m in range(block)
                        ]
                        for spot in range(block * block):
                            carry[spot] = carry[spot] + ones[spot // block] * twos[spot % block]
                    return tuple(carry)

                zero = jnp.zeros((8, LANES), jnp.float32)
                partials = lax.fori_loop(0, elements // 8, body, (zero,) * (block * block))
                begin = (left % a_line) * kept + right
                row = put(
                    sums_of(partials), lambda at: begin + (at // block) * kept + at % block
                )
                line_at = left // a_line
                found[line_at] = found[line_at] + (row if left == right else 2.0 * row)
        return found

    near = against_basis(image)
    far = far_faces(0)
    row = to_row([near[at] + stacked_rows(far_basis[at] * far) for at in range(kept)])

    def between():
        add_far(0)
        return gram()

    sums, gram_lines = all_sum(row, 0, between)
    proj_one = sums / total
    parts = [weight(proj_one, at) for at in range(kept)]
    def first_of(half):
        begin, end = (0, edge) if half == 0 else (edge, elements)
        found = []
        for t in range(tiles):
            lanes = pl.ds(t * LANES, LANES)
            for base in range(begin, end, 8):
                at = (pl.ds(base, 8), lanes)
                first[at] = less_basis(image[at], parts, at)
            found.append(first[pl.ds(begin, end - begin), lanes])
        return found

    with_first = []

    def project_first():
        with_first.append(meeting(first))
        with_first.append(
            to_row(
                against_basis(first) + [against(first, first)],
                kept + 2,
            )
        )

    operate(first_of, 1, lambda: None, project_first)
    near = against_basis(image) + [against(first, image), against(image, image)]
    far_first, row_first = with_first
    far_image = 2.0 * meeting(image)
    far = far_faces(1)
    beyond = [stacked_rows(far_basis[at] * far) for at in range(kept)]
    beyond += [stacked_rows(far_first * far), stacked_rows((far_image + far) * far)]
    row = to_row([one + two for one, two in zip(near, beyond)])
    block = jnp.concatenate([row_first + row] + gram_lines, axis=0)

    sums, _ = all_sum(block, 1, lambda: add_far(1))
    sums = sums / total
    along = sums[0:1]
    spot = lax.broadcasted_iota(jnp.int32, (1, LANES), 1)
    inside = spot < kept
    parts = [weight(along, at) for at in range(kept)]
    cross, whole, one = [weight(along, at) for at in (kept, kept + 1, 2 * kept + 2)]
    with_one = pltpu.roll(jnp.broadcast_to(along, (8, LANES)), LANES - kept - 2, axis=1)[0:1]
    pick = lax.broadcasted_iota(jnp.int32, (a_line, LANES), 0) * kept + (
        lax.broadcasted_iota(jnp.int32, (a_line, LANES), 1) % kept
    )
    spread = [
        take_lanes(jnp.broadcast_to(sums[1 + at : 2 + at], (a_line, LANES)), pick)
        for at in range(lines)
    ]
    found = [
        parts[at][0:1] * spread[at // a_line][at % a_line : at % a_line + 1] for at in range(kept)
    ]
    while len(found) > 1:
        found = [found[at] + found[at + 1] for at in range(0, len(found), 2)]
    along_in = jnp.where(inside, along, 0.0)
    terms = jnp.concatenate([along_in * (found[0] - 2.0 * along), along_in * with_one], axis=0)
    terms = jnp.sum(terms, axis=1, keepdims=True)

    scale_one = lax.rsqrt(one + epsilon)
    norm_one = jnp.sqrt(one + epsilon)
    self_two = cross * (scale_one * scale_one)
    for at in pieces:
        piece = first[at]
        store_out(0, at, piece * scale_one)
        image[at] = less_basis(image[at] - self_two * piece, parts, at)

    square = whole + terms[0:1] + self_two * (2.0 * (terms[1:2] - cross) + self_two * one)
    square = jnp.maximum(square, 0.0) * (scale_one * scale_one)
    scale_two = scale_one * lax.rsqrt(square + epsilon)
    norm_two = jnp.sqrt(square + epsilon)
    for at in pieces:
        store_out(1, at, image[at] * scale_two)

    norm_one, scale_one, self_two, norm_two = (
        each[0:1] for each in (norm_one, scale_one, self_two, norm_two)
    )
    row_first = jnp.where(inside, proj_one, jnp.where(spot == kept, norm_one, 0.0))
    row_second = jnp.where(
        inside, along * scale_one, jnp.where(spot == kept, self_two, norm_two)
    )
    hess[pl.ds(0, 1), :] = row_first[:, : kept + 2]
    hess[pl.ds(1, 1), :] = row_second[:, : kept + 2]

    await_sent()
    for phase in range(2):
        span = messages[phase][1].at[pl.ds(0, devices - 1)]
        pltpu.make_async_copy(span, span, load_sem.at[7 + phase]).wait()


def settle(vectors, matrix, out, hess, sem):
    copies = [pltpu.make_async_copy(matrix, hess, sem.at[1])]
    tiles = vectors.shape[1]
    for tile in range(tiles):
        lanes = pl.ds(tile * LANES, LANES)
        copies.append(
            pltpu.make_async_copy(vectors.at[:, tile], out.at[:, :, lanes], sem.at[0])
        )
    for copy in copies:
        copy.start()
    pltpu.make_async_copy(out, out, sem.at[0]).wait()
    copies[0].wait()


def on_device(n_wide, n_narrow, old_basis, restart_coeffs, geometry, orientation):
    kept, elements, points = old_basis.shape
    tiles = points // LANES
    devices = n_wide * n_narrow
    packed, coef = tables()
    rows = 1 + kept * kept // LANES
    anywhere = pl.BlockSpec(memory_space=pl.ANY)
    vmem = pl.BlockSpec(memory_space=pltpu.VMEM)
    f32 = jnp.float32
    border = EX * EY
    shapes = ((2, tiles, elements, LANES), (2, kept + 2))
    held = pl.pallas_call(
        functools.partial(kernel, n_wide, n_narrow),
        out_shape=tuple(pltpu.VMEM(shape, f32) for shape in shapes),
        in_specs=[anywhere] * 6,
        out_specs=(vmem, vmem),
        scratch_shapes=[
            pltpu.SMEM(restart_coeffs.shape, f32),
            pltpu.VMEM(old_basis.shape, f32),
            pltpu.VMEM(geometry.shape, f32),
            pltpu.VMEM(orientation.shape, jnp.int32),
            pltpu.VMEM(packed.shape, jnp.bfloat16),
            pltpu.VMEM(coef.shape, f32),
            pltpu.VMEM((2 * tiles + 1, elements, LANES), jnp.int32),
            pltpu.VMEM((8, LANES), jnp.int32),
            pltpu.VMEM((elements, points), f32),
            pltpu.VMEM((elements, points), f32),
            pltpu.VMEM((elements, LANES), f32),
            pltpu.VMEM((elements, LANES), f32),
            pltpu.VMEM((2, 3, border, LANES), f32),
            pltpu.VMEM((2, 4, border, LANES), f32),
            pltpu.VMEM((1, LANES), f32),
            pltpu.VMEM((devices, 1, LANES), f32),
            pltpu.VMEM((rows, LANES), f32),
            pltpu.VMEM((devices, rows, LANES), f32),
            pltpu.VMEM((border, LANES), jnp.int32),
            pltpu.VMEM((border, LANES), jnp.int32),
            pltpu.VMEM((kept, border, LANES), f32),
            pltpu.SemaphoreType.DMA((10,)),
            pltpu.SemaphoreType.DMA((2,)),
            pltpu.SemaphoreType.DMA((1,)),
            pltpu.SemaphoreType.REGULAR,
            pltpu.SemaphoreType.REGULAR,
        ],
        compiler_params=pltpu.CompilerParams(collective_id=0, has_side_effects=True),
        name="arnoldi",
    )(restart_coeffs, old_basis, geometry, orientation, packed, coef)
    return pl.pallas_call(
        settle,
        out_shape=tuple(
            jax.ShapeDtypeStruct(shape, f32) for shape in ((2, elements, points), shapes[1])
        ),
        in_specs=[vmem, vmem],
        out_specs=(anywhere, anywhere),
        scratch_shapes=[pltpu.SemaphoreType.DMA((2,))],
        name="settle",
    )(*[pltpu.with_memory_space_constraint(each, pltpu.VMEM) for each in held])


def solution(mesh):
    in_specs = (
        P(None, ("wide", "narrow"), None),
        P(),
        P(None, ("wide", "narrow"), None),
        P(None, ("wide", "narrow")),
    )
    out_specs = (P(None, ("wide", "narrow"), None), P())
    return jax.shard_map(
        functools.partial(on_device, mesh.shape["wide"], mesh.shape["narrow"]),
        mesh=mesh,
        in_specs=in_specs,
        out_specs=out_specs,
        check_vma=False,
    )
```

```python
import functools

import jax
import jax.numpy as jnp
import numpy as np
from jax import lax
from jax.experimental import pallas as pl
from jax.experimental.pallas import tpu as pltpu
from jax.sharding import PartitionSpec as P

NP = 8
EX = 4
EY = 4
EZ = 4
LANES = 128
FACE = NP * NP
MESH = pl.DeviceIdType.MESH
highest = lax.Precision.HIGHEST
epsilon = 1e-06


def legendre_columns(nodes, degree):
    columns = [nodes * 0.0 + 1.0, nodes * 1.0]
    for order in range(2, degree + 1):
        columns.append(
            ((2 * order - 1) * nodes * columns[order - 1] - (order - 1) * columns[order - 2])
            / order
        )
    return columns


def gll_derivative(extent):
    degree = extent - 1
    nodes = np.cos(np.pi * np.arange(extent) / degree)
    for sweep in range(100):
        columns = legendre_columns(nodes, degree)
        nodes = nodes - (nodes * columns[degree] - columns[degree - 1]) / (extent * columns[degree])
    gll_nodes = nodes[::-1] * 1.0
    values = legendre_columns(gll_nodes, degree)[degree]
    matrix = np.zeros((extent, extent))
    for row_idx in range(extent):
        for col_idx in range(extent):
            if row_idx != col_idx:
                matrix[row_idx, col_idx] = values[row_idx] / (
                    values[col_idx] * (gll_nodes[row_idx] - gll_nodes[col_idx])
                )
    matrix[0, 0] = -degree * (degree + 1) / 4.0
    matrix[extent - 1, extent - 1] = degree * (degree + 1) / 4.0
    return matrix


def halves(table):
    table = np.asarray(table, np.float32)
    upper = table.astype(jnp.bfloat16).astype(np.float32)
    return upper, table - upper


def tables():
    matrix = gll_derivative(NP)
    identity = np.eye(NP)
    pair = np.eye(2)
    along_y = np.kron(pair, np.kron(matrix, identity))
    along_z = np.kron(pair, np.kron(identity, matrix))
    forward = np.concatenate([along_y.T, along_z.T], axis=1)
    backward = np.concatenate([along_y, along_z], axis=0)
    tiles = NP // 2
    coef = np.zeros((2, tiles, tiles, 2, LANES))
    for way, table in enumerate((matrix, matrix.T)):
        for out_tile in range(tiles):
            for in_tile in range(tiles):
                for half in range(2):
                    lanes = slice(half * FACE, (half + 1) * FACE)
                    row = 2 * out_tile + half
                    coef[way, out_tile, in_tile, 0, lanes] = table[row, 2 * in_tile + half]
                    coef[way, out_tile, in_tile, 1, lanes] = table[row, 2 * in_tile + 1 - half]
    ahead, ahead_rest = halves(forward)
    back, back_rest = halves(backward)
    packed = np.concatenate([ahead, ahead_rest, np.concatenate([back, back_rest], axis=1)], axis=0)
    return (
        jnp.asarray(packed, jnp.bfloat16),
        jnp.asarray(coef.reshape(-1, LANES), jnp.float32),
    )


def places():
    order = [0, EZ - 1] + list(range(1, EZ - 1))
    width = EX * EY
    return [
        (slot * width + at, at * EZ + layer) for slot, layer in enumerate(order) for at in range(width)
    ]


def take_lanes(values, index):
    return jnp.take_along_axis(values, index, axis=1, mode="promise_in_bounds")


def rotated(row, col, code):
    row = row ^ (7 * (code & 1))
    col = col ^ (7 * ((code >> 1) & 1))
    return jnp.where((code & 4) != 0, col * NP + row, row * NP + col)


def kernel(
    n_wide,
    n_narrow,
    coeffs_hbm,
    basis_hbm,
    geom_hbm,
    orient_hbm,
    packed_hbm,
    coef_hbm,
    out,
    hess,
    coeffs,
    basis,
    geom,
    orient,
    packed,
    coef,
    index,
    orient_pad,
    image,
    first,
    face_y,
    halo_y,
    outbox,
    inbox,
    row_out,
    row_in,
    pair_out,
    pair_in,
    far_index,
    far_tile,
    far_basis,
    load_sem,
    halo_recv,
    row_recv,
    all_ready,
    from_below,
):
    wide = lax.axis_index("wide")
    narrow = lax.axis_index("narrow")
    devices = n_wide * n_narrow
    me = wide * n_narrow + narrow
    kept, elements, points = basis.shape
    tiles = points // LANES
    total = float(elements * points * devices)

    def load(source, target, slot):
        return pltpu.make_async_copy(source, target, load_sem.at[slot])

    width = EX * EY
    edge = 2 * width

    def load_rows(source, target, begin, count, slot):
        copies = [
            load(source.at[:, pl.ds(there, 1)], target.at[:, pl.ds(here, 1)], slot)
            for here, there in places()[begin : begin + count]
        ]
        for copy in copies:
            copy.start()

    def await_rows(target, begin, count, slot):
        span = target.at[:, pl.ds(begin, count)]
        load(span, span, slot).wait()

    load_coeffs = load(coeffs_hbm, coeffs, 6)
    load_tables = [load(packed_hbm, packed, 7), load(coef_hbm, coef, 8)]
    load_orient = load(orient_hbm, orient, 9)
    load_coeffs.start()
    for copy in load_tables:
        copy.start()
    for slot in range(2):
        load_rows(basis_hbm, basis, slot * width, width, slot)
    messages = ((row_out, row_in), (pair_out, pair_in))

    def peer(step):
        if devices & (devices - 1):
            other = lax.rem(me + step, devices)
        else:
            other = me
            for bit in range(devices.bit_length() - 1):
                if step >> bit & 1:
                    other = other + (1 - 2 * lax.rem(me // 2**bit, 2)) * 2**bit
        return (other // n_narrow, lax.rem(other, n_narrow))

    def each_peer(act, ascending):
        if devices > 64:

            def body(step, carry):
                other = lax.rem(me + step, devices)
                act((other // n_narrow, lax.rem(other, n_narrow)))
                return carry

            lax.fori_loop(1, devices, body, 0)
        elif ascending:
            for at in range(devices - 1):
                other = at + (me <= at).astype(jnp.int32)
                act((other // n_narrow, lax.rem(other, n_narrow)))
        else:
            for step in range(devices - 1, 0, -1):
                act(peer(step))

    barrier = pltpu.get_barrier_semaphore()

    inner = 1
    while n_wide % (2 * inner) == 0 and 4 * inner * inner <= n_wide:
        inner = 2 * inner
    plane = inner * n_narrow
    planes = n_wide // inner
    layer = wide // inner
    column = lax.rem(wide, inner)
    in_plane = column * n_narrow + narrow

    def in_steps(count, act):
        if count <= 64:
            for step in range(count - 1, 0, -1):
                act(step)
        else:

            def body(step, carry):
                act(step)
                return carry

            lax.fori_loop(1, count, body, 0)

    def signal(semaphore, where):
        pl.semaphore_signal(semaphore, inc=1, device_id=where, device_id_type=MESH)

    def to_layer(semaphore, other, there):
        @pl.when(there)
        def _():
            signal(semaphore, (other * inner + column, narrow))

    def to_higher(semaphore):
        for step in range(planes - 1, 0, -1):
            to_layer(semaphore, layer + step, layer + step < planes)

    def to_lower(semaphore):
        for step in range(planes - 1, 0, -1):
            to_layer(semaphore, layer - step, layer >= step)

    def to_plane(semaphore):
        def act(step):
            other = lax.rem(in_plane + step, plane)
            signal(semaphore, (layer * inner + other // n_narrow, lax.rem(other, n_narrow)))

        in_steps(plane, act)

    below = layer > 0
    above = layer < planes - 1
    greetings = plane - 1 + layer + above.astype(jnp.int32)
    crossing = ()
    if 1 < inner < n_wide:
        crossing = (
            ((column == 0) & (wide > 0), -1),
            ((column == inner - 1) & (wide < n_wide - 1), 1),
        )
    for there, shift in crossing:
        greetings = greetings + there.astype(jnp.int32)

    def greet():
        to_plane(barrier)
        to_layer(barrier, layer - 1, below)
        for there, shift in crossing:

            @pl.when(there)
            def _():
                signal(barrier, (wide + shift, narrow))

        to_higher(barrier)

    inbox[...] = jnp.zeros_like(inbox)
    greet()
    load_rows(geom_hbm, geom, 0, edge, 4)
    for slot in range(2, EZ):
        load_rows(basis_hbm, basis, slot * width, width, slot)
    load_rows(geom_hbm, geom, edge, elements - edge, 5)
    load_orient.start()

    lane = lax.broadcasted_iota(jnp.int32, (elements, LANES), 1)
    line = lax.broadcasted_iota(jnp.int32, (elements, LANES), 0)
    low_half = lane < FACE
    border = width
    low_border = low_half[:border]
    half = lane // FACE
    mid = (lane // NP) % NP
    fast = lane % NP
    row_x = (line // EY) % EX
    row_y = line % EY
    at_y = (mid == 0) | (mid == NP - 1)
    at_z = (fast == 0) | (fast == NP - 1)

    pick_y = (mid % 2) * FACE + half * (FACE - NP) + fast
    pick_z = (mid % 2) * FACE + fast * NP + half * (NP - 1)
    source_tile = mid // 2

    def make_index():
        load_orient.wait()
        orient_pad[...] = jnp.zeros_like(orient_pad)
        orient_pad[pl.ds(0, 6), pl.ds(0, elements)] = orient[...]
        across = lax.broadcasted_iota(jnp.int32, (8, LANES), 1)
        slot = (across // width) % EZ
        depth = jnp.where(slot < 2, slot * (EZ - 1), slot - 1)
        shuffled = take_lanes(orient_pad[...], (across % width) * EZ + depth)
        codes = jnp.transpose(shuffled)[:elements]
        code = [jnp.broadcast_to(codes[:, f : f + 1], (elements, LANES)) for f in range(6)]
        code_x = jnp.where(low_half, code[0], code[1])
        index[2 * tiles] = rotated(mid, fast, code_x) + jnp.where(low_half, FACE, 0)
        code_y = jnp.where(mid == 0, code[2], code[3])
        code_z = jnp.where(fast == 0, code[4], code[5])
        for tile in range(tiles):
            first_pos = 2 * tile + half
            index[tile] = rotated(first_pos, fast, code_y) + jnp.where(mid == 0, FACE, 0)
            index[tiles + tile] = rotated(first_pos, mid, code_z) + jnp.where(fast == 0, FACE, 0)
        found = jnp.where(low_border, code[5][width:edge], code[4][:width])
        turned = (found & 4) != 0
        along_a = jnp.where(turned, fast[:border], mid[:border]) ^ (7 * (found & 1))
        along_b = jnp.where(turned, mid[:border], fast[:border]) ^ (7 * ((found >> 1) & 1))
        far_index[...] = (along_a % 2) * FACE + along_b * NP + jnp.where(low_border, NP - 1, 0)
        far_tile[...] = along_a // 2

    def meeting(ref, *at):
        found = None
        for t in range(tiles):
            lanes = pl.ds(t * LANES, LANES)
            last = ref[at + (pl.ds(width, width), lanes)]
            begin = ref[at + (pl.ds(0, width), lanes)]
            got = take_lanes(jnp.where(fast[:border] == NP - 1, last, begin), far_index[...])
            found = got if found is None else jnp.where(far_tile[...] == t, got, found)
        return found

    def tile_of(values, tile):
        return values[:, tile * LANES : (tile + 1) * LANES]

    def swap(values):
        return pltpu.roll(values, FACE, axis=1)

    def along_x(parts, way):
        swapped = [swap(part) for part in parts]
        outs = []
        for out_tile in range(tiles):
            acc = None
            for in_tile in range(tiles):
                at = ((way * tiles + out_tile) * tiles + in_tile) * 2
                term = (
                    coef[pl.ds(at, 1), :] * parts[in_tile]
                    + coef[pl.ds(at + 1, 1), :] * swapped[in_tile]
                )
                acc = term if acc is None else acc + term
            outs.append(acc)
        return outs

    def split(values):
        upper = values.astype(jnp.bfloat16)
        return upper, (values - upper.astype(jnp.float32)).astype(jnp.bfloat16)

    def product(left, right):
        return jnp.dot(left, right, preferred_element_type=jnp.float32)

    def local(parts, rows, geometry_here=lambda: None):
        count = parts[0].shape[0]
        stacked = jnp.concatenate(split(jnp.concatenate(parts, axis=0)), axis=1)
        ahead = packed[pl.ds(0, LANES), :]
        ahead_rest = packed[pl.ds(LANES, LANES), :]
        grads = product(stacked, jnp.concatenate([ahead, ahead], axis=0)) + product(
            stacked, jnp.concatenate([ahead_rest, ahead_rest], axis=0)
        )
        grad_x = along_x(parts, 0)
        geometry_here()
        geom_y = jnp.concatenate([geom[1, rows, pl.ds(t * LANES, LANES)] for t in range(tiles)], axis=0)
        geom_z = jnp.concatenate([geom[2, rows, pl.ds(t * LANES, LANES)] for t in range(tiles)], axis=0)
        flux = jnp.concatenate([grads[:, :LANES] * geom_y, grads[:, LANES:] * geom_z], axis=1)
        flux, flux_rest = split(flux)
        behind = packed[pl.ds(2 * LANES, 2 * LANES), :]
        back = product(flux, behind) + product(flux_rest, behind)
        back = back[:, :LANES] + back[:, LANES:]
        flux_x = [grad_x[t] * geom[0, rows, pl.ds(t * LANES, LANES)] for t in range(tiles)]
        back_x = along_x(flux_x, 1)
        return [
            back[t * count : (t + 1) * count]
            + back_x[t]
            + geom[3, rows, pl.ds(t * LANES, LANES)] * parts[t]
            for t in range(tiles)
        ]

    def faces(parts, pick):
        count = parts[0].shape[0]
        pick, source = pick[:count], source_tile[:count]
        found = take_lanes(parts[0], pick)
        for tile in range(1, tiles):
            found = jnp.where(source == tile, take_lanes(parts[tile], pick), found)
        return found

    has = (narrow > 0, narrow < n_narrow - 1, wide > 0, wide < n_wide - 1)
    where_to = ((wide, narrow - 1), (wide, narrow + 1), (wide - 1, narrow), (wide + 1, narrow))

    def face_copy(step, side):
        return pltpu.make_async_remote_copy(
            src_ref=outbox.at[step, min(side, 2)],
            dst_ref=inbox.at[step, side ^ 1],
            send_sem=load_sem.at[6],
            recv_sem=halo_recv.at[side // 2],
            device_id=where_to[side],
            device_id_type=MESH,
        )

    def await_faces(step, axis):
        low, high = has[2 * axis], has[2 * axis + 1]
        for count, here in ((2, low & high), (1, low ^ high)):

            @pl.when(here)
            def _():
                span = inbox.at[step, pl.ds(2 * axis, count)]
                pltpu.make_async_copy(span, span, halo_recv.at[axis]).wait()

    def await_sent():
        sides = sum(side.astype(jnp.int32) for side in has)
        for count in range(1, 5):

            @pl.when(sides == count)
            def _():
                span = inbox.at[:, pl.ds(0, count)]
                pltpu.make_async_copy(span, span, load_sem.at[6]).wait()

    ahead_of_most = 2 * layer < planes

    def operate(prepare, step, ready, beside):
        def send_faces(sides):
            for side in sides:

                @pl.when(has[side])
                def _():
                    face_copy(step, side).start()

        parts = prepare(0)
        rows = pl.ds(0, edge)
        outer = local(parts, rows, lambda: step or await_rows(geom, 0, edge, 4))
        ends = [
            jnp.where(fast[:width] == NP - 1, part[width:], part[:width]) for part in outer
        ]
        outbox[step, 2] = faces(ends, pick_z)

        early_parts = prepare(1) if step else None

        def inner_work():
            parts = early_parts if step else prepare(1)
            rows = pl.ds(edge, elements - edge)
            found = local(
                parts, rows, lambda: step or await_rows(geom, edge, elements - edge, 5)
            )
            if step == 0:
                for t in range(tiles):
                    image[rows, pl.ds(t * LANES, LANES)] = found[t]
                return None
            return found

        if step == 0:
            pl.when(ahead_of_most)(inner_work)
            ready()
            send_faces((2, 3))
            pl.when(jnp.logical_not(ahead_of_most))(inner_work)
            inner_part = [
                image[pl.ds(edge, elements - edge), pl.ds(t * LANES, LANES)] for t in range(tiles)
            ]
        else:
            send_faces((2, 3))
            inner_part = inner_work()
        result = [jnp.concatenate(pair, axis=0) for pair in zip(outer, inner_part)]
        found_y = faces(result, pick_y)
        face_y[...] = found_y
        outbox[step, 0] = face_y[pl.ds(0, width, stride=EY), :]
        outbox[step, 1] = face_y[pl.ds(EY - 1, width, stride=EY), :]
        send_faces((0, 1))
        found_z = faces(result, pick_z)

        if step == 0:
            make_index()

        face_x = jnp.where(low_half, result[0], result[tiles - 1])
        in_x = jnp.where(
            low_half,
            jnp.where(row_x < EX - 1, pltpu.roll(face_x, elements - EY, axis=0), 0.0),
            jnp.where(row_x > 0, pltpu.roll(face_x, EY, axis=0), 0.0),
        )
        in_y = jnp.where(
            low_half, pltpu.roll(found_y, elements - 1, axis=0), pltpu.roll(found_y, 1, axis=0)
        )
        slot_of = [0] + list(range(2, EZ)) + [1]
        blank = jnp.zeros((width, LANES), jnp.float32)

        def layer(at):
            if at < 0 or at >= EZ:
                return blank
            return found_z[slot_of[at] * width : (slot_of[at] + 1) * width]

        in_z = jnp.concatenate(
            [
                jnp.where(low_border, layer(at + 1), layer(at - 1))
                for at in [0, EZ - 1] + list(range(1, EZ - 1))
            ],
            axis=0,
        )
        got_x = take_lanes(in_x, index[2 * tiles])
        result[0] = result[0] + jnp.where(low_half, got_x, 0.0)
        result[tiles - 1] = result[tiles - 1] + jnp.where(low_half, 0.0, got_x)

        for t in range(tiles):
            result[t] = result[t] + jnp.where(at_z, take_lanes(in_z, index[tiles + t]), 0.0)

        beside()

        await_faces(step, 0)
        halo_y[pl.ds(0, width, stride=EY), :] = inbox[step, 0]
        halo_y[pl.ds(EY - 1, width, stride=EY), :] = inbox[step, 1]
        edge_y = row_y == jnp.where(low_half, EY - 1, 0)
        in_y = jnp.where(edge_y, halo_y[...], in_y)
        for t in range(tiles):
            result[t] = result[t] + jnp.where(at_y, take_lanes(in_y, index[t]), 0.0)
            image[:, pl.ds(t * LANES, LANES)] = result[t]

    def far_faces(step):
        await_faces(step, 1)
        return jnp.where(low_border, inbox[step, 3], inbox[step, 2])

    def add_far(step):
        in_z = jnp.concatenate(
            [
                jnp.where(low_border, 0.0, inbox[step, 2]),
                jnp.where(low_border, inbox[step, 3], 0.0),
            ],
            axis=0,
        )
        for t in range(tiles):
            at = (pl.ds(0, edge), pl.ds(t * LANES, LANES))
            got = take_lanes(in_z, index[tiles + t, pl.ds(0, edge), :])
            image[at] = image[at] + jnp.where(at_z[:edge], got, 0.0)

    def stacked_rows(values):
        return jnp.sum(values.reshape(border // 8, 8, LANES), axis=0)

    def folded(values):
        acc = tile_of(values, 0)
        for tile in range(1, tiles):
            acc = acc + tile_of(values, tile)
        return jnp.sum(acc.reshape(elements // 8, 8, LANES), axis=0)

    def sums_of(partials):
        count = -(-len(partials) // 8) * 8
        rows = [jnp.sum(part, axis=0, keepdims=True) for part in partials]
        rows += [jnp.zeros((1, LANES), jnp.float32)] * (count - len(rows))
        return jnp.sum(jnp.concatenate(rows, axis=0), axis=1, keepdims=True)

    def put(sums, place_of):
        shape = (sums.shape[0], LANES)
        place = place_of(lax.broadcasted_iota(jnp.int32, shape, 0))
        here = place == lax.broadcasted_iota(jnp.int32, shape, 1)
        return jnp.sum(jnp.where(here, sums, 0.0), axis=0, keepdims=True)

    def to_row(partials, begin=0):
        return put(sums_of(partials), lambda at: at + begin)

    def all_sum(block, phase, beside):
        outgoing, incoming = messages[phase]
        outgoing[...] = block
        incoming[pl.ds(me, 1)] = block.reshape((1,) + block.shape)

        def send(where):
            pltpu.make_async_remote_copy(
                src_ref=outgoing,
                dst_ref=incoming.at[me],
                send_sem=load_sem.at[7 + phase],
                recv_sem=(row_recv if phase == 0 else load_sem).at[0],
                device_id=where,
                device_id_type=MESH,
            ).start()

        if phase == 0:

            @pl.when(above)
            def _():
                pl.semaphore_wait(all_ready, planes - 1 - layer)

            @pl.when(below & jnp.logical_not(above))
            def _():
                pl.semaphore_wait(from_below, 1)

        each_peer(send, phase == 1)
        result = beside()
        span = incoming.at[pl.ds(0, devices - 1)]
        pltpu.make_async_copy(span, span, (row_recv if phase == 0 else load_sem).at[0]).wait()
        if devices > 64:
            return jnp.sum(incoming[...], axis=0), result
        found = [incoming[at] for at in range(devices)]
        while len(found) > 1:
            half_way = len(found) // 2
            odd = found[2 * half_way :]
            found = [found[at] + found[half_way + at] for at in range(half_way)] + odd
        return found[0], result

    def weight(row, at):
        spot = jnp.full((8, LANES), at, jnp.int32)
        return take_lanes(jnp.broadcast_to(row, (8, LANES)), spot)

    pieces = [
        (pl.ds(base, 8), pl.ds(tile * LANES, LANES))
        for base in range(0, elements, 8)
        for tile in range(tiles)
    ]

    def against_basis(ref):
        found = [None] * kept
        for at in pieces:
            piece = ref[at]
            for one in range(kept):
                term = basis[(one,) + at] * piece
                found[one] = term if found[one] is None else found[one] + term
        return found

    def against(left, right):
        found = None
        for at in pieces:
            term = left[at] * right[at]
            found = term if found is None else found + term
        return found

    def store_out(which, at, piece):
        begin, tile = at[0].start, at[1].start // LANES
        out[which, tile, pl.ds(places()[begin][1], 8, stride=EZ), :] = piece

    def less_basis(piece, parts, at):
        for one in range(kept):
            piece = piece - parts[one] * basis[(one,) + at]
        return piece

    load_coeffs.wait()

    def start_of(half):
        slots = (0, 1) if half == 0 else range(2, EZ)
        parts = [[] for t in range(tiles)]
        for slot in slots:
            await_rows(basis, slot * width, width, slot)
            for base in range(slot * width, (slot + 1) * width, 8):
                for t in range(tiles):
                    at = (pl.ds(base, 8), pl.ds(t * LANES, LANES))
                    found = None
                    for one in range(kept):
                        term = coeffs[one] * basis[(one,) + at]
                        found = term if found is None else found + term
                    parts[t].append(found)
        if half == 0:
            for copy in load_tables:
                copy.wait()
        return [jnp.concatenate(part, axis=0) for part in parts]

    def greeted():
        pl.semaphore_wait(barrier, greetings)
        to_lower(all_ready)
        to_layer(from_below, layer + 1, jnp.logical_not(below) & above)

    def relay():
        @pl.when(below & above)
        def _():
            pl.semaphore_wait(from_below, 1)

        to_layer(from_below, layer + 1, below & above)

    def meet_basis():
        relay()
        for at in range(kept):
            far_basis[at] = meeting(basis, at)

    operate(start_of, 0, greeted, meet_basis)
    block = 4
    a_line = LANES // kept
    lines = kept // a_line

    def gram():
        found = [jnp.zeros((1, LANES), jnp.float32)] * lines
        for left in range(0, kept, block):
            for right in range(left, kept, block):

                def body(step, carry):
                    base = pl.multiple_of(step * 8, 8)
                    carry = list(carry)
                    for tile in range(tiles):
                        at = (pl.ds(base, 8), pl.ds(tile * LANES, LANES))
                        ones = [basis[(left + m,) + at] for m in range(block)]
                        twos = ones if left == right else [
                            basis[(right + m,) + at] for m in range(block)
                        ]
                        for spot in range(block * block):
                            carry[spot] = carry[spot] + ones[spot // block] * twos[spot % block]
                    return tuple(carry)

                zero = jnp.zeros((8, LANES), jnp.float32)
                partials = lax.fori_loop(0, elements // 8, body, (zero,) * (block * block))
                begin = (left % a_line) * kept + right
                row = put(
                    sums_of(partials), lambda at: begin + (at // block) * kept + at % block
                )
                line_at = left // a_line
                found[line_at] = found[line_at] + (row if left == right else 2.0 * row)
        return found

    near = against_basis(image)
    far = far_faces(0)
    row = to_row([near[at] + stacked_rows(far_basis[at] * far) for at in range(kept)])

    def between():
        add_far(0)
        return gram()

    sums, gram_lines = all_sum(row, 0, between)
    proj_one = sums / total
    parts = [weight(proj_one, at) for at in range(kept)]
    def first_of(half):
        begin, end = (0, edge) if half == 0 else (edge, elements)
        found = []
        for t in range(tiles):
            lanes = pl.ds(t * LANES, LANES)
            for base in range(begin, end, 8):
                at = (pl.ds(base, 8), lanes)
                first[at] = less_basis(image[at], parts, at)
            found.append(first[pl.ds(begin, end - begin), lanes])
        return found

    with_first = []

    def project_first():
        with_first.append(meeting(first))
        with_first.append(
            to_row(
                against_basis(first) + [against(first, first)],
                kept + 2,
            )
        )

    operate(first_of, 1, lambda: None, project_first)
    near = against_basis(image) + [against(first, image), against(image, image)]
    far_first, row_first = with_first
    far_image = 2.0 * meeting(image)
    far = far_faces(1)
    beyond = [stacked_rows(far_basis[at] * far) for at in range(kept)]
    beyond += [stacked_rows(far_first * far), stacked_rows((far_image + far) * far)]
    row = to_row([one + two for one, two in zip(near, beyond)])
    block = jnp.concatenate([row_first + row] + gram_lines, axis=0)

    sums, _ = all_sum(block, 1, lambda: add_far(1))
    sums = sums / total
    along = sums[0:1]
    spot = lax.broadcasted_iota(jnp.int32, (1, LANES), 1)
    inside = spot < kept
    parts = [weight(along, at) for at in range(kept)]
    cross, whole, one = [weight(along, at) for at in (kept, kept + 1, 2 * kept + 2)]
    with_one = pltpu.roll(jnp.broadcast_to(along, (8, LANES)), LANES - kept - 2, axis=1)[0:1]
    pick = lax.broadcasted_iota(jnp.int32, (a_line, LANES), 0) * kept + (
        lax.broadcasted_iota(jnp.int32, (a_line, LANES), 1) % kept
    )
    spread = [
        take_lanes(jnp.broadcast_to(sums[1 + at : 2 + at], (a_line, LANES)), pick)
        for at in range(lines)
    ]
    found = [
        parts[at][0:1] * spread[at // a_line][at % a_line : at % a_line + 1] for at in range(kept)
    ]
    while len(found) > 1:
        found = [found[at] + found[at + 1] for at in range(0, len(found), 2)]
    along_in = jnp.where(inside, along, 0.0)
    terms = jnp.concatenate([along_in * (found[0] - 2.0 * along), along_in * with_one], axis=0)
    terms = jnp.sum(terms, axis=1, keepdims=True)

    scale_one = lax.rsqrt(one + epsilon)
    norm_one = jnp.sqrt(one + epsilon)
    self_two = cross * (scale_one * scale_one)
    for at in pieces:
        piece = first[at]
        store_out(0, at, piece * scale_one)
        image[at] = less_basis(image[at] - self_two * piece, parts, at)

    square = whole + terms[0:1] + self_two * (2.0 * (terms[1:2] - cross) + self_two * one)
    square = jnp.maximum(square, 0.0) * (scale_one * scale_one)
    scale_two = scale_one * lax.rsqrt(square + epsilon)
    norm_two = jnp.sqrt(square + epsilon)
    for at in pieces:
        store_out(1, at, image[at] * scale_two)

    norm_one, scale_one, self_two, norm_two = (
        each[0:1] for each in (norm_one, scale_one, self_two, norm_two)
    )
    row_first = jnp.where(inside, proj_one, jnp.where(spot == kept, norm_one, 0.0))
    row_second = jnp.where(
        inside, along * scale_one, jnp.where(spot == kept, self_two, norm_two)
    )
    hess[pl.ds(0, 1), :] = row_first[:, : kept + 2]
    hess[pl.ds(1, 1), :] = row_second[:, : kept + 2]

    await_sent()
    for phase in range(2):
        span = messages[phase][1].at[pl.ds(0, devices - 1)]
        pltpu.make_async_copy(span, span, load_sem.at[7 + phase]).wait()


def settle(vectors, matrix, out, hess, sem):
    copies = [pltpu.make_async_copy(matrix, hess, sem.at[1])]
    tiles = vectors.shape[1]
    for tile in range(tiles):
        lanes = pl.ds(tile * LANES, LANES)
        copies.append(
            pltpu.make_async_copy(vectors.at[:, tile], out.at[:, :, lanes], sem.at[0])
        )
    for copy in copies:
        copy.start()
    pltpu.make_async_copy(out, out, sem.at[0]).wait()
    copies[0].wait()


def on_device(n_wide, n_narrow, old_basis, restart_coeffs, geometry, orientation):
    kept, elements, points = old_basis.shape
    tiles = points // LANES
    devices = n_wide * n_narrow
    packed, coef = tables()
    rows = 1 + kept * kept // LANES
    anywhere = pl.BlockSpec(memory_space=pl.ANY)
    vmem = pl.BlockSpec(memory_space=pltpu.VMEM)
    f32 = jnp.float32
    border = EX * EY
    shapes = ((2, tiles, elements, LANES), (2, kept + 2))
    held = pl.pallas_call(
        functools.partial(kernel, n_wide, n_narrow),
        out_shape=tuple(pltpu.VMEM(shape, f32) for shape in shapes),
        in_specs=[anywhere] * 6,
        out_specs=(vmem, vmem),
        scratch_shapes=[
            pltpu.SMEM(restart_coeffs.shape, f32),
            pltpu.VMEM(old_basis.shape, f32),
            pltpu.VMEM(geometry.shape, f32),
            pltpu.VMEM(orientation.shape, jnp.int32),
            pltpu.VMEM(packed.shape, jnp.bfloat16),
            pltpu.VMEM(coef.shape, f32),
            pltpu.VMEM((2 * tiles + 1, elements, LANES), jnp.int32),
            pltpu.VMEM((8, LANES), jnp.int32),
            pltpu.VMEM((elements, points), f32),
            pltpu.VMEM((elements, points), f32),
            pltpu.VMEM((elements, LANES), f32),
            pltpu.VMEM((elements, LANES), f32),
            pltpu.VMEM((2, 3, border, LANES), f32),
            pltpu.VMEM((2, 4, border, LANES), f32),
            pltpu.VMEM((1, LANES), f32),
            pltpu.VMEM((devices, 1, LANES), f32),
            pltpu.VMEM((rows, LANES), f32),
            pltpu.VMEM((devices, rows, LANES), f32),
            pltpu.VMEM((border, LANES), jnp.int32),
            pltpu.VMEM((border, LANES), jnp.int32),
            pltpu.VMEM((kept, border, LANES), f32),
            pltpu.SemaphoreType.DMA((10,)),
            pltpu.SemaphoreType.DMA((2,)),
            pltpu.SemaphoreType.DMA((1,)),
            pltpu.SemaphoreType.REGULAR,
            pltpu.SemaphoreType.REGULAR,
        ],
        compiler_params=pltpu.CompilerParams(collective_id=0, has_side_effects=True),
        name="arnoldi",
    )(restart_coeffs, old_basis, geometry, orientation, packed, coef)
    return pl.pallas_call(
        settle,
        out_shape=tuple(
            jax.ShapeDtypeStruct(shape, f32) for shape in ((2, elements, points), shapes[1])
        ),
        in_specs=[vmem, vmem],
        out_specs=(anywhere, anywhere),
        scratch_shapes=[pltpu.SemaphoreType.DMA((2,))],
        name="settle",
    )(*[pltpu.with_memory_space_constraint(each, pltpu.VMEM) for each in held])


def solution(mesh):
    in_specs = (
        P(None, ("wide", "narrow"), None),
        P(),
        P(None, ("wide", "narrow"), None),
        P(None, ("wide", "narrow")),
    )
    out_specs = (P(None, ("wide", "narrow"), None), P())
    return jax.shard_map(
        functools.partial(on_device, mesh.shape["wide"], mesh.shape["narrow"]),
        mesh=mesh,
        in_specs=in_specs,
        out_specs=out_specs,
        check_vma=False,
    )
```

```python
import functools

import jax
import jax.numpy as jnp
import numpy as np
from jax import lax
from jax.experimental import pallas as pl
from jax.experimental.pallas import tpu as pltpu
from jax.sharding import PartitionSpec as P

NP = 8
EX = 4
EY = 4
EZ = 4
LANES = 128
FACE = NP * NP
MESH = pl.DeviceIdType.MESH
highest = lax.Precision.HIGHEST
epsilon = 1e-06


def legendre_columns(nodes, degree):
    columns = [nodes * 0.0 + 1.0, nodes * 1.0]
    for order in range(2, degree + 1):
        columns.append(
            ((2 * order - 1) * nodes * columns[order - 1] - (order - 1) * columns[order - 2])
            / order
        )
    return columns


def gll_derivative(extent):
    degree = extent - 1
    nodes = np.cos(np.pi * np.arange(extent) / degree)
    for sweep in range(100):
        columns = legendre_columns(nodes, degree)
        nodes = nodes - (nodes * columns[degree] - columns[degree - 1]) / (extent * columns[degree])
    gll_nodes = nodes[::-1] * 1.0
    values = legendre_columns(gll_nodes, degree)[degree]
    matrix = np.zeros((extent, extent))
    for row_idx in range(extent):
        for col_idx in range(extent):
            if row_idx != col_idx:
                matrix[row_idx, col_idx] = values[row_idx] / (
                    values[col_idx] * (gll_nodes[row_idx] - gll_nodes[col_idx])
                )
    matrix[0, 0] = -degree * (degree + 1) / 4.0
    matrix[extent - 1, extent - 1] = degree * (degree + 1) / 4.0
    return matrix


def halves(table):
    table = np.asarray(table, np.float32)
    upper = table.astype(jnp.bfloat16).astype(np.float32)
    return upper, table - upper


def tables():
    matrix = gll_derivative(NP)
    identity = np.eye(NP)
    pair = np.eye(2)
    along_y = np.kron(pair, np.kron(matrix, identity))
    along_z = np.kron(pair, np.kron(identity, matrix))
    forward = np.concatenate([along_y.T, along_z.T], axis=1)
    backward = np.concatenate([along_y, along_z], axis=0)
    tiles = NP // 2
    coef = np.zeros((2, tiles, tiles, 2, LANES))
    for way, table in enumerate((matrix, matrix.T)):
        for out_tile in range(tiles):
            for in_tile in range(tiles):
                for half in range(2):
                    lanes = slice(half * FACE, (half + 1) * FACE)
                    row = 2 * out_tile + half
                    coef[way, out_tile, in_tile, 0, lanes] = table[row, 2 * in_tile + half]
                    coef[way, out_tile, in_tile, 1, lanes] = table[row, 2 * in_tile + 1 - half]
    ahead, ahead_rest = halves(forward)
    back, back_rest = halves(backward)
    packed = np.concatenate([ahead, ahead_rest, np.concatenate([back, back_rest], axis=1)], axis=0)
    return (
        jnp.asarray(packed, jnp.bfloat16),
        jnp.asarray(coef.reshape(-1, LANES), jnp.float32),
    )


def places():
    order = [0, EZ - 1] + list(range(1, EZ - 1))
    width = EX * EY
    return [
        (slot * width + at, at * EZ + layer) for slot, layer in enumerate(order) for at in range(width)
    ]


def take_lanes(values, index):
    return jnp.take_along_axis(values, index, axis=1, mode="promise_in_bounds")


def rotated(row, col, code):
    row = row ^ (7 * (code & 1))
    col = col ^ (7 * ((code >> 1) & 1))
    return jnp.where((code & 4) != 0, col * NP + row, row * NP + col)


def kernel(
    n_wide,
    n_narrow,
    coeffs_hbm,
    basis_hbm,
    geom_hbm,
    orient_hbm,
    packed_hbm,
    coef_hbm,
    out,
    hess,
    coeffs,
    basis,
    geom,
    orient,
    packed,
    coef,
    index,
    orient_pad,
    image,
    first,
    face_y,
    halo_y,
    outbox,
    inbox,
    row_out,
    row_in,
    pair_out,
    pair_in,
    far_index,
    far_tile,
    far_basis,
    load_sem,
    halo_recv,
    row_recv,
    all_ready,
    from_below,
):
    wide = lax.axis_index("wide")
    narrow = lax.axis_index("narrow")
    devices = n_wide * n_narrow
    me = wide * n_narrow + narrow
    kept, elements, points = basis.shape
    tiles = points // LANES
    total = float(elements * points * devices)

    def load(source, target, slot):
        return pltpu.make_async_copy(source, target, load_sem.at[slot])

    width = EX * EY
    edge = 2 * width

    def load_rows(source, target, begin, count, slot):
        copies = [
            load(source.at[:, pl.ds(there, 1)], target.at[:, pl.ds(here, 1)], slot)
            for here, there in places()[begin : begin + count]
        ]
        for copy in copies:
            copy.start()

    def await_rows(target, begin, count, slot):
        span = target.at[:, pl.ds(begin, count)]
        load(span, span, slot).wait()

    load_coeffs = load(coeffs_hbm, coeffs, 6)
    load_tables = [load(packed_hbm, packed, 7), load(coef_hbm, coef, 8)]
    load_orient = load(orient_hbm, orient, 9)
    load_coeffs.start()
    for copy in load_tables:
        copy.start()
    for slot in range(2):
        load_rows(basis_hbm, basis, slot * width, width, slot)
    messages = ((row_out, row_in), (pair_out, pair_in))

    def peer(step):
        if devices & (devices - 1):
            other = lax.rem(me + step, devices)
        else:
            other = me
            for bit in range(devices.bit_length() - 1):
                if step >> bit & 1:
                    other = other + (1 - 2 * lax.rem(me // 2**bit, 2)) * 2**bit
        return (other // n_narrow, lax.rem(other, n_narrow))

    def each_peer(act, ascending):
        if devices > 64:

            def body(step, carry):
                other = lax.rem(me + step, devices)
                act((other // n_narrow, lax.rem(other, n_narrow)))
                return carry

            lax.fori_loop(1, devices, body, 0)
        elif ascending:
            for at in range(devices - 1):
                other = at + (me <= at).astype(jnp.int32)
                act((other // n_narrow, lax.rem(other, n_narrow)))
        else:
            for step in range(devices - 1, 0, -1):
                act(peer(step))

    barrier = pltpu.get_barrier_semaphore()

    inner = 1
    while n_wide % (2 * inner) == 0 and 4 * inner * inner <= n_wide:
        inner = 2 * inner
    plane = inner * n_narrow
    planes = n_wide // inner
    layer = wide // inner
    column = lax.rem(wide, inner)
    in_plane = column * n_narrow + narrow

    def in_steps(count, act):
        if count <= 64:
            for step in range(count - 1, 0, -1):
                act(step)
        else:

            def body(step, carry):
                act(step)
                return carry

            lax.fori_loop(1, count, body, 0)

    def signal(semaphore, where):
        pl.semaphore_signal(semaphore, inc=1, device_id=where, device_id_type=MESH)

    def to_layer(semaphore, other, there):
        @pl.when(there)
        def _():
            signal(semaphore, (other * inner + column, narrow))

    def to_higher(semaphore):
        for step in range(planes - 1, 0, -1):
            to_layer(semaphore, layer + step, layer + step < planes)

    def to_lower(semaphore):
        for step in range(planes - 1, 0, -1):
            to_layer(semaphore, layer - step, layer >= step)

    def to_plane(semaphore):
        def act(step):
            other = lax.rem(in_plane + step, plane)
            signal(semaphore, (layer * inner + other // n_narrow, lax.rem(other, n_narrow)))

        in_steps(plane, act)

    below = layer > 0
    above = layer < planes - 1
    greetings = plane - 1 + layer + above.astype(jnp.int32)
    crossing = ()
    if 1 < inner < n_wide:
        crossing = (
            ((column == 0) & (wide > 0), -1),
            ((column == inner - 1) & (wide < n_wide - 1), 1),
        )
    for there, shift in crossing:
        greetings = greetings + there.astype(jnp.int32)

    def greet():
        to_layer(barrier, layer - 1, below)
        to_higher(barrier)
        for there, shift in crossing:

            @pl.when(there)
            def _():
                signal(barrier, (wide + shift, narrow))

        to_plane(barrier)

    inbox[...] = jnp.zeros_like(inbox)
    greet()
    load_rows(geom_hbm, geom, 0, edge, 4)
    for slot in range(2, EZ):
        load_rows(basis_hbm, basis, slot * width, width, slot)
    load_rows(geom_hbm, geom, edge, elements - edge, 5)
    load_orient.start()

    lane = lax.broadcasted_iota(jnp.int32, (elements, LANES), 1)
    line = lax.broadcasted_iota(jnp.int32, (elements, LANES), 0)
    low_half = lane < FACE
    border = width
    low_border = low_half[:border]
    half = lane // FACE
    mid = (lane // NP) % NP
    fast = lane % NP
    row_x = (line // EY) % EX
    row_y = line % EY
    at_y = (mid == 0) | (mid == NP - 1)
    at_z = (fast == 0) | (fast == NP - 1)

    pick_y = (mid % 2) * FACE + half * (FACE - NP) + fast
    pick_z = (mid % 2) * FACE + fast * NP + half * (NP - 1)
    source_tile = mid // 2

    def make_index():
        load_orient.wait()
        orient_pad[...] = jnp.zeros_like(orient_pad)
        orient_pad[pl.ds(0, 6), pl.ds(0, elements)] = orient[...]
        across = lax.broadcasted_iota(jnp.int32, (8, LANES), 1)
        slot = (across // width) % EZ
        depth = jnp.where(slot < 2, slot * (EZ - 1), slot - 1)
        shuffled = take_lanes(orient_pad[...], (across % width) * EZ + depth)
        codes = jnp.transpose(shuffled)[:elements]
        code = [jnp.broadcast_to(codes[:, f : f + 1], (elements, LANES)) for f in range(6)]
        code_x = jnp.where(low_half, code[0], code[1])
        index[2 * tiles] = rotated(mid, fast, code_x) + jnp.where(low_half, FACE, 0)
        code_y = jnp.where(mid == 0, code[2], code[3])
        code_z = jnp.where(fast == 0, code[4], code[5])
        for tile in range(tiles):
            first_pos = 2 * tile + half
            index[tile] = rotated(first_pos, fast, code_y) + jnp.where(mid == 0, FACE, 0)
            index[tiles + tile] = rotated(first_pos, mid, code_z) + jnp.where(fast == 0, FACE, 0)
        found = jnp.where(low_border, code[5][width:edge], code[4][:width])
        turned = (found & 4) != 0
        along_a = jnp.where(turned, fast[:border], mid[:border]) ^ (7 * (found & 1))
        along_b = jnp.where(turned, mid[:border], fast[:border]) ^ (7 * ((found >> 1) & 1))
        far_index[...] = (along_a % 2) * FACE + along_b * NP + jnp.where(low_border, NP - 1, 0)
        far_tile[...] = along_a // 2

    def meeting(ref, *at):
        found = None
        for t in range(tiles):
            lanes = pl.ds(t * LANES, LANES)
            last = ref[at + (pl.ds(width, width), lanes)]
            begin = ref[at + (pl.ds(0, width), lanes)]
            got = take_lanes(jnp.where(fast[:border] == NP - 1, last, begin), far_index[...])
            found = got if found is None else jnp.where(far_tile[...] == t, got, found)
        return found

    def tile_of(values, tile):
        return values[:, tile * LANES : (tile + 1) * LANES]

    def swap(values):
        return pltpu.roll(values, FACE, axis=1)

    def along_x(parts, way):
        swapped = [swap(part) for part in parts]
        outs = []
        for out_tile in range(tiles):
            acc = None
            for in_tile in range(tiles):
                at = ((way * tiles + out_tile) * tiles + in_tile) * 2
                term = (
                    coef[pl.ds(at, 1), :] * parts[in_tile]
                    + coef[pl.ds(at + 1, 1), :] * swapped[in_tile]
                )
                acc = term if acc is None else acc + term
            outs.append(acc)
        return outs

    def split(values):
        upper = values.astype(jnp.bfloat16)
        return upper, (values - upper.astype(jnp.float32)).astype(jnp.bfloat16)

    def product(left, right):
        return jnp.dot(left, right, preferred_element_type=jnp.float32)

    def local(parts, rows, geometry_here=lambda: None):
        count = parts[0].shape[0]
        stacked = jnp.concatenate(split(jnp.concatenate(parts, axis=0)), axis=1)
        ahead = packed[pl.ds(0, LANES), :]
        ahead_rest = packed[pl.ds(LANES, LANES), :]
        grads = product(stacked, jnp.concatenate([ahead, ahead], axis=0)) + product(
            stacked, jnp.concatenate([ahead_rest, ahead_rest], axis=0)
        )
        grad_x = along_x(parts, 0)
        geometry_here()
        geom_y = jnp.concatenate([geom[1, rows, pl.ds(t * LANES, LANES)] for t in range(tiles)], axis=0)
        geom_z = jnp.concatenate([geom[2, rows, pl.ds(t * LANES, LANES)] for t in range(tiles)], axis=0)
        flux = jnp.concatenate([grads[:, :LANES] * geom_y, grads[:, LANES:] * geom_z], axis=1)
        flux, flux_rest = split(flux)
        behind = packed[pl.ds(2 * LANES, 2 * LANES), :]
        back = product(flux, behind) + product(flux_rest, behind)
        back = back[:, :LANES] + back[:, LANES:]
        flux_x = [grad_x[t] * geom[0, rows, pl.ds(t * LANES, LANES)] for t in range(tiles)]
        back_x = along_x(flux_x, 1)
        return [
            back[t * count : (t + 1) * count]
            + back_x[t]
            + geom[3, rows, pl.ds(t * LANES, LANES)] * parts[t]
            for t in range(tiles)
        ]

    def faces(parts, pick):
        count = parts[0].shape[0]
        pick, source = pick[:count], source_tile[:count]
        found = take_lanes(parts[0], pick)
        for tile in range(1, tiles):
            found = jnp.where(source == tile, take_lanes(parts[tile], pick), found)
        return found

    has = (narrow > 0, narrow < n_narrow - 1, wide > 0, wide < n_wide - 1)
    where_to = ((wide, narrow - 1), (wide, narrow + 1), (wide - 1, narrow), (wide + 1, narrow))

    def face_copy(step, side):
        return pltpu.make_async_remote_copy(
            src_ref=outbox.at[step, min(side, 2)],
            dst_ref=inbox.at[step, side ^ 1],
            send_sem=load_sem.at[6],
            recv_sem=halo_recv.at[side // 2],
            device_id=where_to[side],
            device_id_type=MESH,
        )

    def await_faces(step, axis):
        low, high = has[2 * axis], has[2 * axis + 1]
        for count, here in ((2, low & high), (1, low ^ high)):

            @pl.when(here)
            def _():
                span = inbox.at[step, pl.ds(2 * axis, count)]
                pltpu.make_async_copy(span, span, halo_recv.at[axis]).wait()

    def await_sent():
        sides = sum(side.astype(jnp.int32) for side in has)
        for count in range(1, 5):

            @pl.when(sides == count)
            def _():
                span = inbox.at[:, pl.ds(0, count)]
                pltpu.make_async_copy(span, span, load_sem.at[6]).wait()

    ahead_of_most = 2 * layer < planes

    def operate(prepare, step, ready, beside):
        def send_faces(sides):
            for side in sides:

                @pl.when(has[side])
                def _():
                    face_copy(step, side).start()

        parts = prepare(0)
        rows = pl.ds(0, edge)
        outer = local(parts, rows, lambda: step or await_rows(geom, 0, edge, 4))
        ends = [
            jnp.where(fast[:width] == NP - 1, part[width:], part[:width]) for part in outer
        ]
        outbox[step, 2] = faces(ends, pick_z)

        def inner_work():
            parts = prepare(1)
            rows = pl.ds(edge, elements - edge)
            found = local(
                parts, rows, lambda: step or await_rows(geom, edge, elements - edge, 5)
            )
            if step == 0:
                for t in range(tiles):
                    image[rows, pl.ds(t * LANES, LANES)] = found[t]
                return None
            return found

        if step == 0:
            pl.when(ahead_of_most)(inner_work)
            ready()
            send_faces((2, 3))
            pl.when(jnp.logical_not(ahead_of_most))(inner_work)
            inner_part = [
                image[pl.ds(edge, elements - edge), pl.ds(t * LANES, LANES)] for t in range(tiles)
            ]
        else:
            send_faces((2, 3))
            inner_part = inner_work()
        result = [jnp.concatenate(pair, axis=0) for pair in zip(outer, inner_part)]
        found_y = faces(result, pick_y)
        face_y[...] = found_y
        outbox[step, 0] = face_y[pl.ds(0, width, stride=EY), :]
        outbox[step, 1] = face_y[pl.ds(EY - 1, width, stride=EY), :]
        send_faces((0, 1))
        found_z = faces(result, pick_z)

        if step == 0:
            make_index()

        face_x = jnp.where(low_half, result[0], result[tiles - 1])
        in_x = jnp.where(
            low_half,
            jnp.where(row_x < EX - 1, pltpu.roll(face_x, elements - EY, axis=0), 0.0),
            jnp.where(row_x > 0, pltpu.roll(face_x, EY, axis=0), 0.0),
        )
        in_y = jnp.where(
            low_half, pltpu.roll(found_y, elements - 1, axis=0), pltpu.roll(found_y, 1, axis=0)
        )
        slot_of = [0] + list(range(2, EZ)) + [1]
        blank = jnp.zeros((width, LANES), jnp.float32)

        def layer(at):
            if at < 0 or at >= EZ:
                return blank
            return found_z[slot_of[at] * width : (slot_of[at] + 1) * width]

        in_z = jnp.concatenate(
            [
                jnp.where(low_border, layer(at + 1), layer(at - 1))
                for at in [0, EZ - 1] + list(range(1, EZ - 1))
            ],
            axis=0,
        )
        got_x = take_lanes(in_x, index[2 * tiles])
        result[0] = result[0] + jnp.where(low_half, got_x, 0.0)
        result[tiles - 1] = result[tiles - 1] + jnp.where(low_half, 0.0, got_x)

        for t in range(tiles):
            result[t] = result[t] + jnp.where(at_z, take_lanes(in_z, index[tiles + t]), 0.0)

        beside()

        await_faces(step, 0)
        halo_y[pl.ds(0, width, stride=EY), :] = inbox[step, 0]
        halo_y[pl.ds(EY - 1, width, stride=EY), :] = inbox[step, 1]
        edge_y = row_y == jnp.where(low_half, EY - 1, 0)
        in_y = jnp.where(edge_y, halo_y[...], in_y)
        for t in range(tiles):
            result[t] = result[t] + jnp.where(at_y, take_lanes(in_y, index[t]), 0.0)
            image[:, pl.ds(t * LANES, LANES)] = result[t]

    def far_faces(step):
        await_faces(step, 1)
        return jnp.where(low_border, inbox[step, 3], inbox[step, 2])

    def add_far(step):
        in_z = jnp.concatenate(
            [
                jnp.where(low_border, 0.0, inbox[step, 2]),
                jnp.where(low_border, inbox[step, 3], 0.0),
            ],
            axis=0,
        )
        for t in range(tiles):
            at = (pl.ds(0, edge), pl.ds(t * LANES, LANES))
            got = take_lanes(in_z, index[tiles + t, pl.ds(0, edge), :])
            image[at] = image[at] + jnp.where(at_z[:edge], got, 0.0)

    def stacked_rows(values):
        return jnp.sum(values.reshape(border // 8, 8, LANES), axis=0)

    def folded(values):
        acc = tile_of(values, 0)
        for tile in range(1, tiles):
            acc = acc + tile_of(values, tile)
        return jnp.sum(acc.reshape(elements // 8, 8, LANES), axis=0)

    def sums_of(partials):
        count = -(-len(partials) // 8) * 8
        rows = [jnp.sum(part, axis=0, keepdims=True) for part in partials]
        rows += [jnp.zeros((1, LANES), jnp.float32)] * (count - len(rows))
        return jnp.sum(jnp.concatenate(rows, axis=0), axis=1, keepdims=True)

    def put(sums, place_of):
        shape = (sums.shape[0], LANES)
        place = place_of(lax.broadcasted_iota(jnp.int32, shape, 0))
        here = place == lax.broadcasted_iota(jnp.int32, shape, 1)
        return jnp.sum(jnp.where(here, sums, 0.0), axis=0, keepdims=True)

    def to_row(partials, begin=0):
        return put(sums_of(partials), lambda at: at + begin)

    def all_sum(block, phase, beside):
        outgoing, incoming = messages[phase]
        outgoing[...] = block
        incoming[pl.ds(me, 1)] = block.reshape((1,) + block.shape)

        def send(where):
            pltpu.make_async_remote_copy(
                src_ref=outgoing,
                dst_ref=incoming.at[me],
                send_sem=load_sem.at[7 + phase],
                recv_sem=(row_recv if phase == 0 else load_sem).at[0],
                device_id=where,
                device_id_type=MESH,
            ).start()

        if phase == 0:

            @pl.when(above)
            def _():
                pl.semaphore_wait(all_ready, planes - 1 - layer)

            @pl.when(below & jnp.logical_not(above))
            def _():
                pl.semaphore_wait(from_below, 1)

        each_peer(send, phase == 1)
        result = beside()
        span = incoming.at[pl.ds(0, devices - 1)]
        pltpu.make_async_copy(span, span, (row_recv if phase == 0 else load_sem).at[0]).wait()
        if devices > 64:
            return jnp.sum(incoming[...], axis=0), result
        found = [incoming[at] for at in range(devices)]
        while len(found) > 1:
            half_way = len(found) // 2
            odd = found[2 * half_way :]
            found = [found[at] + found[half_way + at] for at in range(half_way)] + odd
        return found[0], result

    def weight(row, at):
        spot = jnp.full((8, LANES), at, jnp.int32)
        return take_lanes(jnp.broadcast_to(row, (8, LANES)), spot)

    pieces = [
        (pl.ds(base, 8), pl.ds(tile * LANES, LANES))
        for base in range(0, elements, 8)
        for tile in range(tiles)
    ]

    def against_basis(ref):
        found = [None] * kept
        for at in pieces:
            piece = ref[at]
            for one in range(kept):
                term = basis[(one,) + at] * piece
                found[one] = term if found[one] is None else found[one] + term
        return found

    def against(left, right):
        found = None
        for at in pieces:
            term = left[at] * right[at]
            found = term if found is None else found + term
        return found

    def store_out(which, at, piece):
        begin, tile = at[0].start, at[1].start // LANES
        out[which, tile, pl.ds(places()[begin][1], 8, stride=EZ), :] = piece

    def less_basis(piece, parts, at):
        for one in range(kept):
            piece = piece - parts[one] * basis[(one,) + at]
        return piece

    load_coeffs.wait()

    def start_of(half):
        slots = (0, 1) if half == 0 else range(2, EZ)
        parts = [[] for t in range(tiles)]
        for slot in slots:
            await_rows(basis, slot * width, width, slot)
            for base in range(slot * width, (slot + 1) * width, 8):
                for t in range(tiles):
                    at = (pl.ds(base, 8), pl.ds(t * LANES, LANES))
                    found = None
                    for one in range(kept):
                        term = coeffs[one] * basis[(one,) + at]
                        found = term if found is None else found + term
                    parts[t].append(found)
        if half == 0:
            for copy in load_tables:
                copy.wait()
        return [jnp.concatenate(part, axis=0) for part in parts]

    def greeted():
        pl.semaphore_wait(barrier, greetings)
        to_lower(all_ready)
        to_layer(from_below, layer + 1, jnp.logical_not(below) & above)

    def relay():
        @pl.when(below & above)
        def _():
            pl.semaphore_wait(from_below, 1)

        to_layer(from_below, layer + 1, below & above)

    def meet_basis():
        relay()
        for at in range(kept):
            far_basis[at] = meeting(basis, at)

    operate(start_of, 0, greeted, meet_basis)
    block = 4
    a_line = LANES // kept
    lines = kept // a_line

    def gram():
        found = [jnp.zeros((1, LANES), jnp.float32)] * lines
        for left in range(0, kept, block):
            for right in range(left, kept, block):

                def body(step, carry):
                    base = pl.multiple_of(step * 8, 8)
                    carry = list(carry)
                    for tile in range(tiles):
                        at = (pl.ds(base, 8), pl.ds(tile * LANES, LANES))
                        ones = [basis[(left + m,) + at] for m in range(block)]
                        twos = ones if left == right else [
                            basis[(right + m,) + at] for m in range(block)
                        ]
                        for spot in range(block * block):
                            carry[spot] = carry[spot] + ones[spot // block] * twos[spot % block]
                    return tuple(carry)

                zero = jnp.zeros((8, LANES), jnp.float32)
                partials = lax.fori_loop(0, elements // 8, body, (zero,) * (block * block))
                begin = (left % a_line) * kept + right
                row = put(
                    sums_of(partials), lambda at: begin + (at // block) * kept + at % block
                )
                line_at = left // a_line
                found[line_at] = found[line_at] + (row if left == right else 2.0 * row)
        return found

    near = against_basis(image)
    far = far_faces(0)
    row = to_row([near[at] + stacked_rows(far_basis[at] * far) for at in range(kept)])

    def between():
        add_far(0)
        return gram()

    sums, gram_lines = all_sum(row, 0, between)
    proj_one = sums / total
    parts = [weight(proj_one, at) for at in range(kept)]
    def first_of(half):
        begin, end = (0, edge) if half == 0 else (edge, elements)
        found = []
        for t in range(tiles):
            lanes = pl.ds(t * LANES, LANES)
            for base in range(begin, end, 8):
                at = (pl.ds(base, 8), lanes)
                first[at] = less_basis(image[at], parts, at)
            found.append(first[pl.ds(begin, end - begin), lanes])
        return found

    with_first = []

    def project_first():
        with_first.append(meeting(first))
        with_first.append(
            to_row(
                against_basis(first) + [against(first, first)],
                kept + 2,
            )
        )

    operate(first_of, 1, lambda: None, project_first)
    near = against_basis(image) + [against(first, image), against(image, image)]
    far_first, row_first = with_first
    far_image = 2.0 * meeting(image)
    far = far_faces(1)
    beyond = [stacked_rows(far_basis[at] * far) for at in range(kept)]
    beyond += [stacked_rows(far_first * far), stacked_rows((far_image + far) * far)]
    row = to_row([one + two for one, two in zip(near, beyond)])
    block = jnp.concatenate([row_first + row] + gram_lines, axis=0)

    sums, _ = all_sum(block, 1, lambda: add_far(1))
    sums = sums / total
    along = sums[0:1]
    spot = lax.broadcasted_iota(jnp.int32, (1, LANES), 1)
    inside = spot < kept
    parts = [weight(along, at) for at in range(kept)]
    cross, whole, one = [weight(along, at) for at in (kept, kept + 1, 2 * kept + 2)]
    with_one = pltpu.roll(jnp.broadcast_to(along, (8, LANES)), LANES - kept - 2, axis=1)[0:1]
    pick = lax.broadcasted_iota(jnp.int32, (a_line, LANES), 0) * kept + (
        lax.broadcasted_iota(jnp.int32, (a_line, LANES), 1) % kept
    )
    spread = [
        take_lanes(jnp.broadcast_to(sums[1 + at : 2 + at], (a_line, LANES)), pick)
        for at in range(lines)
    ]
    found = [
        parts[at][0:1] * spread[at // a_line][at % a_line : at % a_line + 1] for at in range(kept)
    ]
    while len(found) > 1:
        found = [found[at] + found[at + 1] for at in range(0, len(found), 2)]
    along_in = jnp.where(inside, along, 0.0)
    terms = jnp.concatenate([along_in * (found[0] - 2.0 * along), along_in * with_one], axis=0)
    terms = jnp.sum(terms, axis=1, keepdims=True)

    scale_one = lax.rsqrt(one + epsilon)
    norm_one = jnp.sqrt(one + epsilon)
    self_two = cross * (scale_one * scale_one)
    for at in pieces:
        image[at] = less_basis(image[at], parts, at)
    for at in pieces:
        piece = first[at]
        store_out(0, at, piece * scale_one)
        image[at] = image[at] - self_two * piece

    square = whole + terms[0:1] + self_two * (2.0 * (terms[1:2] - cross) + self_two * one)
    square = jnp.maximum(square, 0.0) * (scale_one * scale_one)
    scale_two = scale_one * lax.rsqrt(square + epsilon)
    norm_two = jnp.sqrt(square + epsilon)
    for at in pieces:
        store_out(1, at, image[at] * scale_two)

    norm_one, scale_one, self_two, norm_two = (
        each[0:1] for each in (norm_one, scale_one, self_two, norm_two)
    )
    row_first = jnp.where(inside, proj_one, jnp.where(spot == kept, norm_one, 0.0))
    row_second = jnp.where(
        inside, along * scale_one, jnp.where(spot == kept, self_two, norm_two)
    )
    hess[pl.ds(0, 1), :] = row_first[:, : kept + 2]
    hess[pl.ds(1, 1), :] = row_second[:, : kept + 2]

    await_sent()
    for phase in range(2):
        span = messages[phase][1].at[pl.ds(0, devices - 1)]
        pltpu.make_async_copy(span, span, load_sem.at[7 + phase]).wait()


def settle(vectors, matrix, out, hess, sem):
    copies = [pltpu.make_async_copy(matrix, hess, sem.at[1])]
    tiles = vectors.shape[1]
    for tile in range(tiles):
        lanes = pl.ds(tile * LANES, LANES)
        copies.append(
            pltpu.make_async_copy(vectors.at[:, tile], out.at[:, :, lanes], sem.at[0])
        )
    for copy in copies:
        copy.start()
    pltpu.make_async_copy(out, out, sem.at[0]).wait()
    copies[0].wait()


def on_device(n_wide, n_narrow, old_basis, restart_coeffs, geometry, orientation):
    kept, elements, points = old_basis.shape
    tiles = points // LANES
    devices = n_wide * n_narrow
    packed, coef = tables()
    rows = 1 + kept * kept // LANES
    anywhere = pl.BlockSpec(memory_space=pl.ANY)
    vmem = pl.BlockSpec(memory_space=pltpu.VMEM)
    f32 = jnp.float32
    border = EX * EY
    shapes = ((2, tiles, elements, LANES), (2, kept + 2))
    held = pl.pallas_call(
        functools.partial(kernel, n_wide, n_narrow),
        out_shape=tuple(pltpu.VMEM(shape, f32) for shape in shapes),
        in_specs=[anywhere] * 6,
        out_specs=(vmem, vmem),
        scratch_shapes=[
            pltpu.SMEM(restart_coeffs.shape, f32),
            pltpu.VMEM(old_basis.shape, f32),
            pltpu.VMEM(geometry.shape, f32),
            pltpu.VMEM(orientation.shape, jnp.int32),
            pltpu.VMEM(packed.shape, jnp.bfloat16),
            pltpu.VMEM(coef.shape, f32),
            pltpu.VMEM((2 * tiles + 1, elements, LANES), jnp.int32),
            pltpu.VMEM((8, LANES), jnp.int32),
            pltpu.VMEM((elements, points), f32),
            pltpu.VMEM((elements, points), f32),
            pltpu.VMEM((elements, LANES), f32),
            pltpu.VMEM((elements, LANES), f32),
            pltpu.VMEM((2, 3, border, LANES), f32),
            pltpu.VMEM((2, 4, border, LANES), f32),
            pltpu.VMEM((1, LANES), f32),
            pltpu.VMEM((devices, 1, LANES), f32),
            pltpu.VMEM((rows, LANES), f32),
            pltpu.VMEM((devices, rows, LANES), f32),
            pltpu.VMEM((border, LANES), jnp.int32),
            pltpu.VMEM((border, LANES), jnp.int32),
            pltpu.VMEM((kept, border, LANES), f32),
            pltpu.SemaphoreType.DMA((10,)),
            pltpu.SemaphoreType.DMA((2,)),
            pltpu.SemaphoreType.DMA((1,)),
            pltpu.SemaphoreType.REGULAR,
            pltpu.SemaphoreType.REGULAR,
        ],
        compiler_params=pltpu.CompilerParams(collective_id=0, has_side_effects=True),
        name="arnoldi",
    )(restart_coeffs, old_basis, geometry, orientation, packed, coef)
    return pl.pallas_call(
        settle,
        out_shape=tuple(
            jax.ShapeDtypeStruct(shape, f32) for shape in ((2, elements, points), shapes[1])
        ),
        in_specs=[vmem, vmem],
        out_specs=(anywhere, anywhere),
        scratch_shapes=[pltpu.SemaphoreType.DMA((2,))],
        name="settle",
    )(*[pltpu.with_memory_space_constraint(each, pltpu.VMEM) for each in held])


def solution(mesh):
    in_specs = (
        P(None, ("wide", "narrow"), None),
        P(),
        P(None, ("wide", "narrow"), None),
        P(None, ("wide", "narrow")),
    )
    out_specs = (P(None, ("wide", "narrow"), None), P())
    return jax.shard_map(
        functools.partial(on_device, mesh.shape["wide"], mesh.shape["narrow"]),
        mesh=mesh,
        in_specs=in_specs,
        out_specs=out_specs,
        check_vma=False,
    )
```
